256 devices in a mesh: rep: 2 (over core), dp: 128 (over x, y, z).
Axes of the slice: x: 4, y: 4, z: 8, core: 2. Of those that a mesh axis runs over, the one named last changes fastest.
Arguments:
- x: bfloat16 [256, 2048, 896], P(('rep', 'dp')), parts along dimension 0
- dy: bfloat16 [256, 2048, 896], P(('rep', 'dp')), parts along dimension 0
- w_gate: bfloat16 [2, 896, 2560], replicated
- w_up: bfloat16 [2, 896, 2560], replicated
- w_down: bfloat16 [2, 2560, 896], replicated
- m_w_gate: float32 [2, 896, 2560], P(None, 'dp')
- m_w_up: float32 [2, 896, 2560], P(None, 'dp')
- m_w_down: float32 [2, 2560, 896], P(None, 'dp')
- v_w_gate: float32 [2, 896, 2560], P(None, 'dp')
- v_w_up: float32 [2, 896, 2560], P(None, 'dp')
- v_w_down: float32 [2, 2560, 896], P(None, 'dp')
Outputs:
- output 1: bfloat16 [4, 896, 2560], P('rep'), parts along dimension 0
- output 2: bfloat16 [4, 896, 2560], P('rep'), parts along dimension 0
- output 3: bfloat16 [4, 2560, 896], P('rep'), parts along dimension 0
- output 4: float32 [4, 896, 2560], P('rep', 'dp'), parts along dimension 0
- output 5: float32 [4, 896, 2560], P('rep', 'dp'), parts along dimension 0
- output 6: float32 [4, 2560, 896], P('rep', 'dp'), parts along dimension 0
- output 7: float32 [4, 896, 2560], P('rep', 'dp'), parts along dimension 0
- output 8: float32 [4, 896, 2560], P('rep', 'dp'), parts along dimension 0
- output 9: float32 [4, 2560, 896], P('rep', 'dp'), parts along dimension 0
There are 2 independent parts. The reference program is written for one: setup_inputs(seed, part) draws one part's arguments, and reference() takes and returns one part's arrays. A program takes and returns all parts, laid end to end along the dimension named above; an argument that names none is the same for every part.
All inputs are finite; a program needn't handle non-finite values.
Results may differ from the reference program's by a relative error of at most 0.022.
Values are sent between devices in bfloat16 or wider.
A program may use at most 768 MiB of HBM per device.

```python
import jax
import jax.numpy as jnp
from jax import lax

SEQUENCES = 128
TOKENS = 2048
D = 896
FF = 2560
LAYERS = 2
NAMES = ("w_gate", "w_up", "w_down")
SHAPES = {"w_gate": (LAYERS, D, FF), "w_up": (LAYERS, D, FF), "w_down": (LAYERS, FF, D)}


def bump(key, n, height):
    away = (jnp.arange(n, dtype=jnp.int32) - jax.random.randint(key, (), 0, n, jnp.int32)) % n
    return jnp.where(away < n // 8, height, 1.0)


def together(key, own, strength):
    shared = jax.random.normal(key, own.shape[1:], jnp.float32)
    return (own + strength * shared) * lax.rsqrt(1 + strength * strength)


def setup_inputs(seed: int = 0, part: int = 0) -> dict:
    kx, kdy, ka, kb, kz, kf, kh, kl, *keys = jax.random.split(jax.random.key(seed), 8 + 3 * len(NAMES))
    kx, kdy, ka, kb = (jax.random.fold_in(k, part) for k in (kx, kdy, ka, kb))
    kw, km, kv = (keys[i::3] for i in range(3))
    shape = (SEQUENCES, TOKENS, D)
    much_x, much_dy = jax.random.uniform(kz, (2,), jnp.float32, 0.0, 1.0)
    loud = 2.0 ** jax.random.uniform(jax.random.fold_in(kz, 1), (), jnp.float32, -1.0, 2.0)
    layers = 2.0 ** jax.random.uniform(kl, (LAYERS, 1, 1), jnp.float32, -1.0, 1.0)
    x = together(ka, jax.random.normal(kx, shape, jnp.float32), much_x) * bump(kf, D, 4.0)
    dy = together(kb, jax.random.normal(kdy, shape, jnp.float32), much_dy)
    drawn = {"x": x.astype(jnp.bfloat16), "dy": (loud * dy * (SEQUENCES * TOKENS) ** -0.5).astype(jnp.bfloat16)}
    for key, name in zip(kw, NAMES, strict=True):
        w = jax.random.normal(key, SHAPES[name], jnp.float32) * SHAPES[name][1] ** -0.5
        drawn[name] = (w * {"w_gate": 1.0, "w_up": bump(kh, FF, 4.0), "w_down": layers}[name]).astype(jnp.bfloat16)
    for key, name in zip(km, NAMES, strict=True):
        drawn[f"m_{name}"] = 0.1 * jax.random.normal(key, SHAPES[name], jnp.float32)
    for key, name in zip(kv, NAMES, strict=True):
        drawn[f"v_{name}"] = jax.random.uniform(key, SHAPES[name], jnp.float32, 0.005, 0.015)
    return drawn


def matmul(a, w):
    return jnp.dot(a, w, preferred_element_type=jnp.float32).astype(jnp.bfloat16)


def normed(h):
    wide = h.astype(jnp.float32)
    scale = lax.rsqrt(jnp.mean(wide**2, -1, keepdims=True) + 1e-6)
    return (wide * scale).astype(jnp.bfloat16)


def layer(h, w):
    a = normed(h)
    gate = jnp.dot(a, w["w_gate"], preferred_element_type=jnp.float32)
    up = jnp.dot(a, w["w_up"], preferred_element_type=jnp.float32)
    return h + matmul((jax.nn.silu(gate) * up).astype(jnp.bfloat16), w["w_down"])


def adamw(w, m, v, g):
    m = 0.9 * m + 0.1 * g
    v = 0.95 * v + 0.05 * g * g
    step = m * lax.rsqrt(v + 1e-8) + 0.1 * w
    return (w - 0.02 * step).astype(jnp.bfloat16), m, v


def clipped(gradients, sum_of_squares, count):
    factor = jnp.minimum(1.0, 0.5 * lax.rsqrt(sum_of_squares / count + 1e-30))
    return [g * factor for g in gradients]


def stack(weights, h):
    return lax.scan(lambda h, w: (layer(h, w), None), h, weights)[0]


def reference(x, dy, w_gate, w_up, w_down, m_w_gate, m_w_up, m_w_down, v_w_gate, v_w_up, v_w_down):
    weights = dict(zip(NAMES, (w_gate, w_up, w_down), strict=True))

    def take(so_far, sequence):
        h, by_y = sequence
        _, back = jax.vjp(lambda w: stack(w, h), weights)
        return jax.tree.map(lambda total, term: total + term.astype(jnp.float32), so_far, back(by_y)[0]), None

    none_yet = {name: jnp.zeros(w.shape, jnp.float32) for name, w in weights.items()}
    by_weights, _ = lax.scan(take, none_yet, (x, dy))
    gradients = [by_weights[name].astype(jnp.bfloat16).astype(jnp.float32) for name in NAMES]
    gradients = clipped(gradients, sum(jnp.sum(g * g) for g in gradients), sum(g.size for g in gradients))
    new = [
        adamw(w.astype(jnp.float32), m, v, g)
        for w, m, v, g in zip((w_gate, w_up, w_down), (m_w_gate, m_w_up, m_w_down), (v_w_gate, v_w_up, v_w_down), gradients, strict=True)
    ]
    return tuple(one[which] for which in range(3) for one in new)
```

```python
import functools
import heapq
import jax
import jax.numpy as jnp
from jax import lax
from jax.experimental import pallas as pl
from jax.experimental.pallas import tpu as pltpu

F32, BF16 = jnp.float32, jnp.bfloat16
MESH = pl.DeviceIdType.MESH
RATE, LATENCY = 46.6e3, 2.3
TURN, ADD, HOP = 0.1, 2.0e6, 0.7
WAYS = (1, -1)
RING, CROSS, DIRECT = range(3)


class Torus:
    def __init__(self, nx, ny, nz):
        self.n = {"x": nx, "y": ny, "z": nz}
        self.size = nx * ny * nz

    def me(self):
        p = lax.axis_index("dp")
        ny, nz = self.n["y"], self.n["z"]
        return {"z": lax.rem(p, nz), "y": lax.rem(lax.div(p, nz), ny), "x": lax.div(p, ny * nz)}

    def peer(self, me, dim, delta):
        at = dict(me)
        at[dim] = lax.rem(me[dim] + delta + self.n[dim], self.n[dim])
        return {"dp": (at["x"] * self.n["y"] + at["y"]) * self.n["z"] + at["z"]}


ORDERS = ("zxy", "xyz", "yxz")


def hops(n, flip):
    far, near = n // 2, n - 1 - n // 2
    return {1: near, -1: far} if flip else {1: far, -1: near}


class Balance:
    def __init__(self):
        self.load = {}

    def flip(self, dim, n, size):
        plain = [self.load.get((dim, s), 0) + size * hops(n, False)[s] for s in WAYS]
        turned = [self.load.get((dim, s), 0) + size * hops(n, True)[s] for s in WAYS]
        flip = max(turned) < max(plain)
        self.load[dim, 1], self.load[dim, -1] = turned if flip else plain
        return flip


def wrap(value, n):
    return lax.rem(value + 2 * n, n)


def simulate(actions, copies):
    links, arrived, order = {}, {}, []
    waiting = {a: set(needs) for a, (needs, _, _, _) in actions.items()}
    by_need = {}
    for a, (needs, _, _, _) in actions.items():
        for c in needs:
            by_need.setdefault(c, []).append(a)
    ready = [(actions[a][3], i, a) for i, a in enumerate(actions) if not waiting[a]]
    rank = {a: i for i, a in enumerate(actions)}
    heapq.heapify(ready)
    now, done = 0.0, {}
    while ready:
        at, _, a = heapq.heappop(ready)
        now = max(now, at) + actions[a][2]
        order.append(a)
        done[a] = now
        for c in [("action", a)] + list(actions[a][1]):
            if c[0] == "action":
                end = now
            else:
                link, size, extra = copies[c]
                start = max(now, links.get(link, 0.0))
                links[link] = start + size / RATE
                end = links[link] + LATENCY + extra
            for b in by_need.get(c, ()):
                waiting[b].discard(c)
                arrived[b] = max(arrived.get(b, 0.0), end)
                if not waiting[b]:
                    heapq.heappush(ready, (max(arrived[b], actions[b][3]), rank[b], b))
    assert len(order) == len(actions), (len(order), len(actions))
    return order, now


def barrier(torus, me, peers):
    sem = pltpu.get_barrier_semaphore()
    for dim, delta in peers:
        pl.semaphore_signal(sem, inc=1, device_id=torus.peer(me, dim, delta), device_id_type=MESH)
    pl.semaphore_wait(sem, len(peers))


def both_ways(torus, dim):
    n = torus.n[dim]
    return [] if n == 1 else [(dim, 1)] if n == 2 else [(dim, 1), (dim, -1)]


def all_others(torus, dim):
    return [(dim, d) for d in range(1, torus.n[dim])]


class ReduceScatter:
    def __init__(self, torus, rows, units):
        self.t, self.rows, self.units = torus, rows, units
        self.dims = [tuple(order) for order in ORDERS]
        self.nslots = sum(torus.n.values()) - 3

    def sizes(self, c):
        return [self.t.n[d] for d in self.dims[c]]

    def here(self, c):
        return [self.me[d] for d in self.dims[c]]

    def peers(self):
        full = {dims[DIRECT] for dims in self.dims}
        out = []
        for dim in "xyz":
            out += all_others(self.t, dim) if dim in full else both_ways(self.t, dim)
        return out

    def credit_peers(self, c):
        a, b, d = self.dims[c]
        return both_ways(self.t, a) + both_ways(self.t, b) + all_others(self.t, d)

    def scratch(self):
        n = self.t.n
        t, r1, r2, r3, k2, k3 = [], [], [], [], [], []
        for dims in self.dims:
            n1, n2, n3 = (n[d] for d in dims)
            tail = (self.rows, 128)
            t.append(pltpu.VMEM((self.units, n1, n2 * n3) + tail, BF16))
            r1.append(pltpu.VMEM((self.units, max(n1 - 1, 1), n2 * n3) + tail, BF16))
            r2.append(pltpu.VMEM((self.units, max(n2 - 1, 1), n3) + tail, BF16))
            r3.append(pltpu.VMEM((self.units, max(n3 - 1, 1)) + tail, BF16))
            k2.append(pltpu.VMEM((self.units, n3) + tail, F32))
            k3.append(pltpu.VMEM((self.units,) + tail, F32))
        sems = [pltpu.SemaphoreType.DMA((self.units, 3, self.nslots)), pltpu.SemaphoreType.DMA((self.units, 3, self.nslots)), pltpu.SemaphoreType.REGULAR((self.units, 3))]
        return [t, r1, r2, r3, k2, k3] + sems

    def slots(self, c, phase, flip):
        n = self.t.n[self.dims[c][phase]]
        k = hops(n, flip[phase])
        out, s = {}, 0
        for sign in WAYS:
            for h in range(k[sign]):
                out[sign, h] = s
                s += 1
        return out

    def base(self, c, phase):
        return sum(self.t.n[d] - 1 for d in self.dims[c][:phase])

    def flips(self, balance, c):
        n1, n2, n3 = self.sizes(c)
        block, (a, b, _) = self.rows * 256, self.dims[c]
        return balance.flip(a, n1, block * n2 * n3), balance.flip(b, n2, block * n3)

    def plan(self, unit, c, flip):
        n = self.sizes(c)
        n1, n2, n3 = n
        block = self.rows * 256
        size = [block * n2 * n3, block * n3, block]
        actions, copies = {}, {}
        key = (unit, c)

        def send(phase, sign, h):
            cid = ("copy", key, phase, sign, h)
            copies[cid] = ((self.dims[c][phase], sign), size[phase], 0)
            return cid

        first, last = [], []
        for phase in (RING, CROSS):
            k = hops(n[phase], flip[phase])
            first.append([send(phase, s, k[s] - 1) for s in WAYS if k[s]])
            last.append([("copy", key, phase, s, 0) for s in WAYS if k[s]])
            for s in WAYS:
                for h in range(k[s] - 1, 0, -1):
                    actions[key, "step", phase, s, h] = ([("copy", key, phase, s, h)], [send(phase, s, h - 1)], size[phase] / ADD)
        direct = []
        for rel in range(1, n3):
            cid = ("copy", key, DIRECT, 0, rel)
            far = min(rel, n3 - rel)
            copies[cid] = ((self.dims[c][DIRECT], 1 if rel <= n3 // 2 else -1), size[DIRECT] * far, HOP * (far - 1))
            direct.append(cid)
        sends = first + [direct, []]
        actions[key, "start"] = ([], sends[RING], TURN)
        before = (key, "start")
        for phase, needs in enumerate(last + [direct]):
            a = (key, "end", phase)
            actions[a] = (needs + [("action", before)], sends[phase + 1], size[phase] / ADD + TURN)
            before = a
        return actions, copies

    def bind(self, me, refs):
        self.me, (self.T, self.R1, self.R2, self.R3, self.K2, self.K3, self.ssem, self.rsem, self.credit) = me, refs
        return self

    def remote(self, u, c, flip, phase, sign, h):
        n1, n2, n3 = self.sizes(c)
        m1, m2, m3 = self.here(c)
        mine = self.T[c].at[u]
        if phase == RING:
            slot = self.slots(c, phase, flip)[sign, h]
            src, dst = mine.at[wrap(m1 + sign * (h + 1), n1)], self.R1[c].at[u, slot]
        elif phase == CROSS:
            slot = self.slots(c, phase, flip)[sign, h]
            src, dst = mine.at[m1, pl.ds(wrap(m2 + sign * (h + 1), n2) * n3, n3)], self.R2[c].at[u, slot]
        else:
            slot, sign = h - 1, h
            src, dst = mine.at[m1, m2 * n3 + wrap(m3 + h, n3)], self.R3[c].at[u, slot]
        s = self.base(c, phase) + slot
        to = self.t.peer(self.me, self.dims[c][phase], sign)
        return pltpu.make_async_remote_copy(src_ref=src, dst_ref=dst, send_sem=self.ssem.at[u, c, s], recv_sem=self.rsem.at[u, c, s], device_id=to, device_id_type=MESH)

    def all_sends(self, c, flip):
        n = self.sizes(c)
        out = []
        for phase in (RING, CROSS):
            k = hops(n[phase], flip[phase])
            out += [(phase, s, h) for s in WAYS for h in range(k[s])]
        return out + [(DIRECT, 0, rel) for rel in range(1, n[DIRECT])]

    def run(self, u, c, flip, what, store):
        n = self.sizes(c)
        n1, n2, n3 = n
        m1, m2, m3 = self.here(c)
        T, R1, R2, R3 = (r[c].at[u] for r in (self.T, self.R1, self.R2, self.R3))
        K2, K3 = self.K2[c].at[u], self.K3[c].at[u]
        mine = T.at[m1]
        wide = lambda v: v.astype(F32)
        go = lambda *a: self.remote(u, c, flip, *a)

        def loop(count, body):
            def one(i, carry):
                body(i)
                return carry

            lax.fori_loop(0, count, one, 0, unroll=2 - count % 2)

        def sends(phase):
            k = hops(n[phase], flip[phase])
            for s in WAYS:
                if k[s]:
                    go(phase, s, k[s] - 1).start()

        def arrived(phase):
            slots = self.slots(c, phase, flip)
            ways = [s for s in WAYS if (s, 0) in slots]
            for s in ways:
                go(phase, s, 0).wait_recv()
            return [slots[s, 0] for s in ways]

        kind, *where = what
        if kind == "start":
            sends(RING)
        elif kind == "step":
            phase, s, h = where
            go(phase, s, h).wait_recv()
            slot = self.slots(c, phase, flip)[s, h]
            q = wrap(self.here(c)[phase] + s * h, n[phase])

            def ring(i):
                T[q, i] = (wide(T[q, i]) + wide(R1[slot, i])).astype(BF16)

            def cross(i):
                b = q * n3 + i
                mine[b] = (wide(mine[b]) + wide(R2[slot, i])).astype(BF16)

            loop(n2 * n3 if phase == RING else n3, cross if phase else ring)
            go(phase, s, h - 1).start()
        elif where == [RING]:
            got = arrived(RING)

            def total(b):
                return sum((wide(R1[g, b]) for g in got), wide(mine[b]))

            def own(i):
                K2[i] = total(m2 * n3 + i)

            def others(i):
                b = lax.rem((m2 + 1) * n3 + i, n2 * n3)
                mine[b] = total(b).astype(BF16)

            loop((n2 - 1) * n3, others)
            sends(CROSS)
            loop(n3, own)
        elif where == [CROSS]:
            got = arrived(CROSS)

            def total(q):
                return sum((wide(R2[g, q]) for g in got), K2[q])

            for rel in range(1, n3):
                q = wrap(m3 + rel, n3)
                mine[m2 * n3 + q] = total(q).astype(BF16)
            for rel in range(1, n3):
                go(DIRECT, 0, rel).start()
            K3[...] = total(m3)
        else:
            for rel in range(1, n3):
                go(DIRECT, 0, rel).wait_recv()
            store(sum((wide(R3[i]) for i in range(n3 - 1)), K3[...]).astype(BF16).astype(F32))

    def wait_sends(self, u, c, flip):
        for a in self.all_sends(c, flip):
            self.remote(u, c, flip, *a).wait_send()

    def give_credit(self, u, c):
        for dim, delta in self.credit_peers(c):
            pl.semaphore_signal(self.credit.at[u, c], inc=1, device_id=self.t.peer(self.me, dim, delta), device_id_type=MESH)

    def take_credit(self, u, c):
        pl.semaphore_wait(self.credit.at[u, c], len(self.credit_peers(c)))


def reduce_scatter(torus, terms, rows, collective_id):
    layers, units = len(terms), len(terms[0])
    rs = ReduceScatter(torus, rows, units)
    actions, copies, balance, flips = {}, {}, Balance(), {}
    for l in range(layers):
        for u in range(units):
            for c in range(3):
                flips[l, u, c] = rs.flips(balance, c)
                got, sent = rs.plan((l, u), c, flips[l, u, c])
                copies |= sent
                for a, (needs, sends, cost) in got.items():
                    if l and a[1] == "start":
                        actions[a[0], "load"] = ([("action", (((l - 1, u), c), "end", 2))], [], TURN, 0)
                        needs = needs + [("action", (a[0], "load"))]
                    actions[a] = (needs, sends, cost, 0)
    order, took = simulate(actions, copies)
    flat = [t for layer in terms for unit in layer for t in unit]

    def kernel(*refs):
        ins, out, scratch, lsem = refs[: len(flat)], refs[len(flat)], refs[len(flat) + 1 : -1], refs[-1]
        me = torus.me()
        it = rs.bind(me, scratch)
        barrier(torus, me, rs.peers())

        def load(l, u, c):
            return pltpu.make_async_copy(ins[(l * units + u) * 3 + c], it.T[c].at[u], lsem.at[u, c])

        for u in range(units):
            for c in range(3):
                load(0, u, c).start()
        for a in order:
            ((l, u), c), what = a[0], a[1:]
            flip = flips[l, u, c]
            if what[0] == "load":
                it.wait_sends(u, c, flips[l - 1, u, c])
                it.give_credit(u, c)
                load(l, u, c).start()
                continue
            if what[0] == "start":
                load(l, u, c).wait()
                if l:
                    it.take_credit(u, c)

            def store(value):
                out[l, u, c] = value

            it.run(u, c, flip, what, store)
        for u in range(units):
            for c in range(3):
                it.wait_sends(u, c, flips[layers - 1, u, c])

    return pl.pallas_call(
        kernel,
        out_shape=jax.ShapeDtypeStruct((layers, units, 3, rows, 128), F32),
        in_specs=[pl.BlockSpec(memory_space=pl.ANY)] * len(flat),
        out_specs=pl.BlockSpec(memory_space=pltpu.VMEM),
        scratch_shapes=rs.scratch() + [pltpu.SemaphoreType.DMA((units, 3))],
        compiler_params=pltpu.CompilerParams(collective_id=collective_id, has_side_effects=True, vmem_limit_bytes=56 * 2**20),
        name="reduce_scatter",
    )(*flat)


class AllGather:
    def __init__(self, torus, block_bytes, split=2):
        self.t, self.bytes, self.split = torus, block_bytes, split
        self.dims = [tuple(order) for order in ORDERS]
        self.copies, self.actions, self.index, self.flip = {}, {}, {}, {}
        self.balance = Balance()
        for c in range(3):
            self.plan(c)
        self.order, self.took = simulate({a: (*v, 0) for a, v in self.actions.items()}, self.copies)

    def peers(self):
        return [p for dim in "xyz" for p in both_ways(self.t, dim)]

    def pieces(self, c, j):
        n3 = self.t.n[self.dims[c][DIRECT]]
        return n3 if not j else self.split if n3 % self.split == 0 else 1

    def size(self, c, phase, j):
        line = self.bytes * self.t.n[self.dims[c][DIRECT]]
        return self.bytes if phase == DIRECT else line if phase == CROSS else line // self.pieces(c, j)

    def k(self, c, phase, j, i):
        dim = self.dims[c][phase]
        key = (c, phase, j, i)
        if key not in self.flip:
            self.flip[key] = self.balance.flip(dim, self.t.n[dim], self.size(c, phase, j))
        return hops(self.t.n[dim], self.flip[key])

    def plan(self, c):
        n1, n2, n3 = (self.t.n[d] for d in self.dims[c])

        def send(where, s, h):
            phase, j, _ = where
            cid = (c, where, s, h)
            self.copies[cid] = ((self.dims[c][phase], s), self.size(c, phase, j), 0)
            self.index[cid] = len(self.index)
            return cid

        def own(*where):
            k = self.k(c, *where)
            return [send(where, s, 1) for s in WAYS if k[s]]

        def line(j):
            return [x for i in range(self.pieces(c, j)) for x in own(RING, j, i)]

        def passing(*where):
            k = self.k(c, *where)
            for s in WAYS:
                for h in range(1, k[s] + 1):
                    yield s, h, (c, "pass", where, s, h), [(c, where, s, h)], [send(where, s, h + 1)] if h < k[s] else []

        def act(a, needs, sends):
            self.actions[a] = (needs, sends, TURN / 2)

        act((c, "start"), [], own(DIRECT, 0, 0) + own(RING, 0, 0))
        got = [("action", (c, "start"))]
        for s, h, a, needs, sends in passing(DIRECT, 0, 0):
            act(a, needs, sends + own(RING, 0, (-s * h) % n3))
            got.append(("action", a))
        act((c, "line"), got, own(CROSS, 0, 0))
        for s, h, a, needs, sends in passing(CROSS, 0, 0):
            act(a, needs, sends + line((-s * h) % n2))
        for j in range(n2):
            for i in range(self.pieces(c, j)):
                for _, _, a, needs, sends in passing(RING, j, i):
                    act(a, needs, sends)

    def bind(self, me, G, ssem, rsem):
        self.me, self.G, self.ssem, self.rsem = me, G, ssem, rsem
        return self

    def remote(self, cid, back):
        c, (phase, j, i), s, h = cid
        a, b, d = self.dims[c]
        n1, n2, n3 = (self.t.n[x] for x in (a, b, d))
        m1, m2, m3 = (self.me[x] for x in (a, b, d))
        off = s * (back - h)
        G = self.G[c]
        if phase == DIRECT:
            ref = G.at[m1, m2 * n3 + wrap(m3 + off, n3)]
        elif phase == CROSS:
            ref = G.at[m1, pl.ds(wrap(m2 + off, n2) * n3, n3)]
        elif j == 0:
            ref = G.at[wrap(m1 + off, n1), m2 * n3 + wrap(m3 + i, n3)]
        else:
            size = n3 // self.pieces(c, j)
            ref = G.at[wrap(m1 + off, n1), pl.ds(wrap(m2 + j, n2) * n3 + i * size, size)]
        x = self.index[cid]
        return pltpu.make_async_remote_copy(src_ref=ref, dst_ref=ref, send_sem=self.ssem.at[x], recv_sem=self.rsem.at[x], device_id=self.t.peer(self.me, self.dims[c][phase], s), device_id_type=MESH)

    def run(self, a):
        needs, sends, _ = self.actions[a]
        for cid in needs:
            if cid in self.index:
                self.remote(cid, 0).wait_recv()
        for cid in sends:
            self.remote(cid, 1).start()

    def wait_sends(self):
        for cid in self.copies:
            self.remote(cid, 1).wait_send()


MIB = 2**20
LAYERS, D, FF = 2, 896, 2560
LANES, ROWS, CHUNK = 128, 144, 48
HIGH = {0: 7, 1: 7, 2: 20}
WIDE = {0: FF, 1: FF, 2: D}


def tiles(u):
    high, wide = HIGH[u], WIDE[u] // LANES
    out = []
    for k in range(ROWS // 8):
        ct, row = divmod(8 * k, high)
        out.append((ct, row, min(8, high - row), ct + 1 < wide))
    return out


def owner_index(torus, c, i):
    ny, nz = torus.n["y"], torus.n["z"]
    at = {"z": lax.rem(i, nz), "y": lax.rem(lax.div(i, nz), ny), "x": lax.div(i, ny * nz)}
    n = torus.n
    a, b, d = ORDERS[c]
    return at[a], at[b] * n[d] + at[d]


def pack(torus, u, X, outs):
    high = HIGH[u]
    sub = lax.broadcasted_iota(jnp.int32, (8, LANES), 0)

    def piece(i, ct, row, count, more):
        start = high * i + row + 8
        a = X[ct, pl.ds(start, 8), :]
        if count == 8:
            return a
        b = X[ct + 1, pl.ds(start - row - count, 8), :] if more else jnp.zeros((8, LANES), F32)
        return jnp.where(sub < count, a, b)

    got = tiles(u)

    def body(i, carry):
        at = [owner_index(torus, c, i) for c in range(3)]
        for j in range(ROWS // 16):
            both = jnp.concatenate([piece(i, *got[2 * j]), piece(i, *got[2 * j + 1])], axis=0).astype(BF16)
            c, r = divmod(16 * j, CHUNK)
            outs[c][at[c][0], at[c][1], pl.ds(r, 16), :] = both
        return carry

    lax.fori_loop(0, torus.size, body, 0, unroll=4)


def pieces_shapes(torus, dtype, *mid):
    out = []
    for order in ORDERS:
        a, b, d = (torus.n[x] for x in order)
        out.append(jax.ShapeDtypeStruct((a, b * d) + mid + (CHUNK, LANES), dtype))
    return out


def weight_terms(torus, u, a, b):
    tokens = a.shape[0]
    rows, cols = a.shape[1], b.shape[1]
    step = 256
    by_rows = u == 2
    steps = (rows if by_rows else cols) // step

    def kernel(a_ref, b_ref, o0, o1, o2, X):
        s = pl.program_id(0)
        got = lax.dot_general(a_ref[...], b_ref[...], (((0,), (0,)), ((), ())), preferred_element_type=F32)
        if by_rows:
            for ct in range(cols // LANES):
                X[ct, pl.ds(pl.multiple_of(s * step, step) + 8, step), :] = got[:, ct * LANES : (ct + 1) * LANES]
        else:
            for k in range(step // LANES):
                X[s * (step // LANES) + k, pl.ds(8, rows), :] = got[:, k * LANES : (k + 1) * LANES]

        @pl.when(s == steps - 1)
        def _():
            pack(torus, u, X, (o0, o1, o2))

    a_spec = pl.BlockSpec((tokens, step), lambda s: (0, s)) if by_rows else pl.BlockSpec((tokens, rows), lambda s: (0, 0))
    b_spec = pl.BlockSpec((tokens, cols), lambda s: (0, 0)) if by_rows else pl.BlockSpec((tokens, step), lambda s: (0, s))
    shapes = pieces_shapes(torus, BF16)
    return pl.pallas_call(
        kernel,
        grid=(steps,),
        out_shape=shapes,
        in_specs=[a_spec, b_spec],
        out_specs=[pl.BlockSpec(s.shape, lambda i: (0, 0, 0, 0)) for s in shapes],
        scratch_shapes=[pltpu.VMEM((cols // LANES, rows + 24, LANES), F32)],
        compiler_params=pltpu.CompilerParams(vmem_limit_bytes=56 * MIB),
        cost_estimate=pl.CostEstimate(flops=2 * tokens * rows * cols, bytes_accessed=2 * (tokens * (rows + cols) + rows * cols), transcendentals=0),
        name=f"terms_{u}",
    )(a, b)


def step_and_gather(torus, g, w, m, v, count, collective_id):
    ag = AllGather(torus, LAYERS * 3 * CHUNK * 256)
    dims = "zxy"
    slots = {d: torus.n[d] - 1 for d in dims}

    def kernel(g_ref, *refs):
        w_in, m_in, v_in, G, m_out, v_out = (refs[i : i + 3] for i in range(0, 18, 3))
        flat, wflat, part, E, esend, erecv, ssem, rsem = refs[18:]
        me = torus.me()
        barrier(torus, me, [p for d in "xyz" for p in all_others(torus, d)])
        acc = jnp.zeros((8, LANES), F32)
        for l in range(LAYERS):
            for u in range(3):
                for c in range(3):
                    value = g_ref[l, u, c]
                    flat[l, u, pl.ds(c * CHUNK, CHUNK), :] = value
                    for r in range(0, CHUNK, 8):
                        acc = acc + value[r : r + 8] * value[r : r + 8]
        part[0] = acc
        base = 0
        for i, d in enumerate(dims):
            n = torus.n[d]
            copies = []
            for rel in range(1, n):
                s = base + rel - 1
                copies.append(pltpu.make_async_remote_copy(src_ref=part.at[i], dst_ref=E.at[s], send_sem=esend.at[s], recv_sem=erecv.at[s], device_id=torus.peer(me, d, rel), device_id_type=MESH))
            for copy in copies:
                copy.start()
            total = part[i]
            for rel in range(1, n):
                copies[rel - 1].wait_recv()
                total = total + E[base + rel - 1]
            part[i + 1] = total
            for copy in copies:
                copy.wait_send()
            base += n - 1
        mean = jnp.sum(part[3], keepdims=True) / count
        factor = jnp.minimum(1.0, 0.5 * lax.rsqrt(mean + 1e-30))
        for l in range(LAYERS):
            for u in range(3):
                high = HIGH[u]
                wflat[l, u, pl.ds(ROWS - 8, 8), :] = jnp.zeros((8, LANES), F32)
                for ct in range(WIDE[u] // LANES):
                    at = (l, slice(None), pl.ds(ct * LANES, LANES))
                    grad = flat[l, u, pl.ds(ct * high, high), :] * factor
                    new_m = 0.9 * m_in[u][at] + 0.1 * grad
                    new_v = 0.95 * v_in[u][at] + 0.05 * grad * grad
                    wide = w_in[u][at]
                    new_w = wide - 0.02 * (new_m * lax.rsqrt(new_v + 1e-8) + 0.1 * wide)
                    m_out[u][at] = new_m
                    v_out[u][at] = new_v
                    wflat[l, u, pl.ds(ct * high, high), :] = new_w
        it = ag.bind(me, G, ssem, rsem)
        for c in range(3):
            n = [torus.n[d] for d in ORDERS[c]]
            at = [me[d] for d in ORDERS[c]]
            for l in range(LAYERS):
                for u in range(3):
                    G[c][at[0], at[1] * n[2] + at[2], l, u] = wflat[l, u, pl.ds(c * CHUNK, CHUNK), :].astype(BF16)
        for a in ag.order:
            it.run(a)
        it.wait_sends()

    vmem = pl.BlockSpec(memory_space=pltpu.VMEM)
    nsum = sum(slots.values())
    shapes = pieces_shapes(torus, BF16, LAYERS, 3)
    f32 = [jax.ShapeDtypeStruct(t.shape, F32) for t in m]
    k = len(ag.copies)
    got = pl.pallas_call(
        kernel,
        out_shape=[pltpu.MemorySpace.VMEM(s.shape, s.dtype) for s in shapes] + f32 * 2,
        in_specs=[vmem] * 10,
        out_specs=[vmem] * 9,
        scratch_shapes=[
            pltpu.VMEM((LAYERS, 3, ROWS, LANES), F32),
            pltpu.VMEM((LAYERS, 3, ROWS, LANES), F32),
            pltpu.VMEM((4, 8, LANES), F32),
            pltpu.VMEM((nsum, 8, LANES), F32),
            pltpu.SemaphoreType.DMA((nsum,)),
            pltpu.SemaphoreType.DMA((nsum,)),
            pltpu.SemaphoreType.DMA((k,)),
            pltpu.SemaphoreType.DMA((k,)),
        ],
        compiler_params=pltpu.CompilerParams(collective_id=collective_id, has_side_effects=True, vmem_limit_bytes=10 * MIB),
        name="step_and_gather",
    )(g, *w, *m, *v)
    return got[:3], got[3:6], got[6:]


def unpack(torus, G):
    nx, ny, nz = (torus.n[d] for d in "xyz")
    pair = 2
    group = pair * nz
    groups = torus.size // group
    pairs = ny // pair

    def kernel(g0, g1, g2, *refs):
        outs, Z, Y = refs[:3], refs[3], refs[4]
        l, s = pl.program_id(0), pl.program_id(1)
        corner = {"x": lax.div(s, pairs), "y": lax.rem(s, pairs) * pair, "z": 0}
        for u in range(3):
            high, wide = HIGH[u], WIDE[u] // LANES
            for i in range(group):
                y, z = divmod(i, nz)
                at = corner | {"y": corner["y"] + y, "z": z}
                for c, ref in enumerate((g0, g1, g2)):
                    a, b, d = ORDERS[c]
                    Z[i, pl.ds(c * CHUNK, CHUNK), :] = ref[at[a], at[b] * torus.n[d] + at[d], l, u].astype(F32)
            for i in range(group):
                for ct in range(wide):
                    for r in range(0, high, 8):
                        Y[ct, pl.ds(high * i + r, 8), :] = Z[i, pl.ds(high * ct + r, 8), :]
            rows = high * group
            for ct in range(wide):
                outs[u][0, :, pl.ds(ct * LANES, LANES)] = Y[ct, pl.ds(0, rows), :].astype(BF16)

    shapes = [(LAYERS, HIGH[u] * torus.size, WIDE[u]) for u in range(3)]
    return pl.pallas_call(
        kernel,
        grid=(LAYERS, groups),
        out_shape=[jax.ShapeDtypeStruct(s, BF16) for s in shapes],
        in_specs=[pl.BlockSpec(memory_space=pltpu.VMEM)] * 3,
        out_specs=[pl.BlockSpec((1, HIGH[u] * group, WIDE[u]), lambda l, s: (l, s, 0)) for u in range(3)],
        scratch_shapes=[pltpu.VMEM((group, ROWS + 8, LANES), F32), pltpu.VMEM((FF // LANES, HIGH[2] * group + 8, LANES), F32)],
        compiler_params=pltpu.CompilerParams(vmem_limit_bytes=16 * MIB),
        name="unpack",
    )(*G)


def dot(a, b, dims):
    return lax.dot_general(a, b, (dims, ((), ())), preferred_element_type=F32)


def normed(h):
    wide = h.astype(F32)
    scale = lax.rsqrt(jnp.mean(wide**2, -1, keepdims=True) + 1e-6)
    return (wide * scale).astype(BF16), wide, scale


def hidden(a, gate_w, up_w):
    gate, up = dot(a, gate_w, ((1,), (0,))), dot(a, up_w, ((1,), (0,)))
    s = jax.nn.sigmoid(gate)
    act = gate * s
    return (act * up).astype(BF16), act, up, s * (1.0 + gate * (1.0 - s))


def hidden_back(d, act, up, slope):
    return (d * up * slope).astype(BF16), (d * act).astype(BF16)


def solution(mesh):
    torus = Torus(4, 4, 8)
    count = float(LAYERS * 3 * D * FF)

    def step(x, dy, wg, wu, wd, mg, mu, md, vg, vu, vd):
        x, dy = x[0], dy[0]
        a0, _, _ = normed(x)
        mid0, act0, up0, slope0 = hidden(a0, wg[0], wu[0])
        h1 = x + dot(mid0, wd[0], ((1,), (0,))).astype(BF16)
        a1, wide1, scale1 = normed(h1)
        mid1, act1, up1, slope1 = hidden(a1, wg[1], wu[1])
        dmid1 = dot(dy, wd[1], ((1,), (1,))).astype(BF16).astype(F32)
        dgate1, dup1 = hidden_back(dmid1, act1, up1, slope1)
        t1 = [weight_terms(torus, 0, a1, dgate1), weight_terms(torus, 1, a1, dup1), weight_terms(torus, 2, mid1, dy)]
        da = (dot(dgate1, wg[1], ((1,), (1,))) + dot(dup1, wu[1], ((1,), (1,)))).astype(BF16).astype(F32)
        inner = jnp.mean(da * wide1, -1, keepdims=True)
        dh = dy + (scale1 * da - wide1 * (scale1 * scale1 * scale1 * inner)).astype(BF16)
        dmid0 = dot(dh, wd[0], ((1,), (1,))).astype(BF16).astype(F32)
        dgate0, dup0 = hidden_back(dmid0, act0, up0, slope0)
        t0 = [weight_terms(torus, 0, a0, dgate0), weight_terms(torus, 1, a0, dup0), weight_terms(torus, 2, mid0, dh)]
        g = reduce_scatter(torus, [t1, t0], CHUNK, 1)[::-1]
        p = lax.axis_index("dp")
        mine = [lax.dynamic_slice_in_dim(w, p * HIGH[u], HIGH[u], 1).astype(F32) for u, w in enumerate((wg, wu, wd))]
        G, m, v = step_and_gather(torus, g, mine, (mg, mu, md), (vg, vu, vd), count, 2)
        return (*unpack(torus, G), *m, *v)

    P = jax.sharding.PartitionSpec
    return jax.shard_map(
        step,
        mesh=mesh,
        in_specs=(P(("rep", "dp")),) * 2 + (P(),) * 3 + (P(None, "dp"),) * 6,
        out_specs=(P("rep"),) * 3 + (P("rep", "dp"),) * 6,
        check_vma=False,
    )
```

```python
import heapq
import jax
import jax.numpy as jnp
from jax import lax
from jax.experimental import pallas as pl
from jax.experimental.pallas import tpu as pltpu

F32, BF16 = jnp.float32, jnp.bfloat16
MESH = pl.DeviceIdType.MESH
RATE, LATENCY = 46.6e3, 2.3
TURN, ADD, HOP = 0.1, 2.0e6, 0.7
WAYS = (1, -1)
RING, CROSS, DIRECT = range(3)
PACKING, MARGIN = 2.5, 1.0


class Torus:
    def __init__(self, nx, ny, nz):
        self.n = {"x": nx, "y": ny, "z": nz}
        self.size = nx * ny * nz

    def me(self):
        p = lax.axis_index("dp")
        ny, nz = self.n["y"], self.n["z"]
        return {"z": lax.rem(p, nz), "y": lax.rem(lax.div(p, nz), ny), "x": lax.div(p, ny * nz)}

    def peer(self, me, dim, delta):
        at = dict(me)
        at[dim] = lax.rem(me[dim] + delta + self.n[dim], self.n[dim])
        return {"dp": (at["x"] * self.n["y"] + at["y"]) * self.n["z"] + at["z"]}


ORDERS = ("zxy", "xyz", "yxz")


def hops(n, flip):
    far, near = n // 2, n - 1 - n // 2
    return {1: near, -1: far} if flip else {1: far, -1: near}


class Balance:
    def __init__(self):
        self.load = {}

    def flip(self, dim, n, size):
        plain = [self.load.get((dim, s), 0) + size * hops(n, False)[s] for s in WAYS]
        turned = [self.load.get((dim, s), 0) + size * hops(n, True)[s] for s in WAYS]
        flip = max(turned) < max(plain)
        self.load[dim, 1], self.load[dim, -1] = turned if flip else plain
        return flip


def wrap(value, n):
    return lax.rem(value + 2 * n, n)


def simulate(actions, copies):
    links, arrived, order = {}, {}, []
    waiting = {a: set(needs) for a, (needs, _, _, _) in actions.items()}
    by_need = {}
    for a, (needs, _, _, _) in actions.items():
        for c in needs:
            by_need.setdefault(c, []).append(a)
    ready = [(actions[a][3], i, a) for i, a in enumerate(actions) if not waiting[a]]
    rank = {a: i for i, a in enumerate(actions)}
    heapq.heapify(ready)
    now, done = 0.0, {}
    while ready:
        at, _, a = heapq.heappop(ready)
        now = max(now, at) + actions[a][2]
        order.append(a)
        done[a] = now
        for c in [("action", a)] + list(actions[a][1]):
            if c[0] == "action":
                end = now
            else:
                link, size, extra = copies[c]
                start = max(now, links.get(link, 0.0))
                links[link] = start + size / RATE
                end = links[link] + LATENCY + extra
            for b in by_need.get(c, ()):
                waiting[b].discard(c)
                arrived[b] = max(arrived.get(b, 0.0), end)
                if not waiting[b]:
                    heapq.heappush(ready, (max(arrived[b], actions[b][3]), rank[b], b))
    assert len(order) == len(actions), (len(order), len(actions))
    return order, now


def place(actions, copies, stages):
    links, known, done = {}, {}, set()
    now, left = 0.0, dict(actions)
    slots = {}

    def ready(a, at):
        needs, _, _ = actions[a]
        return all(c in known and known[c] <= at for c in needs)

    def do(a, where):
        nonlocal now
        _, sends, cost = actions[a]
        now += cost
        known["action", a] = now
        for c in sends:
            link, size, extra = copies[c]
            links[link] = max(now, links.get(link, 0.0)) + size / RATE
            known[c] = links[link] + LATENCY + extra + MARGIN
        del left[a]
        slots.setdefault(where, []).append(a)

    def drain(where, allowed, wait):
        nonlocal now
        while True:
            able = [a for a in left if allowed(a)]
            best = min((max([known.get(c, 1e9) for c in actions[a][0]], default=0.0) for a in able), default=1e9)
            if best > (1e8 if wait else now):
                return
            now = max(now, best)
            for a in able:
                if ready(a, now):
                    do(a, where)
                    break

    packed = set()
    usual = lambda a: a[1] != "start" or a[0][0] in packed
    for number, cost, count, unit in stages:
        for t in range(count):
            now += cost
            slots[number, t] = []
            drain((number, t), usual, False)
        slots[number, "before"], slots[number, "after"] = [], []
        if unit:
            other = [a for a in left if a[0][0][1] == unit[1] and a[0][0][0] > unit[0]]
            if other:
                drain((number, "before"), lambda a: a in other, True)
            now += PACKING
            packed.add(unit)
            drain((number, "after"), usual, False)
    drain((stages[-1][0], "after"), lambda a: True, True)
    assert not left, left
    place.took = now
    return slots


def barrier(torus, me, peers):
    sem = pltpu.get_barrier_semaphore()
    for dim, delta in peers:
        pl.semaphore_signal(sem, inc=1, device_id=torus.peer(me, dim, delta), device_id_type=MESH)
    pl.semaphore_wait(sem, len(peers))


def both_ways(torus, dim):
    n = torus.n[dim]
    return [] if n == 1 else [(dim, 1)] if n == 2 else [(dim, 1), (dim, -1)]


def all_others(torus, dim):
    return [(dim, d) for d in range(1, torus.n[dim])]


class ReduceScatter:
    def __init__(self, torus, rows, units):
        self.t, self.rows, self.units = torus, rows, units
        self.dims = [tuple(order) for order in ORDERS]
        self.nslots = sum(torus.n.values()) - 3

    def sizes(self, c):
        return [self.t.n[d] for d in self.dims[c]]

    def here(self, c):
        return [self.me[d] for d in self.dims[c]]

    def peers(self):
        full = {dims[DIRECT] for dims in self.dims}
        out = []
        for dim in "xyz":
            out += all_others(self.t, dim) if dim in full else both_ways(self.t, dim)
        return out

    def credit_peers(self, c):
        a, b, d = self.dims[c]
        return both_ways(self.t, a) + both_ways(self.t, b) + all_others(self.t, d)

    def scratch(self):
        n = self.t.n
        t, r1, r2, r3, k2, k3 = [], [], [], [], [], []
        for dims in self.dims:
            n1, n2, n3 = (n[d] for d in dims)
            tail = (self.rows, 128)
            t.append(pltpu.VMEM((self.units, n1, n2 * n3) + tail, BF16))
            r1.append(pltpu.VMEM((self.units, max(n1 - 1, 1), n2 * n3) + tail, BF16))
            r2.append(pltpu.VMEM((self.units, max(n2 - 1, 1), n3) + tail, BF16))
            r3.append(pltpu.VMEM((self.units, max(n3 - 1, 1)) + tail, BF16))
            k2.append(pltpu.VMEM((self.units, n3) + tail, F32))
            k3.append(pltpu.VMEM((self.units,) + tail, F32))
        sems = [pltpu.SemaphoreType.DMA((self.units, 3, self.nslots)), pltpu.SemaphoreType.DMA((self.units, 3, self.nslots)), pltpu.SemaphoreType.REGULAR((self.units, 3))]
        return [t, r1, r2, r3, k2, k3] + sems

    def slots(self, c, phase, flip):
        n = self.t.n[self.dims[c][phase]]
        k = hops(n, flip[phase])
        out, s = {}, 0
        for sign in WAYS:
            for h in range(k[sign]):
                out[sign, h] = s
                s += 1
        return out

    def base(self, c, phase):
        return sum(self.t.n[d] - 1 for d in self.dims[c][:phase])

    def flips(self, balance, c):
        n1, n2, n3 = self.sizes(c)
        block, (a, b, _) = self.rows * 256, self.dims[c]
        return balance.flip(a, n1, block * n2 * n3), balance.flip(b, n2, block * n3)

    def plan(self, unit, c, flip):
        n = self.sizes(c)
        n1, n2, n3 = n
        block = self.rows * 256
        size = [block * n2 * n3, block * n3, block]
        actions, copies = {}, {}
        key = (unit, c)

        def send(phase, sign, h):
            cid = ("copy", key, phase, sign, h)
            copies[cid] = ((self.dims[c][phase], sign), size[phase], 0)
            return cid

        first, last = [], []
        for phase in (RING, CROSS):
            k = hops(n[phase], flip[phase])
            first.append([send(phase, s, k[s] - 1) for s in WAYS if k[s]])
            last.append([("copy", key, phase, s, 0) for s in WAYS if k[s]])
            for s in WAYS:
                for h in range(k[s] - 1, 0, -1):
                    actions[key, "step", phase, s, h] = ([("copy", key, phase, s, h)], [send(phase, s, h - 1)], size[phase] / ADD)
        direct = []
        for rel in range(1, n3):
            cid = ("copy", key, DIRECT, 0, rel)
            far = min(rel, n3 - rel)
            copies[cid] = ((self.dims[c][DIRECT], 1 if rel <= n3 // 2 else -1), size[DIRECT] * far, HOP * (far - 1))
            direct.append(cid)
        sends = first + [direct, []]
        actions[key, "start"] = ([], sends[RING], TURN)
        before = (key, "start")
        for phase, needs in enumerate(last + [direct]):
            a = (key, "end", phase)
            actions[a] = (needs + [("action", before)], sends[phase + 1], size[phase] / ADD + TURN)
            before = a
        return actions, copies

    def bind(self, me, refs):
        self.me, (self.T, self.R1, self.R2, self.R3, self.K2, self.K3, self.ssem, self.rsem, self.credit) = me, refs
        return self

    def remote(self, u, c, flip, phase, sign, h):
        n1, n2, n3 = self.sizes(c)
        m1, m2, m3 = self.here(c)
        mine = self.T[c].at[u]
        if phase == RING:
            slot = self.slots(c, phase, flip)[sign, h]
            src, dst = mine.at[wrap(m1 + sign * (h + 1), n1)], self.R1[c].at[u, slot]
        elif phase == CROSS:
            slot = self.slots(c, phase, flip)[sign, h]
            src, dst = mine.at[m1, pl.ds(wrap(m2 + sign * (h + 1), n2) * n3, n3)], self.R2[c].at[u, slot]
        else:
            slot, sign = h - 1, h
            src, dst = mine.at[m1, m2 * n3 + wrap(m3 + h, n3)], self.R3[c].at[u, slot]
        s = self.base(c, phase) + slot
        to = self.t.peer(self.me, self.dims[c][phase], sign)
        return pltpu.make_async_remote_copy(src_ref=src, dst_ref=dst, send_sem=self.ssem.at[u, c, s], recv_sem=self.rsem.at[u, c, s], device_id=to, device_id_type=MESH)

    def all_sends(self, c, flip):
        n = self.sizes(c)
        out = []
        for phase in (RING, CROSS):
            k = hops(n[phase], flip[phase])
            out += [(phase, s, h) for s in WAYS for h in range(k[s])]
        return out + [(DIRECT, 0, rel) for rel in range(1, n[DIRECT])]

    def run(self, u, c, flip, what, store):
        n = self.sizes(c)
        n1, n2, n3 = n
        m1, m2, m3 = self.here(c)
        T, R1, R2, R3 = (r[c].at[u] for r in (self.T, self.R1, self.R2, self.R3))
        K2, K3 = self.K2[c].at[u], self.K3[c].at[u]
        mine = T.at[m1]
        wide = lambda v: v.astype(F32)
        go = lambda *a: self.remote(u, c, flip, *a)

        def loop(count, body):
            def one(i, carry):
                body(i)
                return carry

            lax.fori_loop(0, count, one, 0, unroll=2 - count % 2)

        def sends(phase):
            k = hops(n[phase], flip[phase])
            for s in WAYS:
                if k[s]:
                    go(phase, s, k[s] - 1).start()

        def arrived(phase):
            slots = self.slots(c, phase, flip)
            ways = [s for s in WAYS if (s, 0) in slots]
            for s in ways:
                go(phase, s, 0).wait_recv()
            return [slots[s, 0] for s in ways]

        kind, *where = what
        if kind == "start":
            sends(RING)
        elif kind == "step":
            phase, s, h = where
            go(phase, s, h).wait_recv()
            slot = self.slots(c, phase, flip)[s, h]
            q = wrap(self.here(c)[phase] + s * h, n[phase])

            def ring(i):
                T[q, i] = (wide(T[q, i]) + wide(R1[slot, i])).astype(BF16)

            def cross(i):
                b = q * n3 + i
                mine[b] = (wide(mine[b]) + wide(R2[slot, i])).astype(BF16)

            loop(n2 * n3 if phase == RING else n3, cross if phase else ring)
            go(phase, s, h - 1).start()
        elif where == [RING]:
            got = arrived(RING)

            def total(b):
                return sum((wide(R1[g, b]) for g in got), wide(mine[b]))

            def own(i):
                K2[i] = total(m2 * n3 + i)

            def others(i):
                b = lax.rem((m2 + 1) * n3 + i, n2 * n3)
                mine[b] = total(b).astype(BF16)

            loop((n2 - 1) * n3, others)
            sends(CROSS)
            loop(n3, own)
        elif where == [CROSS]:
            got = arrived(CROSS)

            def total(q):
                return sum((wide(R2[g, q]) for g in got), K2[q])

            for rel in range(1, n3):
                q = wrap(m3 + rel, n3)
                mine[m2 * n3 + q] = total(q).astype(BF16)
            for rel in range(1, n3):
                go(DIRECT, 0, rel).start()
            K3[...] = total(m3)
        else:
            for rel in range(1, n3):
                go(DIRECT, 0, rel).wait_recv()
            store(sum((wide(R3[i]) for i in range(n3 - 1)), K3[...]).astype(BF16).astype(F32))

    def wait_sends(self, u, c, flip):
        for a in self.all_sends(c, flip):
            self.remote(u, c, flip, *a).wait_send()

    def give_credit(self, u, c):
        for dim, delta in self.credit_peers(c):
            pl.semaphore_signal(self.credit.at[u, c], inc=1, device_id=self.t.peer(self.me, dim, delta), device_id_type=MESH)

    def take_credit(self, u, c):
        pl.semaphore_wait(self.credit.at[u, c], len(self.credit_peers(c)))


class AllGather:
    def __init__(self, torus, block_bytes, split=2):
        self.t, self.bytes, self.split = torus, block_bytes, split
        self.dims = [tuple(order) for order in ORDERS]
        self.copies, self.actions, self.index, self.flip = {}, {}, {}, {}
        self.balance = Balance()
        for c in range(3):
            self.plan(c)
        self.order, self.took = simulate({a: (*v, 0) for a, v in self.actions.items()}, self.copies)

    def peers(self):
        return [p for dim in "xyz" for p in both_ways(self.t, dim)]

    def pieces(self, c, j):
        n3 = self.t.n[self.dims[c][DIRECT]]
        return n3 if not j else self.split if n3 % self.split == 0 else 1

    def size(self, c, phase, j):
        line = self.bytes * self.t.n[self.dims[c][DIRECT]]
        return self.bytes if phase == DIRECT else line if phase == CROSS else line // self.pieces(c, j)

    def k(self, c, phase, j, i):
        dim = self.dims[c][phase]
        key = (c, phase, j, i)
        if key not in self.flip:
            self.flip[key] = self.balance.flip(dim, self.t.n[dim], self.size(c, phase, j))
        return hops(self.t.n[dim], self.flip[key])

    def plan(self, c):
        n1, n2, n3 = (self.t.n[d] for d in self.dims[c])

        def send(where, s, h):
            phase, j, _ = where
            cid = (c, where, s, h)
            self.copies[cid] = ((self.dims[c][phase], s), self.size(c, phase, j), 0)
            self.index[cid] = len(self.index)
            return cid

        def own(*where):
            k = self.k(c, *where)
            return [send(where, s, 1) for s in WAYS if k[s]]

        def line(j):
            return [x for i in range(self.pieces(c, j)) for x in own(RING, j, i)]

        def passing(*where):
            k = self.k(c, *where)
            for s in WAYS:
                for h in range(1, k[s] + 1):
                    yield s, h, (c, "pass", where, s, h), [(c, where, s, h)], [send(where, s, h + 1)] if h < k[s] else []

        def act(a, needs, sends):
            self.actions[a] = (needs, sends, TURN / 2)

        act((c, "start"), [], own(DIRECT, 0, 0) + own(RING, 0, 0))
        got = [("action", (c, "start"))]
        for s, h, a, needs, sends in passing(DIRECT, 0, 0):
            act(a, needs, sends + own(RING, 0, (-s * h) % n3))
            got.append(("action", a))
        act((c, "line"), got, own(CROSS, 0, 0))
        for s, h, a, needs, sends in passing(CROSS, 0, 0):
            act(a, needs, sends + line((-s * h) % n2))
        for j in range(n2):
            for i in range(self.pieces(c, j)):
                for _, _, a, needs, sends in passing(RING, j, i):
                    act(a, needs, sends)

    def bind(self, me, G, ssem, rsem):
        self.me, self.G, self.ssem, self.rsem = me, G, ssem, rsem
        return self

    def remote(self, cid, back):
        c, (phase, j, i), s, h = cid
        a, b, d = self.dims[c]
        n1, n2, n3 = (self.t.n[x] for x in (a, b, d))
        m1, m2, m3 = (self.me[x] for x in (a, b, d))
        off = s * (back - h)
        G = self.G[c]
        if phase == DIRECT:
            ref = G.at[m1, m2 * n3 + wrap(m3 + off, n3)]
        elif phase == CROSS:
            ref = G.at[m1, pl.ds(wrap(m2 + off, n2) * n3, n3)]
        elif j == 0:
            ref = G.at[wrap(m1 + off, n1), m2 * n3 + wrap(m3 + i, n3)]
        else:
            size = n3 // self.pieces(c, j)
            ref = G.at[wrap(m1 + off, n1), pl.ds(wrap(m2 + j, n2) * n3 + i * size, size)]
        x = self.index[cid]
        return pltpu.make_async_remote_copy(src_ref=ref, dst_ref=ref, send_sem=self.ssem.at[x], recv_sem=self.rsem.at[x], device_id=self.t.peer(self.me, self.dims[c][phase], s), device_id_type=MESH)

    def run(self, a):
        needs, sends, _ = self.actions[a]
        for cid in needs:
            if cid in self.index:
                self.remote(cid, 0).wait_recv()
        for cid in sends:
            self.remote(cid, 1).start()

    def wait_sends(self):
        for cid in self.copies:
            self.remote(cid, 1).wait_send()


MIB = 2**20
VMEM_ALL = 67043328
LAYERS, D, FF = 2, 896, 2560
LANES, ROWS, CHUNK = 128, 144, 48
HIGH = {0: 7, 1: 7, 2: 20}
WIDE = {0: FF, 1: FF, 2: D}


def tiles(u):
    high, wide = HIGH[u], WIDE[u] // LANES
    out = []
    for k in range(ROWS // 8):
        ct, row = divmod(8 * k, high)
        out.append((ct, row, min(8, high - row), ct + 1 < wide))
    return out


def owner_index(torus, c, i):
    ny, nz = torus.n["y"], torus.n["z"]
    at = {"z": lax.rem(i, nz), "y": lax.rem(lax.div(i, nz), ny), "x": lax.div(i, ny * nz)}
    n = torus.n
    a, b, d = ORDERS[c]
    return at[a], at[b] * n[d] + at[d]


def pack(torus, u, X, stride, outs):
    high = HIGH[u]
    sub = lax.broadcasted_iota(jnp.int32, (8, LANES), 0)

    def piece(i, ct, row, count, more):
        start = high * i + 8 + ct * stride
        a = X[pl.ds(start + row, 8), :]
        if count == 8:
            return a
        b = X[pl.ds(start + stride - count, 8), :] if more else jnp.zeros((8, LANES), F32)
        return jnp.where(sub < count, a, b)

    got = tiles(u)

    def body(i, carry):
        at = [owner_index(torus, c, i) for c in range(3)]
        for j in range(ROWS // 16):
            both = jnp.concatenate([piece(i, *got[2 * j]), piece(i, *got[2 * j + 1])], axis=0).astype(BF16)
            c, r = divmod(16 * j, CHUNK)
            outs[c][at[c][0], at[c][1], pl.ds(r, 16), :] = both
        return carry

    lax.fori_loop(0, torus.size, body, 0, unroll=4)


def pieces_shapes(torus, dtype, *mid):
    out = []
    for order in ORDERS:
        a, b, d = (torus.n[x] for x in order)
        out.append(jax.ShapeDtypeStruct((a, b * d) + mid + (CHUNK, LANES), dtype))
    return out


def step_and_gather(torus, g, w, m, v, count, collective_id):
    ag = AllGather(torus, LAYERS * 3 * CHUNK * 256)
    dims = "zxy"
    slots = {d: torus.n[d] - 1 for d in dims}

    def kernel(g_ref, *refs):
        w_in, m_in, v_in, G, m_out, v_out = (refs[i : i + 3] for i in range(0, 18, 3))
        flat, wflat, part, E, esend, erecv, ssem, rsem = refs[18:]
        me = torus.me()
        barrier(torus, me, [p for d in "xyz" for p in all_others(torus, d)])
        acc = jnp.zeros((8, LANES), F32)
        for l in range(LAYERS):
            for u in range(3):
                for c in range(3):
                    value = g_ref[l, u, c]
                    flat[l, u, pl.ds(c * CHUNK, CHUNK), :] = value
                    for r in range(0, CHUNK, 8):
                        acc = acc + value[r : r + 8] * value[r : r + 8]
        part[0] = acc
        base = 0
        for i, d in enumerate(dims):
            n = torus.n[d]
            copies = []
            for rel in range(1, n):
                s = base + rel - 1
                copies.append(pltpu.make_async_remote_copy(src_ref=part.at[i], dst_ref=E.at[s], send_sem=esend.at[s], recv_sem=erecv.at[s], device_id=torus.peer(me, d, rel), device_id_type=MESH))
            for copy in copies:
                copy.start()
            total = part[i]
            for rel in range(1, n):
                copies[rel - 1].wait_recv()
                total = total + E[base + rel - 1]
            part[i + 1] = total
            for copy in copies:
                copy.wait_send()
            base += n - 1
        mean = jnp.sum(part[3], keepdims=True) / count
        factor = jnp.minimum(1.0, 0.5 * lax.rsqrt(mean + 1e-30))
        for l in range(LAYERS):
            for u in range(3):
                high = HIGH[u]
                wflat[l, u, pl.ds(ROWS - 8, 8), :] = jnp.zeros((8, LANES), F32)
                for ct in range(WIDE[u] // LANES):
                    at = (l, slice(None), pl.ds(ct * LANES, LANES))
                    grad = flat[l, u, pl.ds(ct * high, high), :] * factor
                    new_m = 0.9 * m_in[u][at] + 0.1 * grad
                    new_v = 0.95 * v_in[u][at] + 0.05 * grad * grad
                    wide = w_in[u][at]
                    new_w = wide - 0.02 * (new_m * lax.rsqrt(new_v + 1e-8) + 0.1 * wide)
                    m_out[u][at] = new_m
                    v_out[u][at] = new_v
                    wflat[l, u, pl.ds(ct * high, high), :] = new_w
        it = ag.bind(me, G, ssem, rsem)
        for c in range(3):
            n = [torus.n[d] for d in ORDERS[c]]
            at = [me[d] for d in ORDERS[c]]
            for l in range(LAYERS):
                for u in range(3):
                    G[c][at[0], at[1] * n[2] + at[2], l, u] = wflat[l, u, pl.ds(c * CHUNK, CHUNK), :].astype(BF16)
        for a in ag.order:
            it.run(a)
        it.wait_sends()

    vmem = pl.BlockSpec(memory_space=pltpu.VMEM)
    nsum = sum(slots.values())
    shapes = pieces_shapes(torus, BF16, LAYERS, 3)
    f32 = [jax.ShapeDtypeStruct(t.shape, F32) for t in m]
    k = len(ag.copies)
    got = pl.pallas_call(
        kernel,
        out_shape=[pltpu.MemorySpace.VMEM(s.shape, s.dtype) for s in shapes] + f32 * 2,
        in_specs=[vmem] * 10,
        out_specs=[vmem] * 9,
        scratch_shapes=[
            pltpu.VMEM((LAYERS, 3, ROWS, LANES), F32),
            pltpu.VMEM((LAYERS, 3, ROWS, LANES), F32),
            pltpu.VMEM((4, 8, LANES), F32),
            pltpu.VMEM((nsum, 8, LANES), F32),
            pltpu.SemaphoreType.DMA((nsum,)),
            pltpu.SemaphoreType.DMA((nsum,)),
            pltpu.SemaphoreType.DMA((k,)),
            pltpu.SemaphoreType.DMA((k,)),
        ],
        compiler_params=pltpu.CompilerParams(collective_id=collective_id, has_side_effects=True, vmem_limit_bytes=10 * MIB),
        name="step_and_gather",
    )(g, *w, *m, *v)
    return got[:3], got[3:6], got[6:]


def unpack(torus, G):
    nx, ny, nz = (torus.n[d] for d in "xyz")
    pair = 2
    group = pair * nz
    groups = torus.size // group
    pairs = ny // pair

    def kernel(g0, g1, g2, *refs):
        outs, Z, Y = refs[:3], refs[3], refs[4]
        l, s = pl.program_id(0), pl.program_id(1)
        corner = {"x": lax.div(s, pairs), "y": lax.rem(s, pairs) * pair, "z": 0}
        for u in range(3):
            high, wide = HIGH[u], WIDE[u] // LANES
            for i in range(group):
                y, z = divmod(i, nz)
                at = corner | {"y": corner["y"] + y, "z": z}
                for c, ref in enumerate((g0, g1, g2)):
                    a, b, d = ORDERS[c]
                    Z[i, pl.ds(c * CHUNK, CHUNK), :] = ref[at[a], at[b] * torus.n[d] + at[d], l, u].astype(F32)
            for i in range(group):
                for ct in range(wide):
                    for r in range(0, high, 8):
                        Y[ct, pl.ds(high * i + r, 8), :] = Z[i, pl.ds(high * ct + r, 8), :]
            rows = high * group
            for ct in range(wide):
                outs[u][0, :, pl.ds(ct * LANES, LANES)] = Y[ct, pl.ds(0, rows), :].astype(BF16)

    shapes = [(LAYERS, HIGH[u] * torus.size, WIDE[u]) for u in range(3)]
    return pl.pallas_call(
        kernel,
        grid=(LAYERS, groups),
        out_shape=[jax.ShapeDtypeStruct(s, BF16) for s in shapes],
        in_specs=[pl.BlockSpec(memory_space=pltpu.VMEM)] * 3,
        out_specs=[pl.BlockSpec((1, HIGH[u] * group, WIDE[u]), lambda l, s: (l, s, 0)) for u in range(3)],
        scratch_shapes=[pltpu.VMEM((group, ROWS + 8, LANES), F32), pltpu.VMEM((FF // LANES, HIGH[2] * group + 8, LANES), F32)],
        compiler_params=pltpu.CompilerParams(vmem_limit_bytes=16 * MIB),
        name="unpack",
    )(*G)


TOKENS, TILE, PART = 2048, 256, 512
LT = TILE // LANES
NN, NT, TN = ((1,), (0,)), ((1,), (1,)), ((0,), (0,))


def dot(a, b, dims=NN):
    return lax.dot_general(a, b, (dims, ((), ())), preferred_element_type=F32)


def scale_of(wide):
    return lax.rsqrt(jnp.mean(wide * wide, -1, keepdims=True) + 1e-6)


def normed_into(h_ref, a_ref, t_ref):
    for r in range(0, TOKENS, TILE):
        wide = h_ref[pl.ds(r, TILE), :].astype(F32)
        a = (wide * scale_of(wide)).astype(BF16)
        a_ref[pl.ds(r, TILE), :] = a
        t_ref[:, pl.ds(r, TILE)] = a.T


def forward(x, wg, wu, wd):
    steps = FF // TILE

    def kernel(x_ref, wg_ref, wu_ref, wd_ref, gate_ref, up_ref, h_ref, a_ref, at_ref, xt_ref, xa, acc):
        t = pl.program_id(0)

        @pl.when(t == 0)
        def _():
            normed_into(x_ref, xa, xt_ref)
            acc[...] = jnp.zeros_like(acc)

        for r in range(0, TOKENS, PART):
            rows = pl.ds(r, PART)
            a = xa[rows, :]
            gate, up = dot(a, wg_ref[...]), dot(a, wu_ref[...])
            for k in range(LT):
                lanes = slice(k * LANES, (k + 1) * LANES)
                gate_ref[k, rows, :] = gate[:, lanes]
                up_ref[k, rows, :] = up[:, lanes]
            mid = (jax.nn.silu(gate) * up).astype(BF16)
            acc[rows, :] += dot(mid, wd_ref[...])

        @pl.when(t == steps - 1)
        def _():
            for r in range(0, TOKENS, TILE):
                rows = pl.ds(r, TILE)
                h_ref[rows, :] = x_ref[rows, :] + acc[rows, :].astype(BF16)
            normed_into(h_ref, a_ref, at_ref)

    whole = pl.BlockSpec(memory_space=pltpu.VMEM)
    cols = pl.BlockSpec((D, TILE), lambda t: (0, t))
    saved = pl.BlockSpec((LT, TOKENS, LANES), lambda t: (t, 0, 0))
    return pl.pallas_call(
        kernel,
        grid=(steps,),
        out_shape=[jax.ShapeDtypeStruct((FF // LANES, TOKENS, LANES), F32)] * 2 + [jax.ShapeDtypeStruct((TOKENS, D), BF16)] * 2 + [jax.ShapeDtypeStruct((D, TOKENS), BF16)] * 2,
        in_specs=[whole, cols, cols, pl.BlockSpec((TILE, D), lambda t: (t, 0))],
        out_specs=[saved] * 2 + [whole] * 4,
        scratch_shapes=[pltpu.VMEM((TOKENS, D), BF16), pltpu.VMEM((TOKENS, D), F32)],
        compiler_params=pltpu.CompilerParams(vmem_limit_bytes=60 * MIB),
        cost_estimate=pl.CostEstimate(flops=6 * TOKENS * D * FF, bytes_accessed=10 * TOKENS * FF, transcendentals=0),
        name="forward",
    )(x, wg, wu, wd)


def hidden_back(gate, up, d):
    s = jax.nn.sigmoid(gate)
    act = gate * s
    return (act * up).astype(BF16), (d * up * (s + act * (1.0 - s))).astype(BF16), (d * act).astype(BF16)


def last_layer(a, dy, wg, wu, wd):
    steps = FF // TILE

    def kernel(a_ref, dy_ref, wg_ref, wu_ref, wd_ref, mid_ref, dgate_ref, dup_ref):
        for r in range(0, TOKENS, PART):
            rows = pl.ds(r, PART)
            part = a_ref[rows, :]
            gate, up = dot(part, wg_ref[...]), dot(part, wu_ref[...])
            d = dot(dy_ref[rows, :], wd_ref[...], NT).astype(BF16).astype(F32)
            mid, dgate_ref[0, rows, :], dup_ref[0, rows, :] = hidden_back(gate, up, d)
            mid_ref[:, rows] = mid.T

    whole = pl.BlockSpec(memory_space=pltpu.VMEM)
    cols = pl.BlockSpec((D, TILE), lambda t: (0, t))
    rows = pl.BlockSpec((TILE, D), lambda t: (t, 0))
    saved = pl.BlockSpec((1, TOKENS, TILE), lambda t: (t, 0, 0))
    return pl.pallas_call(
        kernel,
        grid=(steps,),
        out_shape=[jax.ShapeDtypeStruct((FF, TOKENS), BF16)] + [jax.ShapeDtypeStruct((steps, TOKENS, TILE), BF16)] * 2,
        in_specs=[whole, whole, cols, cols, rows],
        out_specs=[pl.BlockSpec((TILE, TOKENS), lambda t: (t, 0))] + [saved] * 2,
        compiler_params=pltpu.CompilerParams(vmem_limit_bytes=60 * MIB),
        cost_estimate=pl.CostEstimate(flops=6 * TOKENS * D * FF, bytes_accessed=6 * TOKENS * FF, transcendentals=0),
        name="last_layer",
    )(a, dy, wg, wu, wd)


STEPS = FF // TILE
GAP = 24
STRIDE = {u: HIGH[u] * 128 + GAP for u in range(3)}
COST = {"down": 1.2, "side": 1.05, "da": 2.4, "norm": 0.5, "hidden": 1.45}


def backward(torus, mid1, dgate1, dup1, h1, dy, at1, at0, wg1, wu1, wd0, gate0, up0, collective_id):
    rs = ReduceScatter(torus, CHUNK, 3)
    DOWN = 2
    stages = [("down", (1, DOWN)), ("side", (1, 0)), ("side", (1, 1)), ("da", None), ("norm", None), ("hidden", None), ("down", (0, DOWN)), ("side", (0, 0)), ("side", (0, 1))]
    length = {kind: STEPS for kind in COST} | {"norm": TOKENS // TILE}
    actions, copies, balance, flips = {}, {}, Balance(), {}
    for kind, unit in stages:
        if unit is None:
            continue
        l, u = unit
        for c in range(3):
            flips[l, u, c] = rs.flips(balance, c)
            got, sent = rs.plan(unit, c, flips[l, u, c])
            copies |= sent
            actions |= {a: v for a, v in got.items()}
            if l:
                actions[(unit, c), "free"] = ([("action", ((unit, c), "end", DIRECT))], [], TURN)
    slots = place(actions, copies, [(i, COST[kind], length[kind], unit) for i, (kind, unit) in enumerate(stages)])

    def kernel(mid1_ref, dg1_ref, du1_ref, h1_ref, dy_ref, at1_ref, at0_ref, wg_ref, wu_ref, wd_ref, g0_ref, u0_ref, out, mid0_ref, dg0_ref, du0_ref, dyv, at, X, Mb, Db, Wb, Vb, one, pair, rsc):
        me = torus.me()
        it = rs.bind(me, rsc)
        copy = pltpu.make_async_copy
        sem_dy, sem_at = one.at[0], one.at[1]
        load_dy, load_at = copy(dy_ref, dyv, sem_dy), copy(at1_ref, at, sem_at)
        load_dy.start()
        load_at.start()

        def part(i):
            return pl.ds(i * TILE, TILE)

        def fetches(stage):
            kind, unit = stages[stage]
            layer = unit[0] if unit else 0
            src = {"mid": (mid0_ref, mid1_ref)[layer], 0: (dg0_ref, dg1_ref)[layer], 1: (du0_ref, du1_ref)[layer]}

            def of(t, s):
                if kind == "down":
                    return [copy(src["mid"].at[part(t)], Mb.at[s], pair.at[0, s])]
                if kind == "side":
                    return [copy(src[unit[1]].at[t], Db.at[s, :, part(0)], pair.at[1, s])]
                if kind == "da":
                    return [
                        copy(dg1_ref.at[t], Db.at[s, :, part(0)], pair.at[1, s]),
                        copy(du1_ref.at[t], Db.at[s, :, part(1)], pair.at[2, s]),
                        copy(wg_ref.at[:, part(t)], Wb.at[s, :, part(0)], pair.at[3, s]),
                        copy(wu_ref.at[:, part(t)], Wb.at[s, :, part(1)], pair.at[4, s]),
                    ]
                if kind == "norm":
                    return [copy(h1_ref.at[part(t)], Vb.at[s], pair.at[5, s])]
                out = [copy(wd_ref.at[part(t)], Vb.at[s], pair.at[5, s])]
                for k, ref in enumerate((g0_ref, u0_ref)):
                    out.append(copy(ref.at[pl.ds(t * LT * TOKENS, LT * TOKENS)], X.at[pl.ds((s * 2 + k) * LT * TOKENS, LT * TOKENS)], pair.at[6 + k, s]))
                return out

            return of

        def saves(t, s):
            return [copy(Mb.at[s], mid0_ref.at[part(t)], pair.at[0, s]), copy(Db.at[s, :, part(0)], dg0_ref.at[t], pair.at[1, s]), copy(Db.at[s, :, part(1)], du0_ref.at[t], pair.at[2, s])]

        def tile(stage, t, s):
            kind, unit = stages[stage]
            if kind == "down":
                got = dot(Mb[s], dyv[...])
                for ct in range(D // LANES):
                    X[pl.ds(ct * STRIDE[DOWN] + 8 + t * TILE, TILE), :] = got[:, ct * LANES : (ct + 1) * LANES]
            elif kind == "side":
                got = dot(at[...], Db[s, :, part(0)])
                for k in range(LT):
                    X[pl.ds((t * LT + k) * STRIDE[0] + 8, D), :] = got[:, k * LANES : (k + 1) * LANES]
            elif kind == "da":
                for r in range(0, TOKENS, PART):
                    got = dot(Db[s, pl.ds(r, PART), :], Wb[s], NT)
                    for ct in range(D // LANES):
                        rows = pl.ds(ct * TOKENS + r, PART)
                        X[rows, :] = jnp.where(t == 0, 0.0, X[rows, :]) + got[:, ct * LANES : (ct + 1) * LANES]
            elif kind == "norm":
                da = jnp.concatenate([X[pl.ds(ct * TOKENS + t * TILE, TILE), :] for ct in range(D // LANES)], axis=1).astype(BF16).astype(F32)
                wide = Vb[s].astype(F32)
                scale = scale_of(wide)
                inner = jnp.mean(da * wide, -1, keepdims=True)
                dyv[part(t), :] = dyv[part(t), :] + (scale * da - wide * (scale * scale * scale * inner)).astype(BF16)
            else:
                for r in range(0, TOKENS, PART):
                    rows = pl.ds(r, PART)
                    d = dot(dyv[rows, :], Vb[s], NT).astype(BF16).astype(F32)
                    gate, up = (jnp.concatenate([X[pl.ds(((s * 2 + k) * LT + j) * TOKENS + r, PART), :] for j in range(LT)], axis=1) for k in range(2))
                    mid, Db[s, rows, part(0)], Db[s, rows, part(1)] = hidden_back(gate, up, d)
                    Mb[s, :, rows] = mid.T

        def act(a):
            ((l, u), c), what = a[0], a[1:]
            flip = flips[l, u, c]
            if what[0] == "free":
                it.wait_sends(u, c, flip)
                it.give_credit(u, c)
                return
            if what[0] == "start" and l == 0:
                it.take_credit(u, c)

            def store(value):
                out[l, u, c] = value

            it.run(u, c, flip, what, store)

        def begin(stage):
            for f in fetches(stage)(0, 0):
                f.start()

        begin(0)
        barrier(torus, me, rs.peers())
        load_dy.wait()
        load_at.wait()
        for stage, (kind, unit) in enumerate(stages):
            count = length[kind]
            ahead = stage + 1 < len(stages) and stages[stage + 1][0] != "hidden" and kind != "hidden"
            of = fetches(stage)
            if kind == "da":
                copy(at0_ref, at, sem_at).start()
            if unit == (0, 0):
                copy(at0_ref, at, sem_at).wait()

            def body(t, carry, stage=stage, kind=kind, of=of, count=count, ahead=ahead):
                s = lax.rem(t, 2)
                for f in of(t, s):
                    f.wait()

                @pl.when(t + 1 < count)
                def _():
                    for f in of(t + 1, 1 - s):
                        f.start()

                if ahead:

                    @pl.when(t == count - 1)
                    def _():
                        begin(stage + 1)

                if kind == "hidden":

                    @pl.when(t > 1)
                    def _():
                        for f in saves(t - 2, s):
                            f.wait()

                tile(stage, t, s)
                if kind == "hidden":
                    for f in saves(t, s):
                        f.start()
                for k in range(count):
                    if slots[stage, k]:

                        @pl.when(t == k)
                        def _(k=k):
                            for a in slots[stage, k]:
                                act(a)

                return carry

            lax.fori_loop(0, count, body, 0)
            if kind == "hidden":
                for t in (count - 2, count - 1):
                    for f in saves(t, t % 2):
                        f.wait()
            if kind == "hidden" or stages[min(stage + 1, len(stages) - 1)][0] == "hidden":
                begin(stage + 1)
            if unit:
                for a in slots[stage, "before"]:
                    act(a)
                u = unit[1]
                pack(torus, u, X, STRIDE[u], [T.at[u] for T in it.T])
            for a in slots[stage, "after"]:
                act(a)
        for u in range(3):
            for c in range(3):
                it.wait_sends(u, c, flips[0, u, c])

    any_space = pl.BlockSpec(memory_space=pl.ANY)
    flops = 2 * TOKENS * D * FF * 9
    return pl.pallas_call(
        kernel,
        out_shape=[jax.ShapeDtypeStruct((LAYERS, 3, 3, CHUNK, LANES), F32), jax.ShapeDtypeStruct(mid1.shape, BF16), jax.ShapeDtypeStruct(dgate1.shape, BF16), jax.ShapeDtypeStruct(dup1.shape, BF16)],
        in_specs=[any_space] * 12,
        out_specs=[pl.BlockSpec(memory_space=pltpu.VMEM)] + [any_space] * 3,
        scratch_shapes=[
            pltpu.VMEM((TOKENS, D), BF16),
            pltpu.VMEM((D, TOKENS), BF16),
            pltpu.VMEM((FF // LANES * STRIDE[0], LANES), F32),
            pltpu.VMEM((2, TILE, TOKENS), BF16),
            pltpu.VMEM((2, TOKENS, 2 * TILE), BF16),
            pltpu.VMEM((2, D, 2 * TILE), BF16),
            pltpu.VMEM((2, TILE, D), BF16),
            pltpu.SemaphoreType.DMA((2,)),
            pltpu.SemaphoreType.DMA((8, 2)),
            rs.scratch(),
        ],
        compiler_params=pltpu.CompilerParams(collective_id=collective_id, has_side_effects=True, vmem_limit_bytes=VMEM_ALL),
        cost_estimate=pl.CostEstimate(flops=flops, bytes_accessed=TOKENS * FF * 20, transcendentals=0),
        name="backward",
    )(mid1, dgate1, dup1, h1, dy, at1, at0, wg1, wu1, wd0, gate0.reshape(-1, LANES), up0.reshape(-1, LANES))[0]


def solution(mesh):
    torus = Torus(4, 4, 8)
    count = float(LAYERS * 3 * D * FF)

    def step(x, dy, wg, wu, wd, mg, mu, md, vg, vu, vd):
        x, dy = x[0], dy[0]
        gate0, up0, h1, a1, at1, at0 = forward(x, wg[0], wu[0], wd[0])
        mid1, dgate1, dup1 = last_layer(a1, dy, wg[1], wu[1], wd[1])
        g = backward(torus, mid1, dgate1, dup1, h1, dy, at1, at0, wg[1], wu[1], wd[0], gate0, up0, 1)
        p = lax.axis_index("dp")
        mine = [lax.dynamic_slice_in_dim(w, p * HIGH[u], HIGH[u], 1).astype(F32) for u, w in enumerate((wg, wu, wd))]
        G, m, v = step_and_gather(torus, g, mine, (mg, mu, md), (vg, vu, vd), count, 2)
        return (*unpack(torus, G), *m, *v)

    P = jax.sharding.PartitionSpec
    return jax.shard_map(
        step,
        mesh=mesh,
        in_specs=(P(("rep", "dp")),) * 2 + (P(),) * 3 + (P(None, "dp"),) * 6,
        out_specs=(P("rep"),) * 3 + (P("rep", "dp"),) * 6,
        check_vma=False,
    )
```

```python
import heapq
import jax
import jax.numpy as jnp
from jax import lax
from jax.experimental import pallas as pl
from jax.experimental.pallas import tpu as pltpu

F32, BF16 = jnp.float32, jnp.bfloat16
MESH = pl.DeviceIdType.MESH
RATE, LATENCY = 46.6e3, 2.3
TURN, ADD, HOP = 0.1, 2.0e6, 0.7
WAYS = (1, -1)
RING, CROSS, DIRECT = range(3)
NEVER, MARGIN, SWEEPS = 1e9, 0.5, 2


class Torus:
    def __init__(self, nx, ny, nz):
        self.n = {"x": nx, "y": ny, "z": nz}
        self.size = nx * ny * nz

    def here(self):
        return Here(self)


class Here:
    def __init__(self, torus):
        p, n = lax.axis_index("dp"), torus.n
        ny, nz = n["y"], n["z"]
        mine = {"z": lax.rem(p, nz), "y": lax.rem(lax.div(p, nz), ny), "x": lax.div(p, ny * nz)}
        step = {"z": 1, "y": nz, "x": ny * nz}
        self.at = {d: [mine[d]] + [lax.rem(mine[d] + i, n[d]) for i in range(1, n[d])] for d in n}
        self.to = {d: [p + (self.at[d][i] - mine[d]) * step[d] for i in range(n[d])] for d in n}

    def peer(self, dim, delta):
        return {"dp": self.to[dim][delta % len(self.to[dim])]}

    def up(self, dim, delta):
        return self.at[dim][delta % len(self.at[dim])]


ORDERS = ("zxy", "xyz", "yxz")


def hops(n, flip):
    far, near = n // 2, n - 1 - n // 2
    return {1: near, -1: far} if flip else {1: far, -1: near}


class Balance:
    def __init__(self):
        self.load = {}

    def flip(self, dim, n, size):
        plain = [self.load.get((dim, s), 0) + size * hops(n, False)[s] for s in WAYS]
        turned = [self.load.get((dim, s), 0) + size * hops(n, True)[s] for s in WAYS]
        flip = max(turned) < max(plain)
        self.load[dim, 1], self.load[dim, -1] = turned if flip else plain
        return flip


def simulate(actions, copies):
    links, arrived, order = {}, {}, []
    waiting = {a: set(needs) for a, (needs, _, _, _) in actions.items()}
    by_need = {}
    for a, (needs, _, _, _) in actions.items():
        for c in needs:
            by_need.setdefault(c, []).append(a)
    ready = [(actions[a][3], i, a) for i, a in enumerate(actions) if not waiting[a]]
    rank = {a: i for i, a in enumerate(actions)}
    heapq.heapify(ready)
    now, done = 0.0, {}
    while ready:
        at, _, a = heapq.heappop(ready)
        now = max(now, at) + actions[a][2]
        order.append(a)
        done[a] = now
        for c in [("action", a)] + list(actions[a][1]):
            if c[0] == "action":
                end = now
            else:
                link, size, extra = copies[c]
                start = max(now, links.get(link, 0.0))
                links[link] = start + size / RATE
                end = links[link] + LATENCY + extra
            for b in by_need.get(c, ()):
                waiting[b].discard(c)
                arrived[b] = max(arrived.get(b, 0.0), end)
                if not waiting[b]:
                    heapq.heappush(ready, (max(arrived[b], actions[b][3]), rank[b], b))
    assert len(order) == len(actions), (len(order), len(actions))
    return order, now


def place(actions, copies, segments):
    links, known, left, slots, open_keys = {}, {}, dict(actions), {}, set()
    now = 0.0

    def do(a, where):
        nonlocal now
        _, sends, cost = left.pop(a)
        now += cost
        known["action", a] = now
        for c in sends:
            link, size, extra = copies[c]
            links[link] = max(now, links.get(link, 0.0)) + size / RATE
            known[c] = links[link] + LATENCY + extra
        where.append(a)

    def drain(where, allowed, wait):
        nonlocal now
        while True:
            able = [(max([known.get(c, NEVER) for c in actions[a][0]], default=0.0), i, a) for i, a in enumerate(left) if allowed(a)]
            best, _, a = min(able, default=(NEVER, 0, None))
            if best >= NEVER or not wait and best + MARGIN > now:
                return
            now = max(now, best)
            do(a, where)

    for key, cost, writes, whole in segments:
        now += cost
        slots[key] = ([], [])
        others = {(l, u, c) for (l, u), c in writes}
        drain(slots[key][0], lambda a: any(a[0][0][1] == u and a[0][1] == c and a[0][0][0] > l for l, u, c in others), True)
        open_keys |= set(whole)
        drain(slots[key][1], lambda a: a[1] != "start" or a[0] in open_keys, False)
    drain(slots[segments[-1][0]][1], lambda a: True, True)
    assert not left
    place.took = now
    return slots


def barrier(me, peers):
    sem = pltpu.get_barrier_semaphore()
    for dim, delta in peers:
        pl.semaphore_signal(sem, inc=1, device_id=me.peer(dim, delta), device_id_type=MESH)
    pl.semaphore_wait(sem, len(peers))


def both_ways(torus, dim):
    n = torus.n[dim]
    return [] if n == 1 else [(dim, 1)] if n == 2 else [(dim, 1), (dim, -1)]


def all_others(torus, dim):
    return [(dim, d) for d in range(1, torus.n[dim])]


class ReduceScatter:
    LANES = (2, 1, 1)

    def __init__(self, torus, rows, units):
        self.t, self.rows, self.units = torus, rows, units
        self.dims = [tuple(order) for order in ORDERS]
        self.nslots = max(self.base(c, DIRECT, 0) + self.sizes(c)[DIRECT] - 1 for c in range(3))

    def sizes(self, c):
        return [self.t.n[d] for d in self.dims[c]]

    def here(self, c):
        return [self.me.up(d, 0) for d in self.dims[c]]

    def base(self, c, phase, lane):
        n = self.sizes(c)
        return sum((n[i] - 1) * self.LANES[i] for i in range(phase)) + lane * (n[phase] - 1)

    def peers(self):
        full = {dims[DIRECT] for dims in self.dims}
        out = []
        for dim in "xyz":
            out += all_others(self.t, dim) if dim in full else both_ways(self.t, dim)
        return out

    def credit_peers(self, c):
        a, b, d = self.dims[c]
        return both_ways(self.t, a) + both_ways(self.t, b) + all_others(self.t, d)

    def scratch(self):
        n = self.t.n
        t, r1, r2, r3, k2, k3 = [], [], [], [], [], []
        for dims in self.dims:
            n1, n2, n3 = (n[d] for d in dims)
            tail = (self.rows, 128)
            t.append(pltpu.VMEM((self.units, n1, n2 * n3) + tail, BF16))
            r1.append(pltpu.VMEM((self.units, max(n1 - 1, 1), n2 * n3) + tail, BF16))
            r2.append(pltpu.VMEM((self.units, max(n2 - 1, 1), n3) + tail, BF16))
            r3.append(pltpu.VMEM((self.units, max(n3 - 1, 1)) + tail, BF16))
            k2.append(pltpu.VMEM((self.units, n3) + tail, F32))
            k3.append(pltpu.VMEM((self.units,) + tail, F32))
        sems = [pltpu.SemaphoreType.DMA((self.units, 3, self.nslots)), pltpu.SemaphoreType.DMA((self.units, 3, self.nslots)), pltpu.SemaphoreType.REGULAR((self.units, 3))]
        return [t, r1, r2, r3, k2, k3] + sems

    def slot(self, c, phase, sign, h):
        return h if sign > 0 else self.sizes(c)[phase] - 2 - h

    def flips(self, balance, c):
        n1, n2, n3 = self.sizes(c)
        block, (a, b, d) = self.rows * 256, self.dims[c]
        for rel in range(1, n3):
            link = d, 1 if rel <= n3 // 2 else -1
            balance.load[link] = balance.load.get(link, 0) + block * min(rel, n3 - rel)
        ring = [balance.flip(a, n1, block * n2 * n3 // self.LANES[RING]) for _ in range(self.LANES[RING])]
        return ring, [balance.flip(b, n2, block * n3)]

    def plan(self, unit, c, flip):
        n = self.sizes(c)
        n1, n2, n3 = n
        block = self.rows * 256
        size = [block * n2 * n3 // self.LANES[RING], block * n3, block]
        actions, copies = {}, {}
        key = (unit, c)

        def send(phase, lane, sign, h):
            cid = ("copy", key, phase, lane, sign, h)
            copies[cid] = ((self.dims[c][phase], sign), size[phase], 0)
            return cid

        first, last = [[], []], [[], []]
        for phase in (RING, CROSS):
            for lane, turned in enumerate(flip[phase]):
                k = hops(n[phase], turned)
                ways = [s for s in WAYS if k[s]]
                first[phase] += [send(phase, lane, s, k[s] - 1) for s in ways]
                last[phase] += [("copy", key, phase, lane, s, 0) for s in ways]
                for s in ways:
                    for h in range(k[s] - 1, 0, -1):
                        actions[key, "step", phase, lane, s, h] = ([("copy", key, phase, lane, s, h)], [send(phase, lane, s, h - 1)], size[phase] / ADD)
        direct = []
        for rel in range(1, n3):
            cid = ("copy", key, DIRECT, 0, 0, rel)
            far = min(rel, n3 - rel)
            copies[cid] = ((self.dims[c][DIRECT], 1 if rel <= n3 // 2 else -1), size[DIRECT] * far, HOP * (far - 1))
            direct.append(cid)
        sends = first + [direct, []]
        actions[key, "start"] = ([], sends[RING], TURN)
        before = (key, "start")
        for phase, needs in enumerate(last + [direct]):
            a = (key, "end", phase)
            actions[a] = (needs + [("action", before)], sends[phase + 1], size[phase] * self.LANES[phase] / ADD + TURN)
            before = a
        return actions, copies

    def bind(self, me, refs):
        self.me, (self.T, self.R1, self.R2, self.R3, self.K2, self.K3, self.ssem, self.rsem, self.credit) = me, refs
        return self

    def remote(self, u, c, phase, lane, sign, h):
        n1, n2, n3 = self.sizes(c)
        d1, d2, d3 = self.dims[c]
        up = self.me.up
        mine = self.T[c].at[u]
        slot = h - 1 if phase == DIRECT else self.slot(c, phase, sign, h)
        if phase == RING:
            part = n2 * n3 // self.LANES[RING]
            blocks = pl.ds(lane * part, part)
            src, dst = mine.at[up(d1, sign * (h + 1)), blocks], self.R1[c].at[u, slot, blocks]
        elif phase == CROSS:
            src, dst = mine.at[up(d1, 0), pl.ds(up(d2, sign * (h + 1)) * n3, n3)], self.R2[c].at[u, slot]
        else:
            sign = h
            src, dst = mine.at[up(d1, 0), up(d2, 0) * n3 + up(d3, h)], self.R3[c].at[u, slot]
        s = self.base(c, phase, lane) + slot
        to = self.me.peer(self.dims[c][phase], sign)
        return pltpu.make_async_remote_copy(src_ref=src, dst_ref=dst, send_sem=self.ssem.at[u, c, s], recv_sem=self.rsem.at[u, c, s], device_id=to, device_id_type=MESH)

    def all_sends(self, c, flip):
        n = self.sizes(c)
        out = []
        for phase in (RING, CROSS):
            for lane, turned in enumerate(flip[phase]):
                k = hops(n[phase], turned)
                out += [(phase, lane, s, h) for s in WAYS for h in range(k[s])]
        return out + [(DIRECT, 0, 0, rel) for rel in range(1, n[DIRECT])]

    def run(self, u, c, flip, what, store):
        n = self.sizes(c)
        n1, n2, n3 = n
        m1, m2, m3 = self.here(c)
        T, R1, R2, R3 = (r[c].at[u] for r in (self.T, self.R1, self.R2, self.R3))
        K2, K3 = self.K2[c].at[u], self.K3[c].at[u]
        mine = T.at[m1]
        wide = lambda v: v.astype(F32)
        go = lambda *a: self.remote(u, c, *a)

        def loop(count, body):
            def one(i, carry):
                body(i)
                return carry

            lax.fori_loop(0, count, one, 0, unroll=2 - count % 2)

        def ways(phase):
            for lane, turned in enumerate(flip[phase]):
                k = hops(n[phase], turned)
                for s in WAYS:
                    if k[s]:
                        yield lane, s, k[s]

        def sends(phase):
            for lane, s, k in ways(phase):
                go(phase, lane, s, k - 1).start()

        def arrived(phase):
            got = set()
            for lane, s, _ in ways(phase):
                go(phase, lane, s, 0).wait_recv()
                got.add(self.slot(c, phase, s, 0))
            return sorted(got)

        kind, *where = what
        if kind == "start":
            sends(RING)
        elif kind == "step":
            phase, lane, s, h = where
            go(*where).wait_recv()
            slot = self.slot(c, phase, s, h)
            q = self.me.up(self.dims[c][phase], s * h)
            part = n2 * n3 // self.LANES[RING]

            def ring(i):
                b = lane * part + i
                T[q, b] = (wide(T[q, b]) + wide(R1[slot, b])).astype(BF16)

            def cross(i):
                b = q * n3 + i
                mine[b] = (wide(mine[b]) + wide(R2[slot, i])).astype(BF16)

            loop(part if phase == RING else n3, cross if phase else ring)
            go(phase, lane, s, h - 1).start()
        elif where == [RING]:
            got = arrived(RING)

            def total(b):
                return sum((wide(R1[g, b]) for g in got), wide(mine[b]))

            def own(i):
                K2[i] = total(m2 * n3 + i)

            def others(i):
                b = lax.rem((m2 + 1) * n3 + i, n2 * n3)
                mine[b] = total(b).astype(BF16)

            loop((n2 - 1) * n3, others)
            sends(CROSS)
            loop(n3, own)
        elif where == [CROSS]:
            got = arrived(CROSS)

            def total(q):
                return sum((wide(R2[g, q]) for g in got), K2[q])

            for rel in range(1, n3):
                q = self.me.up(self.dims[c][DIRECT], rel)
                mine[m2 * n3 + q] = total(q).astype(BF16)
            for rel in range(1, n3):
                go(DIRECT, 0, 0, rel).start()
            K3[...] = total(m3)
        else:
            for rel in range(1, n3):
                go(DIRECT, 0, 0, rel).wait_recv()
            store(sum((wide(R3[i]) for i in range(n3 - 1)), K3[...]).astype(BF16).astype(F32))

    def wait_sends(self, u, c, flip):
        for a in self.all_sends(c, flip):
            self.remote(u, c, *a).wait_send()

    def give_credit(self, u, c):
        for dim, delta in self.credit_peers(c):
            pl.semaphore_signal(self.credit.at[u, c], inc=1, device_id=self.me.peer(dim, delta), device_id_type=MESH)

    def take_credit(self, u, c):
        pl.semaphore_wait(self.credit.at[u, c], len(self.credit_peers(c)))


class AllGather:
    def __init__(self, torus, block_bytes, split=2):
        self.t, self.bytes, self.split = torus, block_bytes, split
        self.dims = [tuple(order) for order in ORDERS]
        self.flip, self.balance = {}, Balance()
        self.build()
        for key in list(self.flip) * SWEEPS:
            took = self.took
            self.flip[key] = not self.flip[key]
            self.build()
            if self.took >= took:
                self.flip[key] = not self.flip[key]
        self.build()

    def build(self):
        self.copies, self.actions, self.index = {}, {}, {}
        for c in range(3):
            self.plan(c)
        self.order, self.took = simulate({a: (*v, 0) for a, v in self.actions.items()}, self.copies)

    def peers(self):
        return [p for dim in "xyz" for p in both_ways(self.t, dim)]

    def pieces(self, c, j):
        n3 = self.t.n[self.dims[c][DIRECT]]
        return n3 if not j else self.split if n3 % self.split == 0 else 1

    def size(self, c, phase, j):
        line = self.bytes * self.t.n[self.dims[c][DIRECT]]
        return self.bytes if phase == DIRECT else line // self.pieces(c, 1 if phase == CROSS else j)

    def k(self, c, phase, j, i):
        dim = self.dims[c][phase]
        key = (c, phase, j, i)
        if key not in self.flip:
            self.flip[key] = self.balance.flip(dim, self.t.n[dim], self.size(c, phase, j))
        return hops(self.t.n[dim], self.flip[key])

    def plan(self, c):
        n1, n2, n3 = (self.t.n[d] for d in self.dims[c])

        def send(where, s, h):
            phase, j, _ = where
            cid = (c, where, s, h)
            self.copies[cid] = ((self.dims[c][phase], s), self.size(c, phase, j), 0)
            self.index[cid] = len(self.index)
            return cid

        def own(*where):
            k = self.k(c, *where)
            return [send(where, s, 1) for s in WAYS if k[s]]

        def passing(*where):
            k = self.k(c, *where)
            for s in WAYS:
                for h in range(1, k[s] + 1):
                    yield s, h, (c, "pass", where, s, h), [(c, where, s, h)], [send(where, s, h + 1)] if h < k[s] else []

        def act(a, needs, sends):
            self.actions[a] = (needs, sends, TURN / 2)

        act((c, "start"), [], own(DIRECT, 0, 0) + own(RING, 0, 0))
        got = [("action", (c, "start"))]
        for s, h, a, needs, sends in passing(DIRECT, 0, 0):
            act(a, needs, sends + own(RING, 0, (-s * h) % n3))
            got.append(("action", a))
        parts = range(self.pieces(c, 1))
        act((c, "line"), got, [x for i in parts for x in own(CROSS, 0, i)])
        for i in parts:
            for s, h, a, needs, sends in passing(CROSS, 0, i):
                after = (-s * h) % n2, i
                if c:
                    act(a, needs, sends + own(RING, *after))
                else:
                    act(a, needs, sends)
                    act((c, "later", *after), [("action", x) for x in (a, (1, "line"), (2, "line"))], own(RING, *after))
        for j in range(n2):
            for i in range(self.pieces(c, j)):
                for _, _, a, needs, sends in passing(RING, j, i):
                    act(a, needs, sends)

    def bind(self, me, G, ssem, rsem):
        self.me, self.G, self.ssem, self.rsem = me, G, ssem, rsem
        return self

    def remote(self, cid, back):
        c, (phase, j, i), s, h = cid
        d1, d2, d3 = self.dims[c]
        n3, up = self.t.n[d3], self.me.up
        off = s * (back - h)
        G = self.G[c]
        if phase == DIRECT:
            ref = G.at[up(d1, 0), up(d2, 0) * n3 + up(d3, off)]
        elif phase == CROSS:
            size = n3 // self.pieces(c, 1)
            ref = G.at[up(d1, 0), pl.ds(up(d2, off) * n3 + i * size, size)]
        elif j == 0:
            ref = G.at[up(d1, off), up(d2, 0) * n3 + up(d3, i)]
        else:
            size = n3 // self.pieces(c, j)
            ref = G.at[up(d1, off), pl.ds(up(d2, j) * n3 + i * size, size)]
        x = self.index[cid]
        return pltpu.make_async_remote_copy(src_ref=ref, dst_ref=ref, send_sem=self.ssem.at[x], recv_sem=self.rsem.at[x], device_id=self.me.peer(self.dims[c][phase], s), device_id_type=MESH)

    def run(self, a):
        needs, sends, _ = self.actions[a]
        for cid in needs:
            if cid in self.index:
                self.remote(cid, 0).wait_recv()
        for cid in sends:
            self.remote(cid, 1).start()

    def wait_sends(self):
        for cid in self.copies:
            self.remote(cid, 1).wait_send()


MIB = 2**20
VMEM_ALL = 67043328
LAYERS, D, FF = 2, 896, 2560
LANES, ROWS, CHUNK = 128, 144, 48
HIGH = {0: 7, 1: 7, 2: 20}
WIDE = {0: FF, 1: FF, 2: D}
WINDOW = (16, 16, 24)


HALVES, RING_TILES = 2, 8
TOKENS, TILE, PART = 2048, 256, 512
LT, STEPS = TILE // LANES, FF // TILE
HALF = STEPS // HALVES


def home(u, ct):
    if u == HALVES:
        return u, ct
    t, k = divmod(ct, 2 * LT)
    m, j = divmod(k, LT)
    return m, (u * HALF + t) * LT + j


def tiles(u):
    high, wide = HIGH[u], WIDE[u] // LANES
    out = []
    for k in range(ROWS // 8):
        ct, row = divmod(8 * k, high)
        out.append((ct, row, min(8, high - row), ct + 1 < wide))
    return out


def owner_index(torus, c, i):
    ny, nz = torus.n["y"], torus.n["z"]
    at = {"z": lax.rem(i, nz), "y": lax.rem(lax.div(i, nz), ny), "x": lax.div(i, ny * nz)}
    n = torus.n
    a, b, d = ORDERS[c]
    return at[a], at[b] * n[d] + at[d]


def pack(torus, u, X, base, parts, first, count, outs):
    high = HIGH[u]
    sub = lax.broadcasted_iota(jnp.int32, (8, LANES), 0)

    def piece(i, ct, row, whole, more):
        a = X[pl.ds(base(ct) + high * i + row, 8), :]
        if whole == 8:
            return a
        b = X[pl.ds(base(ct + 1) + high * i - whole, 8), :] if more else jnp.zeros((8, LANES), F32)
        return jnp.where(sub < whole, a, b)

    got = tiles(u)

    def body(i, carry):
        at = [owner_index(torus, c, first + i) for c in range(3)]
        for j in parts:
            both = jnp.concatenate([piece(i, *got[2 * j]), piece(i, *got[2 * j + 1])], axis=0).astype(BF16)
            c, r = divmod(16 * j, CHUNK)
            outs[c][at[c][0], at[c][1], pl.ds(r, 16), :] = both
        return carry

    lax.fori_loop(0, count, body, 0, unroll=4)


def pieces_shapes(torus, dtype, *mid):
    out = []
    for order in ORDERS:
        a, b, d = (torus.n[x] for x in order)
        out.append(jax.ShapeDtypeStruct((a, b * d) + mid + (CHUNK, LANES), dtype))
    return out


def step_and_gather(torus, g, w, m, v, count, collective_id):
    ag = AllGather(torus, LAYERS * 3 * CHUNK * 256)
    dims = "zxy"
    slots = {d: torus.n[d] - 1 for d in dims}

    def window(p, x):
        rows = WINDOW[x]
        first = lax.div(p * HIGH[x], 8) * 8
        return pl.multiple_of(jnp.minimum(first, HIGH[x] * torus.size - rows), 8), rows

    def kernel(g_ref, *refs):
        w_in, m_in, v_in, G, m_out, v_out = (refs[i : i + 3] for i in range(0, 18, 3))
        flat, wflat, part, E, esend, erecv, ssem, rsem, win, wide_win, wsem = refs[18:]
        me = torus.here()
        p = lax.axis_index("dp")
        loads = []
        for x in range(3):
            first, rows = window(p, x)
            loads.append(pltpu.make_async_copy(w_in[x].at[:, pl.ds(first, rows)], win[x], wsem.at[x]))
            loads[x].start()
        barrier(me, [p for d in "xyz" for p in all_others(torus, d)])
        for x in range(3):
            loads[x].wait()
            for lt in range(WIDE[x] // LANES):
                wide_win[x][:, lt] = win[x][:, :, pl.ds(lt * LANES, LANES)].astype(F32)
        acc = jnp.zeros((8, LANES), F32)
        for l in range(LAYERS):
            for u in range(3):
                for c in range(3):
                    value = g_ref[l, u, c]
                    flat[l, u, pl.ds(c * CHUNK, CHUNK), :] = value
                    for r in range(0, CHUNK, 8):
                        acc = acc + value[r : r + 8] * value[r : r + 8]
        part[0] = acc
        base = 0
        for i, d in enumerate(dims):
            n = torus.n[d]
            copies = []
            for rel in range(1, n):
                s = base + rel - 1
                copies.append(pltpu.make_async_remote_copy(src_ref=part.at[i], dst_ref=E.at[s], send_sem=esend.at[s], recv_sem=erecv.at[s], device_id=me.peer(d, rel), device_id_type=MESH))
            for copy in copies:
                copy.start()
            total = part[i]
            for rel in range(1, n):
                copies[rel - 1].wait_recv()
                total = total + E[base + rel - 1]
            part[i + 1] = total
            for copy in copies:
                copy.wait_send()
            base += n - 1
        mean = jnp.sum(part[3], keepdims=True) / count
        factor = jnp.minimum(1.0, 0.5 * lax.rsqrt(mean + 1e-30))
        for l in range(LAYERS):
            for u in range(3):
                high = HIGH[u]
                wflat[l, u, pl.ds(ROWS - 8, 8), :] = jnp.zeros((8, LANES), F32)
                for ct in range(WIDE[u] // LANES):
                    x, lt = home(u, ct)
                    at = (slice(None), l, pl.ds(lt * LANES, LANES))
                    grad = flat[l, u, pl.ds(ct * high, high), :] * factor
                    new_m = 0.9 * m_in[x][at] + 0.1 * grad
                    new_v = 0.95 * v_in[x][at] + 0.05 * grad * grad
                    wide = wide_win[x][l, lt, pl.ds(p * high - window(p, x)[0], high), :]
                    new_w = wide - 0.02 * (new_m * lax.rsqrt(new_v + 1e-8) + 0.1 * wide)
                    m_out[x][at] = new_m
                    v_out[x][at] = new_v
                    wflat[l, u, pl.ds(ct * high, high), :] = new_w
        it = ag.bind(me, G, ssem, rsem)
        for c in range(3):
            n = [torus.n[d] for d in ORDERS[c]]
            at = [me.up(d, 0) for d in ORDERS[c]]
            for l in range(LAYERS):
                for u in range(3):
                    G[c][at[0], at[1] * n[2] + at[2], l, u] = wflat[l, u, pl.ds(c * CHUNK, CHUNK), :].astype(BF16)
        for a in ag.order:
            it.run(a)
        it.wait_sends()

    vmem = pl.BlockSpec(memory_space=pltpu.VMEM)
    nsum = sum(slots.values())
    shapes = pieces_shapes(torus, BF16, LAYERS, 3)
    turn = lambda ts: [jnp.transpose(t, (1, 0, 2)) for t in ts]
    m, v = turn(m), turn(v)
    f32 = [jax.ShapeDtypeStruct(t.shape, F32) for t in m]
    k = len(ag.copies)
    got = pl.pallas_call(
        kernel,
        out_shape=[pltpu.MemorySpace.VMEM(s.shape, s.dtype) for s in shapes] + f32 * 2,
        in_specs=[vmem] + [pl.BlockSpec(memory_space=pl.ANY)] * 3 + [vmem] * 6,
        out_specs=[vmem] * 9,
        scratch_shapes=[
            pltpu.VMEM((LAYERS, 3, ROWS, LANES), F32),
            pltpu.VMEM((LAYERS, 3, ROWS, LANES), F32),
            pltpu.VMEM((4, 8, LANES), F32),
            pltpu.VMEM((nsum, 8, LANES), F32),
            pltpu.SemaphoreType.DMA((nsum,)),
            pltpu.SemaphoreType.DMA((nsum,)),
            pltpu.SemaphoreType.DMA((k,)),
            pltpu.SemaphoreType.DMA((k,)),
            [pltpu.VMEM((LAYERS, WINDOW[x], WIDE[x]), BF16) for x in range(3)],
            [pltpu.VMEM((LAYERS, WIDE[x] // LANES, WINDOW[x], LANES), F32) for x in range(3)],
            pltpu.SemaphoreType.DMA((3,)),
        ],
        compiler_params=pltpu.CompilerParams(collective_id=collective_id, has_side_effects=True, vmem_limit_bytes=26 * MIB),
        name="step_and_gather",
    )(g, *w, *m, *v)
    return got[:3], turn(got[3:6]), turn(got[6:])


def unpack(torus, G):
    nx, ny, nz = (torus.n[d] for d in "xyz")
    pair = 2
    group = pair * nz
    groups = torus.size // group
    pairs = ny // pair

    def kernel(g0, g1, g2, *refs):
        outs, Z, Y = refs[:3], refs[3], refs[4]
        l, s = pl.program_id(0), pl.program_id(1)
        corner = {"x": lax.div(s, pairs), "y": lax.rem(s, pairs) * pair, "z": 0}
        for u in range(3):
            high, wide = HIGH[u], WIDE[u] // LANES
            for i in range(group):
                y, z = divmod(i, nz)
                at = corner | {"y": corner["y"] + y, "z": z}
                for c, ref in enumerate((g0, g1, g2)):
                    a, b, d = ORDERS[c]
                    Z[i, pl.ds(c * CHUNK, CHUNK), :] = ref[at[a], at[b] * torus.n[d] + at[d], l, u].astype(F32)
            for i in range(group):
                for ct in range(wide):
                    for r in range(0, high, 8):
                        Y[ct, pl.ds(high * i + r, 8), :] = Z[i, pl.ds(high * ct + r, 8), :]
            rows = high * group
            for ct in range(wide):
                x, lt = home(u, ct)
                outs[x][0, :, pl.ds(lt * LANES, LANES)] = Y[ct, pl.ds(0, rows), :].astype(BF16)

    shapes = [(LAYERS, HIGH[u] * torus.size, WIDE[u]) for u in range(3)]
    return pl.pallas_call(
        kernel,
        grid=(LAYERS, groups),
        out_shape=[jax.ShapeDtypeStruct(s, BF16) for s in shapes],
        in_specs=[pl.BlockSpec(memory_space=pltpu.VMEM)] * 3,
        out_specs=[pl.BlockSpec((1, HIGH[u] * group, WIDE[u]), lambda l, s: (l, s, 0)) for u in range(3)],
        scratch_shapes=[pltpu.VMEM((group, ROWS + 8, LANES), F32), pltpu.VMEM((FF // LANES, HIGH[2] * group + 8, LANES), F32)],
        compiler_params=pltpu.CompilerParams(vmem_limit_bytes=26 * MIB),
        name="unpack",
    )(*G)


NN, NT, TN = ((1,), (0,)), ((1,), (1,)), ((0,), (0,))


def dot(a, b, dims=NN):
    return lax.dot_general(a, b, (dims, ((), ())), preferred_element_type=F32)


def scale_of(wide):
    return lax.rsqrt(jnp.mean(wide * wide, -1, keepdims=True) + 1e-6)


def normed_into(h_ref, a_ref, t_ref):
    for r in range(0, TOKENS, TILE):
        wide = h_ref[pl.ds(r, TILE), :].astype(F32)
        a = (wide * scale_of(wide)).astype(BF16)
        a_ref[pl.ds(r, TILE), :] = a
        t_ref[:, pl.ds(r, TILE)] = a.T


def forward(x, wg, wu, wd):
    steps = STEPS

    def kernel(x_ref, wg_ref, wu_ref, wd_ref, gate_ref, up_ref, h_ref, a_ref, at_ref, xt_ref, xa, acc):
        t = pl.program_id(0)

        @pl.when(t == 0)
        def _():
            normed_into(x_ref, xa, xt_ref)
            acc[...] = jnp.zeros_like(acc)

        for r in range(0, TOKENS, PART):
            rows = pl.ds(r, PART)
            a = xa[rows, :]
            both = dot(a, jnp.concatenate([wg_ref[0], wu_ref[0]], axis=1))
            gate, up = both[:, :TILE], both[:, TILE:]
            for k in range(LT):
                lanes = slice(k * LANES, (k + 1) * LANES)
                gate_ref[k, rows, :] = gate[:, lanes]
                up_ref[k, rows, :] = up[:, lanes]
            mid = (jax.nn.silu(gate) * up).astype(BF16)
            acc[rows, :] += dot(mid, wd_ref[0])

        @pl.when(t == steps - 1)
        def _():
            for r in range(0, TOKENS, TILE):
                rows = pl.ds(r, TILE)
                h_ref[rows, :] = x_ref[rows, :] + acc[rows, :].astype(BF16)
            normed_into(h_ref, a_ref, at_ref)

    whole = pl.BlockSpec(memory_space=pltpu.VMEM)
    cols = pl.BlockSpec((1, D, TILE), lambda t: (0, 0, t))
    saved = pl.BlockSpec((LT, TOKENS, LANES), lambda t: (t, 0, 0))
    return pl.pallas_call(
        kernel,
        grid=(steps,),
        out_shape=[jax.ShapeDtypeStruct((FF // LANES, TOKENS, LANES), F32)] * 2 + [jax.ShapeDtypeStruct((TOKENS, D), BF16)] * 2 + [jax.ShapeDtypeStruct((D, TOKENS), BF16)] * 2,
        in_specs=[whole, cols, cols, pl.BlockSpec((1, TILE, D), lambda t: (0, t, 0))],
        out_specs=[saved] * 2 + [whole] * 4,
        scratch_shapes=[pltpu.VMEM((TOKENS, D), BF16), pltpu.VMEM((TOKENS, D), F32)],
        compiler_params=pltpu.CompilerParams(vmem_limit_bytes=60 * MIB),
        cost_estimate=pl.CostEstimate(flops=6 * TOKENS * D * FF, bytes_accessed=10 * TOKENS * FF, transcendentals=0),
        name="forward",
    )(x, wg, wu, wd)


def hidden_back(gate, up, d):
    s = jax.nn.sigmoid(gate)
    act = gate * s
    return (act * up).astype(BF16), (d * up * (s + act * (1.0 - s))).astype(BF16), (d * act).astype(BF16)


GAP = 24
SIDE_STRIDE, DOWN_STRIDE = D + GAP, FF // HALVES + GAP
DOWN_BASE = RING_TILES * SIDE_STRIDE
X_ROWS = DOWN_BASE + D // LANES * DOWN_STRIDE
COST = {"last": (3.7, 2.6, 1.3), "first": (1.6, 2.6, 1.3), "da": (2.4,), "norm": (0.5,)}
PACK_DOWN = 1.0
WHOLE = ((0,), (1, 2), (3, 4), (5, 6), (7, 8))
COLOUR = {1: 0, 3: 1, 4: 2}
PASSES = ("last", "da", "norm", "first")
COUNT = {"last": STEPS, "da": STEPS, "norm": TOKENS // TILE, "first": STEPS}
SIDE, DOWN = 1, 2


def timeline():
    out = []
    for kind in PASSES:
        layer = {"last": 1, "first": 0}.get(kind)
        for t in range(COUNT[kind]):
            half, tt = divmod(t, HALF)
            for i, cost in enumerate(COST[kind]):
                writes, whole = [], []
                if i == SIDE:
                    unit = (layer, half)
                    writes = [(unit, c) for c in range(3)] if tt == 0 else []
                    whole = [(unit, COLOUR[tt])] if tt in COLOUR else []
                if i == DOWN and tt == HALF - 1:
                    cost += PACK_DOWN
                    mine = [((layer, HALVES), c) for c in range(3)]
                    writes, whole = (mine, []) if half == 0 else ([], mine)
                out.append(((kind, t, i), cost, writes, whole))
    return out


def hidden_back(gate, up, d):
    s = jax.nn.sigmoid(gate)
    act = gate * s
    return (act * up).astype(BF16), (d * up * (s + act * (1.0 - s))).astype(BF16), (d * act).astype(BF16)


def backward(torus, gate0, up0, h1, a1, at1, at0, dy, wg, wu, wd, collective_id):
    rs = ReduceScatter(torus, CHUNK, 3)
    actions, copies, balance, flips = {}, {}, Balance(), {}
    for l in range(LAYERS):
        for u in range(3):
            for c in range(3):
                flips[l, u, c] = rs.flips(balance, c)
                got, sent = rs.plan((l, u), c, flips[l, u, c])
                copies |= sent
                actions |= got
                if l:
                    key = ((l, u), c)
                    actions[key, "free"] = ([("action", (key, "end", DIRECT))], [], TURN)
    slots = place(actions, copies, timeline())

    def kernel(gate_ref, up_ref, h1_ref, a1_ref, at1_ref, at0_ref, dy_ref, wg_ref, wu_ref, wd_ref, out, both_ref, dyv, av, at, X, Mb, Db, Wb, Vb, Hb, once, pair, hsem, rsc):
        me = torus.here()
        it = rs.bind(me, rsc)
        copy = pltpu.make_async_copy
        loads = [copy(src, dst, once.at[i]) for i, (src, dst) in enumerate(((dy_ref, dyv), (a1_ref, av), (at1_ref, at)))]
        load_at0 = copy(at0_ref, at, once.at[3])

        def part(i):
            return pl.ds(i * TILE, TILE)

        def sides(layer, t, s):
            return [copy(ref.at[layer, :, part(t)], Wb.at[s, :, part(k)], pair.at[k, s]) for k, ref in enumerate((wg_ref, wu_ref))]

        def fetch(kind, t, s):
            both, rows = pair.at[2, s], pair.at[3, s]
            if kind == "last":
                return sides(1, t, s) + [copy(wd_ref.at[1, part(t)], Vb.at[s], rows)]
            if kind == "da":
                return sides(1, t, s) + [copy(both_ref.at[t], Db.at[s], both)]
            if kind == "norm":
                return [copy(h1_ref.at[part(t)], Vb.at[s], rows)]
            return [copy(wd_ref.at[0, part(t)], Vb.at[s], rows)]

        def save(t, s):
            return copy(Db.at[s], both_ref.at[t], pair.at[4, s])

        def hiddens(t, q):
            return [copy(ref.at[pl.ds(t * LT, LT), pl.ds(q * PART, PART)], Hb.at[q, k], hsem.at[q, k]) for k, ref in enumerate((gate_ref, up_ref))]

        def act(a):
            ((l, u), c), what = a[0], a[1:]
            if what[0] == "free":
                it.wait_sends(u, c, flips[l, u, c])
                it.give_credit(u, c)
                return
            if what[0] == "start" and l == 0:
                it.take_credit(u, c)

            def store(value):
                out[l, u, c] = value

            it.run(u, c, flips[l, u, c], what, store)

        def point(kind, t, i, which):
            for k in range(COUNT[kind]):
                if slots[kind, k, i][which]:

                    @pl.when(t == k)
                    def _(k=k):
                        for a in slots[kind, k, i][which]:
                            act(a)

        def hidden(kind, t, s):
            for q in range(TOKENS // PART):
                rows = pl.ds(q * PART, PART)
                if kind == "last":
                    both = dot(av[rows, :], Wb[s])
                    gate, up = both[:, :TILE], both[:, TILE:]
                else:
                    for f in hiddens(t, q):
                        f.wait()
                    gate, up = (jnp.concatenate([Hb[q, k, j] for j in range(LT)], axis=1) for k in range(2))
                d = dot(dyv[rows, :], Vb[s], NT).astype(BF16).astype(F32)
                mid, Db[s, rows, part(0)], Db[s, rows, part(1)] = hidden_back(gate, up, d)
                Mb[:, rows] = mid.T
                if kind == "first":

                    @pl.when(t + 1 < STEPS)
                    def _(q=q):
                        for f in hiddens(t + 1, q):
                            f.start()

        def side(kind, t, s):
            half, tt = lax.div(t, HALF), lax.rem(t, HALF)
            got = dot(at[...], Db[s])
            for k in range(2 * LT):
                X[pl.ds((lax.rem(tt, 2) * 2 * LT + k) * SIDE_STRIDE + 8, D), :] = got[:, k * LANES : (k + 1) * LANES]
            point(kind, t, SIDE, 0)
            for v, parts in enumerate(WHOLE):

                @pl.when(tt == v)
                def _(parts=parts):
                    pack(torus, 0, X, lambda ct: ct % RING_TILES * SIDE_STRIDE + 8, parts, 0, torus.size, [T.at[half] for T in it.T])

        def down(kind, t, s):
            half, tt = lax.div(t, HALF), lax.rem(t, HALF)
            got = dot(Mb[...], dyv[...])
            for ct in range(D // LANES):
                X[pl.ds(DOWN_BASE + ct * DOWN_STRIDE + 8 + tt * TILE, TILE), :] = got[:, ct * LANES : (ct + 1) * LANES]
            point(kind, t, DOWN, 0)

            @pl.when(tt == HALF - 1)
            def _():
                some = torus.size // HALVES
                pack(torus, HALVES, X, lambda ct: DOWN_BASE + ct * DOWN_STRIDE + 8, range(ROWS // 16), half * some, some, [T.at[HALVES] for T in it.T])

        def d_a(t, s):
            for r in range(0, TOKENS, PART):
                got = dot(Db[s, pl.ds(r, PART), :], Wb[s], NT)
                for ct in range(D // LANES):
                    rows = pl.ds(ct * TOKENS + r, PART)
                    X[rows, :] = jnp.where(t == 0, 0.0, X[rows, :]) + got[:, ct * LANES : (ct + 1) * LANES]

        def norm(t, s):
            da = jnp.concatenate([X[pl.ds(ct * TOKENS + t * TILE, TILE), :] for ct in range(D // LANES)], axis=1).astype(BF16).astype(F32)
            wide = Vb[s].astype(F32)
            scale = scale_of(wide)
            inner = jnp.mean(da * wide, -1, keepdims=True)
            dyv[part(t), :] = dyv[part(t), :] + (scale * da - wide * (scale * scale * scale * inner)).astype(BF16)

        for f in fetch("last", 0, 0) + loads:
            f.start()
        barrier(me, rs.peers())
        for f in loads:
            f.wait()
        for number, kind in enumerate(PASSES):
            count = COUNT[kind]
            following = PASSES[number + 1] if number + 1 < len(PASSES) else None
            if kind == "da":
                load_at0.start()
            if kind == "norm":
                for q in range(TOKENS // PART):
                    for f in hiddens(0, q):
                        f.start()
            if kind == "first":
                load_at0.wait()

            def body(t, carry, kind=kind, count=count, following=following):
                s = lax.rem(t, 2)
                for f in fetch(kind, t, s):
                    f.wait()

                @pl.when(t + 1 < count)
                def _():
                    for f in fetch(kind, t + 1, 1 - s):
                        f.start()

                if kind == "last":

                    @pl.when(t > 1)
                    def _():
                        save(t - 2, s).wait()

                if following:

                    @pl.when(t == count - 1)
                    def _():
                        if kind == "last":
                            save(t - 1, 1 - s).wait()
                        for f in fetch(following, 0, 0):
                            f.start()

                if kind in ("last", "first"):
                    hidden(kind, t, s)
                    if kind == "last":
                        save(t, s).start()
                    point(kind, t, 0, 1)
                    side(kind, t, s)
                    point(kind, t, SIDE, 1)
                    down(kind, t, s)
                    point(kind, t, DOWN, 1)
                else:
                    (d_a if kind == "da" else norm)(t, s)
                    point(kind, t, 0, 1)
                return carry

            lax.fori_loop(0, count, body, 0)
            if kind == "last":
                save(count - 1, (count - 1) % 2).wait()
        for u in range(3):
            for c in range(3):
                it.wait_sends(u, c, flips[0, u, c])

    any_space = pl.BlockSpec(memory_space=pl.ANY)
    return pl.pallas_call(
        kernel,
        out_shape=[jax.ShapeDtypeStruct((LAYERS, 3, 3, CHUNK, LANES), F32), jax.ShapeDtypeStruct((STEPS, TOKENS, 2 * TILE), BF16)],
        in_specs=[any_space] * 10,
        out_specs=[pl.BlockSpec(memory_space=pltpu.VMEM), any_space],
        scratch_shapes=[
            pltpu.VMEM((TOKENS, D), BF16),
            pltpu.VMEM((TOKENS, D), BF16),
            pltpu.VMEM((D, TOKENS), BF16),
            pltpu.VMEM((X_ROWS, LANES), F32),
            pltpu.VMEM((TILE, TOKENS), BF16),
            pltpu.VMEM((2, TOKENS, 2 * TILE), BF16),
            pltpu.VMEM((2, D, 2 * TILE), BF16),
            pltpu.VMEM((2, TILE, D), BF16),
            pltpu.VMEM((TOKENS // PART, 2, LT, PART, LANES), F32),
            pltpu.SemaphoreType.DMA((4,)),
            pltpu.SemaphoreType.DMA((5, 2)),
            pltpu.SemaphoreType.DMA((TOKENS // PART, 2)),
            rs.scratch(),
        ],
        compiler_params=pltpu.CompilerParams(collective_id=collective_id, has_side_effects=True, vmem_limit_bytes=VMEM_ALL),
        cost_estimate=pl.CostEstimate(flops=TOKENS * D * FF * 24, bytes_accessed=TOKENS * FF * 20, transcendentals=0),
        name="backward",
    )(gate0, up0, h1, a1, at1, at0, dy, wg, wu, wd)[0]


def solution(mesh):
    torus = Torus(4, 4, 8)
    count = float(LAYERS * 3 * D * FF)

    def step(x, dy, wg, wu, wd, mg, mu, md, vg, vu, vd):
        x, dy = x[0], dy[0]
        gate0, up0, h1, a1, at1, at0 = forward(x, wg, wu, wd)
        g = backward(torus, gate0, up0, h1, a1, at1, at0, dy, wg, wu, wd, 1)
        G, m, v = step_and_gather(torus, g, (wg, wu, wd), (mg, mu, md), (vg, vu, vd), count, 2)
        return (*unpack(torus, G), *m, *v)

    P = jax.sharding.PartitionSpec
    return jax.shard_map(
        step,
        mesh=mesh,
        in_specs=(P(("rep", "dp")),) * 2 + (P(),) * 3 + (P(None, "dp"),) * 6,
        out_specs=(P("rep"),) * 3 + (P("rep", "dp"),) * 6,
        check_vma=False,
    )
```

```python
import heapq
import jax
import jax.numpy as jnp
from jax import lax
from jax.experimental import pallas as pl
from jax.experimental.pallas import tpu as pltpu

F32, BF16 = jnp.float32, jnp.bfloat16
MESH = pl.DeviceIdType.MESH
RATE, LATENCY = 46.6e3, 2.3
TURN, ADD, HOP = 0.1, 2.0e6, 0.7
WAYS = (1, -1)
RING, CROSS, DIRECT = range(3)
NEVER, MARGIN, SWEEPS = 1e9, 0.5, 2


class Torus:
    def __init__(self, nx, ny, nz):
        self.n = {"x": nx, "y": ny, "z": nz}
        self.size = nx * ny * nz

    def here(self):
        return Here(self)


class Here:
    def __init__(self, torus):
        p, n = lax.axis_index("dp"), torus.n
        ny, nz = n["y"], n["z"]
        mine = {"z": lax.rem(p, nz), "y": lax.rem(lax.div(p, nz), ny), "x": lax.div(p, ny * nz)}
        step = {"z": 1, "y": nz, "x": ny * nz}
        self.at = {d: [mine[d]] + [lax.rem(mine[d] + i, n[d]) for i in range(1, n[d])] for d in n}
        self.to = {d: [p + (self.at[d][i] - mine[d]) * step[d] for i in range(n[d])] for d in n}

    def peer(self, dim, delta):
        return {"dp": self.to[dim][delta % len(self.to[dim])]}

    def up(self, dim, delta):
        return self.at[dim][delta % len(self.at[dim])]


ORDERS = ("zxy", "xyz", "yxz")


def hops(n, flip):
    far, near = n // 2, n - 1 - n // 2
    return {1: near, -1: far} if flip else {1: far, -1: near}


class Balance:
    def __init__(self):
        self.load = {}

    def flip(self, dim, n, size):
        plain = [self.load.get((dim, s), 0) + size * hops(n, False)[s] for s in WAYS]
        turned = [self.load.get((dim, s), 0) + size * hops(n, True)[s] for s in WAYS]
        flip = max(turned) < max(plain)
        self.load[dim, 1], self.load[dim, -1] = turned if flip else plain
        return flip


def simulate(actions, copies):
    links, arrived, order = {}, {}, []
    waiting = {a: set(needs) for a, (needs, _, _, _) in actions.items()}
    by_need = {}
    for a, (needs, _, _, _) in actions.items():
        for c in needs:
            by_need.setdefault(c, []).append(a)
    ready = [(actions[a][3], i, a) for i, a in enumerate(actions) if not waiting[a]]
    rank = {a: i for i, a in enumerate(actions)}
    heapq.heapify(ready)
    now, done = 0.0, {}
    while ready:
        at, _, a = heapq.heappop(ready)
        now = max(now, at) + actions[a][2]
        order.append(a)
        done[a] = now
        for c in [("action", a)] + list(actions[a][1]):
            if c[0] == "action":
                end = now
            else:
                link, size, extra = copies[c]
                start = max(now, links.get(link, 0.0))
                links[link] = start + size / RATE
                end = links[link] + LATENCY + extra
            for b in by_need.get(c, ()):
                waiting[b].discard(c)
                arrived[b] = max(arrived.get(b, 0.0), end)
                if not waiting[b]:
                    heapq.heappush(ready, (max(arrived[b], actions[b][3]), rank[b], b))
    assert len(order) == len(actions), (len(order), len(actions))
    return order, now


def place(actions, copies, segments):
    links, known, left, slots, open_keys = {}, {}, dict(actions), {}, set()
    now = 0.0

    def do(a, where):
        nonlocal now
        _, sends, cost = left.pop(a)
        now += cost
        known["action", a] = now
        for c in sends:
            link, size, extra = copies[c]
            links[link] = max(now, links.get(link, 0.0)) + size / RATE
            known[c] = links[link] + LATENCY + extra
        where.append(a)

    def drain(where, allowed, wait):
        nonlocal now
        while True:
            able = [(max([known.get(c, NEVER) for c in actions[a][0]], default=0.0), i, a) for i, a in enumerate(left) if allowed(a)]
            best, _, a = min(able, default=(NEVER, 0, None))
            if best >= NEVER or not wait and best + MARGIN > now:
                return
            now = max(now, best)
            do(a, where)

    for key, cost, writes, whole in segments:
        now += cost
        slots[key] = ([], [])
        others = {(l, u, c) for (l, u), c in writes}
        drain(slots[key][0], lambda a: any(a[0][0][1] == u and a[0][1] == c and a[0][0][0] > l for l, u, c in others), True)
        open_keys |= set(whole)
        drain(slots[key][1], lambda a: a[1] != "start" or a[0] in open_keys, False)
    drain(slots[segments[-1][0]][1], lambda a: True, True)
    assert not left
    place.took = now
    return slots


def barrier(me, peers):
    sem = pltpu.get_barrier_semaphore()
    for dim, delta in peers:
        pl.semaphore_signal(sem, inc=1, device_id=me.peer(dim, delta), device_id_type=MESH)
    pl.semaphore_wait(sem, len(peers))


def both_ways(torus, dim):
    n = torus.n[dim]
    return [] if n == 1 else [(dim, 1)] if n == 2 else [(dim, 1), (dim, -1)]


def all_others(torus, dim):
    return [(dim, d) for d in range(1, torus.n[dim])]


class ReduceScatter:
    LANES = (2, 1, 1)

    def __init__(self, torus, rows, units):
        self.t, self.rows, self.units = torus, rows, units
        self.dims = [tuple(order) for order in ORDERS]
        self.nslots = max(self.base(c, DIRECT, 0) + self.sizes(c)[DIRECT] - 1 for c in range(3))

    def sizes(self, c):
        return [self.t.n[d] for d in self.dims[c]]

    def here(self, c):
        return [self.me.up(d, 0) for d in self.dims[c]]

    def base(self, c, phase, lane):
        n = self.sizes(c)
        return sum((n[i] - 1) * self.LANES[i] for i in range(phase)) + lane * (n[phase] - 1)

    def peers(self):
        full = {dims[DIRECT] for dims in self.dims}
        out = []
        for dim in "xyz":
            out += all_others(self.t, dim) if dim in full else both_ways(self.t, dim)
        return out

    def credit_peers(self, c):
        a, b, d = self.dims[c]
        return both_ways(self.t, a) + both_ways(self.t, b) + all_others(self.t, d)

    def scratch(self):
        n = self.t.n
        t, r1, r2, r3, k2, k3 = [], [], [], [], [], []
        for dims in self.dims:
            n1, n2, n3 = (n[d] for d in dims)
            tail = (self.rows, 128)
            t.append(pltpu.VMEM((self.units, n1, n2 * n3) + tail, BF16))
            r1.append(pltpu.VMEM((self.units, max(n1 - 1, 1), n2 * n3) + tail, BF16))
            r2.append(pltpu.VMEM((self.units, max(n2 - 1, 1), n3) + tail, BF16))
            r3.append(pltpu.VMEM((self.units, max(n3 - 1, 1)) + tail, BF16))
            k2.append(pltpu.VMEM((self.units, n3) + tail, F32))
            k3.append(pltpu.VMEM((self.units,) + tail, F32))
        sems = [pltpu.SemaphoreType.DMA((self.units, 3, self.nslots)), pltpu.SemaphoreType.DMA((self.units, 3, self.nslots)), pltpu.SemaphoreType.REGULAR((self.units, 3))]
        return [t, r1, r2, r3, k2, k3] + sems

    def slot(self, c, phase, sign, h):
        return h if sign > 0 else self.sizes(c)[phase] - 2 - h

    def flips(self, balance, c):
        n1, n2, n3 = self.sizes(c)
        block, (a, b, d) = self.rows * 256, self.dims[c]
        for rel in range(1, n3):
            link = d, 1 if rel <= n3 // 2 else -1
            balance.load[link] = balance.load.get(link, 0) + block * min(rel, n3 - rel)
        ring = [balance.flip(a, n1, block * n2 * n3 // self.LANES[RING]) for _ in range(self.LANES[RING])]
        return ring, [balance.flip(b, n2, block * n3)]

    def plan(self, unit, c, flip):
        n = self.sizes(c)
        n1, n2, n3 = n
        block = self.rows * 256
        size = [block * n2 * n3 // self.LANES[RING], block * n3, block]
        actions, copies = {}, {}
        key = (unit, c)

        def send(phase, lane, sign, h):
            cid = ("copy", key, phase, lane, sign, h)
            copies[cid] = ((self.dims[c][phase], sign), size[phase], 0)
            return cid

        first, last = [[], []], [[], []]
        for phase in (RING, CROSS):
            for lane, turned in enumerate(flip[phase]):
                k = hops(n[phase], turned)
                ways = [s for s in WAYS if k[s]]
                first[phase] += [send(phase, lane, s, k[s] - 1) for s in ways]
                last[phase] += [("copy", key, phase, lane, s, 0) for s in ways]
                for s in ways:
                    for h in range(k[s] - 1, 0, -1):
                        actions[key, "step", phase, lane, s, h] = ([("copy", key, phase, lane, s, h)], [send(phase, lane, s, h - 1)], size[phase] / ADD)
        direct = []
        for rel in range(1, n3):
            cid = ("copy", key, DIRECT, 0, 0, rel)
            far = min(rel, n3 - rel)
            copies[cid] = ((self.dims[c][DIRECT], 1 if rel <= n3 // 2 else -1), size[DIRECT] * far, HOP * (far - 1))
            direct.append(cid)
        sends = first + [direct, []]
        actions[key, "start"] = ([], sends[RING], TURN)
        before = (key, "start")
        for phase, needs in enumerate(last + [direct]):
            a = (key, "end", phase)
            actions[a] = (needs + [("action", before)], sends[phase + 1], size[phase] * self.LANES[phase] / ADD + TURN)
            before = a
        return actions, copies

    def bind(self, me, refs):
        self.me, (self.T, self.R1, self.R2, self.R3, self.K2, self.K3, self.ssem, self.rsem, self.credit) = me, refs
        return self

    def remote(self, u, c, phase, lane, sign, h):
        n1, n2, n3 = self.sizes(c)
        d1, d2, d3 = self.dims[c]
        up = self.me.up
        mine = self.T[c].at[u]
        slot = h - 1 if phase == DIRECT else self.slot(c, phase, sign, h)
        if phase == RING:
            part = n2 * n3 // self.LANES[RING]
            blocks = pl.ds(lane * part, part)
            src, dst = mine.at[up(d1, sign * (h + 1)), blocks], self.R1[c].at[u, slot, blocks]
        elif phase == CROSS:
            src, dst = mine.at[up(d1, 0), pl.ds(up(d2, sign * (h + 1)) * n3, n3)], self.R2[c].at[u, slot]
        else:
            sign = h
            src, dst = mine.at[up(d1, 0), up(d2, 0) * n3 + up(d3, h)], self.R3[c].at[u, slot]
        s = self.base(c, phase, lane) + slot
        to = self.me.peer(self.dims[c][phase], sign)
        return pltpu.make_async_remote_copy(src_ref=src, dst_ref=dst, send_sem=self.ssem.at[u, c, s], recv_sem=self.rsem.at[u, c, s], device_id=to, device_id_type=MESH)

    def all_sends(self, c, flip):
        n = self.sizes(c)
        out = []
        for phase in (RING, CROSS):
            for lane, turned in enumerate(flip[phase]):
                k = hops(n[phase], turned)
                out += [(phase, lane, s, h) for s in WAYS for h in range(k[s])]
        return out + [(DIRECT, 0, 0, rel) for rel in range(1, n[DIRECT])]

    def run(self, u, c, flip, what, store):
        n = self.sizes(c)
        n1, n2, n3 = n
        m1, m2, m3 = self.here(c)
        T, R1, R2, R3 = (r[c].at[u] for r in (self.T, self.R1, self.R2, self.R3))
        K2, K3 = self.K2[c].at[u], self.K3[c].at[u]
        mine = T.at[m1]
        wide = lambda v: v.astype(F32)
        go = lambda *a: self.remote(u, c, *a)

        def loop(count, body):
            def one(i, carry):
                body(i)
                return carry

            lax.fori_loop(0, count, one, 0)

        def line(q):
            return pl.ds(q * n3, n3)

        def ways(phase):
            for lane, turned in enumerate(flip[phase]):
                k = hops(n[phase], turned)
                for s in WAYS:
                    if k[s]:
                        yield lane, s, k[s]

        def sends(phase):
            for lane, s, k in ways(phase):
                go(phase, lane, s, k - 1).start()

        def arrived(phase):
            got = set()
            for lane, s, _ in ways(phase):
                go(phase, lane, s, 0).wait_recv()
                got.add(self.slot(c, phase, s, 0))
            return sorted(got)

        kind, *where = what
        if kind == "start":
            sends(RING)
        elif kind == "step":
            phase, lane, s, h = where
            go(*where).wait_recv()
            slot = self.slot(c, phase, s, h)
            q = self.me.up(self.dims[c][phase], s * h)
            if phase == RING:
                lines = n2 // self.LANES[RING]

                def add(i):
                    b = line(lane * lines + i)
                    T[q, b] = (wide(T[q, b]) + wide(R1[slot, b])).astype(BF16)

                loop(lines, add)
            else:
                mine[line(q)] = (wide(mine[line(q)]) + wide(R2[slot])).astype(BF16)
            go(phase, lane, s, h - 1).start()
        elif where == [RING]:
            got = arrived(RING)

            def total(b):
                return sum((wide(R1[g, b]) for g in got), wide(mine[b]))

            def others(i):
                b = line(lax.rem(m2 + 1 + i, n2))
                mine[b] = total(b).astype(BF16)

            loop(n2 - 1, others)
            sends(CROSS)
            K2[...] = total(line(m2))
        elif where == [CROSS]:
            got = arrived(CROSS)
            total = sum((wide(R2[g]) for g in got), K2[...])
            K2[...] = total
            mine[line(m2)] = total.astype(BF16)
            for rel in range(1, n3):
                go(DIRECT, 0, 0, rel).start()
            K3[...] = K2[m3]
        else:
            for rel in range(1, n3):
                go(DIRECT, 0, 0, rel).wait_recv()
            store(sum((wide(R3[i]) for i in range(n3 - 1)), K3[...]).astype(BF16).astype(F32))

    def wait_sends(self, u, c, flip):
        for a in self.all_sends(c, flip):
            self.remote(u, c, *a).wait_send()

    def give_credit(self, u, c):
        for dim, delta in self.credit_peers(c):
            pl.semaphore_signal(self.credit.at[u, c], inc=1, device_id=self.me.peer(dim, delta), device_id_type=MESH)

    def take_credit(self, u, c):
        pl.semaphore_wait(self.credit.at[u, c], len(self.credit_peers(c)))


class AllGather:
    def __init__(self, torus, block_bytes, split=2):
        self.t, self.bytes, self.split = torus, block_bytes, split
        self.dims = [tuple(order) for order in ORDERS]
        self.flip, self.balance = {}, Balance()
        self.build()
        for key in list(self.flip) * SWEEPS:
            took = self.took
            self.flip[key] = not self.flip[key]
            self.build()
            if self.took >= took:
                self.flip[key] = not self.flip[key]
        self.build()

    def build(self):
        self.copies, self.actions, self.index = {}, {}, {}
        for c in range(3):
            self.plan(c)
        self.order, self.took = simulate({a: (*v, 0) for a, v in self.actions.items()}, self.copies)

    def peers(self):
        return [p for dim in "xyz" for p in both_ways(self.t, dim)]

    def pieces(self, c, j):
        n3 = self.t.n[self.dims[c][DIRECT]]
        return n3 if not j else self.split if n3 % self.split == 0 else 1

    def size(self, c, phase, j):
        line = self.bytes * self.t.n[self.dims[c][DIRECT]]
        return self.bytes if phase == DIRECT else line // self.pieces(c, 1 if phase == CROSS else j)

    def k(self, c, phase, j, i):
        dim = self.dims[c][phase]
        key = (c, phase, j, i)
        if key not in self.flip:
            self.flip[key] = self.balance.flip(dim, self.t.n[dim], self.size(c, phase, j))
        return hops(self.t.n[dim], self.flip[key])

    def plan(self, c):
        n1, n2, n3 = (self.t.n[d] for d in self.dims[c])

        def send(where, s, h):
            phase, j, _ = where
            cid = (c, where, s, h)
            self.copies[cid] = ((self.dims[c][phase], s), self.size(c, phase, j), 0)
            self.index[cid] = len(self.index)
            return cid

        def own(*where):
            k = self.k(c, *where)
            return [send(where, s, 1) for s in WAYS if k[s]]

        def passing(*where):
            k = self.k(c, *where)
            for s in WAYS:
                for h in range(1, k[s] + 1):
                    yield s, h, (c, "pass", where, s, h), [(c, where, s, h)], [send(where, s, h + 1)] if h < k[s] else []

        def act(a, needs, sends):
            self.actions[a] = (needs, sends, TURN / 2)

        act((c, "start"), [], own(DIRECT, 0, 0) + own(RING, 0, 0))
        got = [("action", (c, "start"))]
        for s, h, a, needs, sends in passing(DIRECT, 0, 0):
            act(a, needs, sends + own(RING, 0, (-s * h) % n3))
            got.append(("action", a))
        parts = range(self.pieces(c, 1))
        act((c, "line"), got, [x for i in parts for x in own(CROSS, 0, i)])
        for i in parts:
            for s, h, a, needs, sends in passing(CROSS, 0, i):
                after = (-s * h) % n2, i
                if c:
                    act(a, needs, sends + own(RING, *after))
                else:
                    act(a, needs, sends)
                    act((c, "later", *after), [("action", x) for x in (a, (1, "line"), (2, "line"))], own(RING, *after))
        for j in range(n2):
            for i in range(self.pieces(c, j)):
                for _, _, a, needs, sends in passing(RING, j, i):
                    act(a, needs, sends)

    def bind(self, me, G, ssem, rsem):
        self.me, self.G, self.ssem, self.rsem = me, G, ssem, rsem
        return self

    def remote(self, cid, back):
        c, (phase, j, i), s, h = cid
        d1, d2, d3 = self.dims[c]
        n3, up = self.t.n[d3], self.me.up
        off = s * (back - h)
        G = self.G[c]
        if phase == DIRECT:
            ref = G.at[up(d1, 0), up(d2, 0) * n3 + up(d3, off)]
        elif phase == CROSS:
            size = n3 // self.pieces(c, 1)
            ref = G.at[up(d1, 0), pl.ds(up(d2, off) * n3 + i * size, size)]
        elif j == 0:
            ref = G.at[up(d1, off), up(d2, 0) * n3 + up(d3, i)]
        else:
            size = n3 // self.pieces(c, j)
            ref = G.at[up(d1, off), pl.ds(up(d2, j) * n3 + i * size, size)]
        x = self.index[cid]
        return pltpu.make_async_remote_copy(src_ref=ref, dst_ref=ref, send_sem=self.ssem.at[x], recv_sem=self.rsem.at[x], device_id=self.me.peer(self.dims[c][phase], s), device_id_type=MESH)

    def run(self, a):
        needs, sends, _ = self.actions[a]
        for cid in needs:
            if cid in self.index:
                self.remote(cid, 0).wait_recv()
        for cid in sends:
            self.remote(cid, 1).start()

    def wait_sends(self):
        for cid in self.copies:
            self.remote(cid, 1).wait_send()


MIB = 2**20
VMEM_ALL = 67043328
LAYERS, D, FF = 2, 896, 2560
LANES, ROWS, CHUNK = 128, 144, 48
HIGH = {0: 7, 1: 7, 2: 20}
WIDE = {0: FF, 1: FF, 2: D}
WINDOW = (16, 16, 24)


HALVES, RING_TILES = 2, 8
TOKENS, TILE, PART = 2048, 256, 512
LT, STEPS = TILE // LANES, FF // TILE
HALF = STEPS // HALVES


def home(u, ct):
    if u == HALVES:
        return u, ct
    t, k = divmod(ct, 2 * LT)
    m, j = divmod(k, LT)
    return m, (u * HALF + t) * LT + j


def tiles(u):
    high, wide = HIGH[u], WIDE[u] // LANES
    out = []
    for k in range(ROWS // 8):
        ct, row = divmod(8 * k, high)
        out.append((ct, row, min(8, high - row), ct + 1 < wide))
    return out


def pack(torus, u, X, base, parts, first, count, outs):
    high, ny, nz = HIGH[u], torus.n["y"], torus.n["z"]
    sub = lax.broadcasted_iota(jnp.int32, (8, LANES), 0)
    got = tiles(u)

    def body(line, carry):
        x, y = lax.div(first + line, ny), lax.rem(first + line, ny)
        top = pl.multiple_of(line * (high * nz), 8)

        def piece(z, ct, row, whole, more):
            a = X[pl.ds(top + (base(ct) + high * z + row), 8), :]
            if whole == 8:
                return a
            b = X[pl.ds(top + (base(ct + 1) + high * z - whole), 8), :] if more else jnp.zeros((8, LANES), F32)
            return jnp.where(sub < whole, a, b)

        for z in range(nz):
            at = {"x": x, "y": y, "z": z}
            for j in parts:
                both = jnp.concatenate([piece(z, *got[2 * j]), piece(z, *got[2 * j + 1])], axis=0).astype(BF16)
                c, r = divmod(16 * j, CHUNK)
                d1, d2, d3 = ORDERS[c]
                outs[c][at[d1], at[d2] * torus.n[d3] + at[d3], pl.ds(r, 16), :] = both
        return carry

    lax.fori_loop(0, count, body, 0)


def pieces_shapes(torus, dtype, *mid):
    out = []
    for order in ORDERS:
        a, b, d = (torus.n[x] for x in order)
        out.append(jax.ShapeDtypeStruct((a, b * d) + mid + (CHUNK, LANES), dtype))
    return out


def step_and_gather(torus, g, w, m, v, count, collective_id):
    ag = AllGather(torus, LAYERS * 3 * CHUNK * 256)
    dims = "zxy"
    slots = {d: torus.n[d] - 1 for d in dims}

    def window(p, x):
        rows = WINDOW[x]
        first = lax.div(p * HIGH[x], 8) * 8
        return pl.multiple_of(jnp.minimum(first, HIGH[x] * torus.size - rows), 8), rows

    def kernel(g_ref, *refs):
        w_in, m_in, v_in, G, m_out, v_out = (refs[i : i + 3] for i in range(0, 18, 3))
        flat, wflat, part, E, esend, erecv, ssem, rsem, win, wide_win, wsem = refs[18:]
        me = torus.here()
        p = lax.axis_index("dp")
        loads = []
        for x in range(3):
            first, rows = window(p, x)
            loads.append(pltpu.make_async_copy(w_in[x].at[:, pl.ds(first, rows)], win[x], wsem.at[x]))
            loads[x].start()
        barrier(me, [p for d in "xyz" for p in all_others(torus, d)])
        for x in range(3):
            loads[x].wait()
            for lt in range(WIDE[x] // LANES):
                wide_win[x][:, lt] = win[x][:, :, pl.ds(lt * LANES, LANES)].astype(F32)
        acc = jnp.zeros((8, LANES), F32)
        for l in range(LAYERS):
            for u in range(3):
                for c in range(3):
                    value = g_ref[l, u, c]
                    flat[l, u, pl.ds(c * CHUNK, CHUNK), :] = value
                    for r in range(0, CHUNK, 8):
                        acc = acc + value[r : r + 8] * value[r : r + 8]
        part[0] = acc
        base = 0
        for i, d in enumerate(dims):
            n = torus.n[d]
            copies = []
            for rel in range(1, n):
                s = base + rel - 1
                copies.append(pltpu.make_async_remote_copy(src_ref=part.at[i], dst_ref=E.at[s], send_sem=esend.at[s], recv_sem=erecv.at[s], device_id=me.peer(d, rel), device_id_type=MESH))
            for copy in copies:
                copy.start()
            total = part[i]
            for rel in range(1, n):
                copies[rel - 1].wait_recv()
                total = total + E[base + rel - 1]
            part[i + 1] = total
            for copy in copies:
                copy.wait_send()
            base += n - 1
        mean = jnp.sum(part[3], keepdims=True) / count
        factor = jnp.minimum(1.0, 0.5 * lax.rsqrt(mean + 1e-30))
        for l in range(LAYERS):
            for u in range(3):
                high = HIGH[u]
                wflat[l, u, pl.ds(ROWS - 8, 8), :] = jnp.zeros((8, LANES), F32)
                for ct in range(WIDE[u] // LANES):
                    x, lt = home(u, ct)
                    at = (slice(None), l, pl.ds(lt * LANES, LANES))
                    grad = flat[l, u, pl.ds(ct * high, high), :] * factor
                    new_m = 0.9 * m_in[x][at] + 0.1 * grad
                    new_v = 0.95 * v_in[x][at] + 0.05 * grad * grad
                    wide = wide_win[x][l, lt, pl.ds(p * high - window(p, x)[0], high), :]
                    new_w = wide - 0.02 * (new_m * lax.rsqrt(new_v + 1e-8) + 0.1 * wide)
                    m_out[x][at] = new_m
                    v_out[x][at] = new_v
                    wflat[l, u, pl.ds(ct * high, high), :] = new_w
        it = ag.bind(me, G, ssem, rsem)
        for c in range(3):
            n = [torus.n[d] for d in ORDERS[c]]
            at = [me.up(d, 0) for d in ORDERS[c]]
            for l in range(LAYERS):
                for u in range(3):
                    G[c][at[0], at[1] * n[2] + at[2], l, u] = wflat[l, u, pl.ds(c * CHUNK, CHUNK), :].astype(BF16)
        for a in ag.order:
            it.run(a)
        it.wait_sends()

    vmem = pl.BlockSpec(memory_space=pltpu.VMEM)
    nsum = sum(slots.values())
    shapes = pieces_shapes(torus, BF16, LAYERS, 3)
    turn = lambda ts: [jnp.transpose(t, (1, 0, 2)) for t in ts]
    m, v = turn(m), turn(v)
    f32 = [jax.ShapeDtypeStruct(t.shape, F32) for t in m]
    k = len(ag.copies)
    got = pl.pallas_call(
        kernel,
        out_shape=[pltpu.MemorySpace.VMEM(s.shape, s.dtype) for s in shapes] + f32 * 2,
        in_specs=[vmem] + [pl.BlockSpec(memory_space=pl.ANY)] * 3 + [vmem] * 6,
        out_specs=[vmem] * 9,
        scratch_shapes=[
            pltpu.VMEM((LAYERS, 3, ROWS, LANES), F32),
            pltpu.VMEM((LAYERS, 3, ROWS, LANES), F32),
            pltpu.VMEM((4, 8, LANES), F32),
            pltpu.VMEM((nsum, 8, LANES), F32),
            pltpu.SemaphoreType.DMA((nsum,)),
            pltpu.SemaphoreType.DMA((nsum,)),
            pltpu.SemaphoreType.DMA((k,)),
            pltpu.SemaphoreType.DMA((k,)),
            [pltpu.VMEM((LAYERS, WINDOW[x], WIDE[x]), BF16) for x in range(3)],
            [pltpu.VMEM((LAYERS, WIDE[x] // LANES, WINDOW[x], LANES), F32) for x in range(3)],
            pltpu.SemaphoreType.DMA((3,)),
        ],
        compiler_params=pltpu.CompilerParams(collective_id=collective_id, has_side_effects=True, vmem_limit_bytes=26 * MIB),
        name="step_and_gather",
    )(g, *w, *m, *v)
    return got[:3], turn(got[3:6]), turn(got[6:])


def unpack(torus, G):
    nx, ny, nz = (torus.n[d] for d in "xyz")
    pair = 2
    group = pair * nz
    groups = torus.size // group
    pairs = ny // pair

    def kernel(g0, g1, g2, *refs):
        outs, Z, Y = refs[:3], refs[3], refs[4]
        l, s = pl.program_id(0), pl.program_id(1)
        corner = {"x": lax.div(s, pairs), "y": lax.rem(s, pairs) * pair, "z": 0}
        for u in range(3):
            high, wide = HIGH[u], WIDE[u] // LANES
            for i in range(group):
                y, z = divmod(i, nz)
                at = corner | {"y": corner["y"] + y, "z": z}
                for c, ref in enumerate((g0, g1, g2)):
                    a, b, d = ORDERS[c]
                    Z[i, pl.ds(c * CHUNK, CHUNK), :] = ref[at[a], at[b] * torus.n[d] + at[d], l, u].astype(F32)
            for i in range(group):
                for ct in range(wide):
                    for r in range(0, high, 8):
                        Y[ct, pl.ds(high * i + r, 8), :] = Z[i, pl.ds(high * ct + r, 8), :]
            rows = high * group
            for ct in range(wide):
                x, lt = home(u, ct)
                outs[x][0, :, pl.ds(lt * LANES, LANES)] = Y[ct, pl.ds(0, rows), :].astype(BF16)

    shapes = [(LAYERS, HIGH[u] * torus.size, WIDE[u]) for u in range(3)]
    return pl.pallas_call(
        kernel,
        grid=(LAYERS, groups),
        out_shape=[jax.ShapeDtypeStruct(s, BF16) for s in shapes],
        in_specs=[pl.BlockSpec(memory_space=pltpu.VMEM)] * 3,
        out_specs=[pl.BlockSpec((1, HIGH[u] * group, WIDE[u]), lambda l, s: (l, s, 0)) for u in range(3)],
        scratch_shapes=[pltpu.VMEM((group, ROWS + 8, LANES), F32), pltpu.VMEM((FF // LANES, HIGH[2] * group + 8, LANES), F32)],
        compiler_params=pltpu.CompilerParams(vmem_limit_bytes=26 * MIB),
        name="unpack",
    )(*G)


NN, NT, TN = ((1,), (0,)), ((1,), (1,)), ((0,), (0,))


def dot(a, b, dims=NN):
    return lax.dot_general(a, b, (dims, ((), ())), preferred_element_type=F32)


def scale_of(wide):
    return lax.rsqrt(jnp.mean(wide * wide, -1, keepdims=True) + 1e-6)


def normed_into(h_ref, a_ref, t_ref):
    for r in range(0, TOKENS, TILE):
        wide = h_ref[pl.ds(r, TILE), :].astype(F32)
        a = (wide * scale_of(wide)).astype(BF16)
        a_ref[pl.ds(r, TILE), :] = a
        t_ref[:, pl.ds(r, TILE)] = a.T


def forward(x, wg, wu, wd):
    steps = STEPS

    def kernel(x_ref, wg_ref, wu_ref, wd_ref, gate_ref, up_ref, h_ref, a_ref, at_ref, xt_ref, xa, acc):
        t = pl.program_id(0)

        @pl.when(t == 0)
        def _():
            normed_into(x_ref, xa, xt_ref)
            acc[...] = jnp.zeros_like(acc)

        for r in range(0, TOKENS, PART):
            rows = pl.ds(r, PART)
            a = xa[rows, :]
            both = dot(a, jnp.concatenate([wg_ref[0], wu_ref[0]], axis=1))
            gate, up = both[:, :TILE], both[:, TILE:]
            for k in range(LT):
                lanes = slice(k * LANES, (k + 1) * LANES)
                gate_ref[k, rows, :] = gate[:, lanes]
                up_ref[k, rows, :] = up[:, lanes]
            mid = (jax.nn.silu(gate) * up).astype(BF16)
            acc[rows, :] += dot(mid, wd_ref[0])

        @pl.when(t == steps - 1)
        def _():
            for r in range(0, TOKENS, TILE):
                rows = pl.ds(r, TILE)
                h_ref[rows, :] = x_ref[rows, :] + acc[rows, :].astype(BF16)
            normed_into(h_ref, a_ref, at_ref)

    whole = pl.BlockSpec(memory_space=pltpu.VMEM)
    cols = pl.BlockSpec((1, D, TILE), lambda t: (0, 0, t))
    saved = pl.BlockSpec((LT, TOKENS, LANES), lambda t: (t, 0, 0))
    return pl.pallas_call(
        kernel,
        grid=(steps,),
        out_shape=[jax.ShapeDtypeStruct((FF // LANES, TOKENS, LANES), F32)] * 2 + [jax.ShapeDtypeStruct((TOKENS, D), BF16)] * 2 + [jax.ShapeDtypeStruct((D, TOKENS), BF16)] * 2,
        in_specs=[whole, cols, cols, pl.BlockSpec((1, TILE, D), lambda t: (0, t, 0))],
        out_specs=[saved] * 2 + [whole] * 4,
        scratch_shapes=[pltpu.VMEM((TOKENS, D), BF16), pltpu.VMEM((TOKENS, D), F32)],
        compiler_params=pltpu.CompilerParams(vmem_limit_bytes=60 * MIB),
        cost_estimate=pl.CostEstimate(flops=6 * TOKENS * D * FF, bytes_accessed=10 * TOKENS * FF, transcendentals=0),
        name="forward",
    )(x, wg, wu, wd)


def hidden_back(gate, up, d):
    s = jax.nn.sigmoid(gate)
    act = gate * s
    return (act * up).astype(BF16), (d * up * (s + act * (1.0 - s))).astype(BF16), (d * act).astype(BF16)


GAP = 24
SIDE_STRIDE, DOWN_STRIDE = D + GAP, FF // HALVES + GAP
DOWN_BASE = RING_TILES * SIDE_STRIDE
X_ROWS = DOWN_BASE + D // LANES * DOWN_STRIDE
COST = {"last": (3.7, 2.6, 1.3), "first": (1.6, 2.6, 1.3), "da": (2.4,), "norm": (0.5,)}
PACK_DOWN = 1.0
WHOLE = ((0,), (1, 2), (3, 4), (5, 6), (7, 8))
COLOUR = {1: 0, 3: 1, 4: 2}
PASSES = ("last", "da", "norm", "first")
COUNT = {"last": STEPS, "da": STEPS, "norm": TOKENS // TILE, "first": STEPS}
SIDE, DOWN = 1, 2


def timeline():
    out = []
    for kind in PASSES:
        layer = {"last": 1, "first": 0}.get(kind)
        for t in range(COUNT[kind]):
            half, tt = divmod(t, HALF)
            for i, cost in enumerate(COST[kind]):
                writes, whole = [], []
                if i == SIDE:
                    unit = (layer, half)
                    writes = [(unit, c) for c in range(3)] if tt == 0 else []
                    whole = [(unit, COLOUR[tt])] if tt in COLOUR else []
                if i == DOWN and tt == HALF - 1:
                    cost += PACK_DOWN
                    mine = [((layer, HALVES), c) for c in range(3)]
                    writes, whole = (mine, []) if half == 0 else ([], mine)
                out.append(((kind, t, i), cost, writes, whole))
    return out


def hidden_back(gate, up, d):
    s = jax.nn.sigmoid(gate)
    act = gate * s
    return (act * up).astype(BF16), (d * up * (s + act * (1.0 - s))).astype(BF16), (d * act).astype(BF16)


def backward(torus, gate0, up0, h1, a1, at1, at0, dy, wg, wu, wd, collective_id):
    rs = ReduceScatter(torus, CHUNK, 3)
    actions, copies, balance, flips = {}, {}, Balance(), {}
    for l in range(LAYERS):
        for u in range(3):
            for c in range(3):
                flips[l, u, c] = rs.flips(balance, c)
                got, sent = rs.plan((l, u), c, flips[l, u, c])
                copies |= sent
                actions |= got
                if l:
                    key = ((l, u), c)
                    actions[key, "free"] = ([("action", (key, "end", DIRECT))], [], TURN)
    slots = place(actions, copies, timeline())
    lines = torus.n["x"] * torus.n["y"]

    def kernel(gate_ref, up_ref, h1_ref, a1_ref, at1_ref, at0_ref, dy_ref, wg_ref, wu_ref, wd_ref, out, both_ref, dyv, av, at, X, Mb, Db, Wb, Vb, Hb, once, pair, hsem, rsc):
        me = torus.here()
        it = rs.bind(me, rsc)
        copy = pltpu.make_async_copy
        loads = [copy(src, dst, once.at[i]) for i, (src, dst) in enumerate(((dy_ref, dyv), (a1_ref, av), (at1_ref, at)))]
        load_at0 = copy(at0_ref, at, once.at[3])

        def part(i):
            return pl.ds(i * TILE, TILE)

        def sides(layer, t, s):
            return [copy(ref.at[layer, :, part(t)], Wb.at[s, :, part(k)], pair.at[k, s]) for k, ref in enumerate((wg_ref, wu_ref))]

        def fetch(kind, t, s):
            both, rows = pair.at[2, s], pair.at[3, s]
            if kind == "last":
                return sides(1, t, s) + [copy(wd_ref.at[1, part(t)], Vb.at[s], rows)]
            if kind == "da":
                return sides(1, t, s) + [copy(both_ref.at[t], Db.at[s], both)]
            if kind == "norm":
                return [copy(h1_ref.at[part(t)], Vb.at[s], rows)]
            return [copy(wd_ref.at[0, part(t)], Vb.at[s], rows)]

        def save(t, s):
            return copy(Db.at[s], both_ref.at[t], pair.at[4, s])

        def hiddens(t, q):
            return [copy(ref.at[pl.ds(t * LT, LT), pl.ds(q * PART, PART)], Hb.at[q, k], hsem.at[q, k]) for k, ref in enumerate((gate_ref, up_ref))]

        def act(a):
            ((l, u), c), what = a[0], a[1:]
            if what[0] == "free":
                it.wait_sends(u, c, flips[l, u, c])
                it.give_credit(u, c)
                return
            if what[0] == "start" and l == 0:
                it.take_credit(u, c)

            def store(value):
                out[l, u, c] = value

            it.run(u, c, flips[l, u, c], what, store)

        def point(kind, t, i, which):
            for k in range(COUNT[kind]):
                if slots[kind, k, i][which]:

                    @pl.when(t == k)
                    def _(k=k):
                        for a in slots[kind, k, i][which]:
                            act(a)

        def hidden(kind, t, s):
            for q in range(TOKENS // PART):
                rows = pl.ds(q * PART, PART)
                if kind == "last":
                    both = dot(av[rows, :], Wb[s])
                    gate, up = both[:, :TILE], both[:, TILE:]
                else:
                    for f in hiddens(t, q):
                        f.wait()
                    gate, up = (jnp.concatenate([Hb[q, k, j] for j in range(LT)], axis=1) for k in range(2))
                d = dot(dyv[rows, :], Vb[s], NT).astype(BF16).astype(F32)
                mid, Db[s, rows, part(0)], Db[s, rows, part(1)] = hidden_back(gate, up, d)
                Mb[:, rows] = mid.T
                if kind == "first":

                    @pl.when(t + 1 < STEPS)
                    def _(q=q):
                        for f in hiddens(t + 1, q):
                            f.start()

        def side(kind, t, s):
            half, tt = lax.div(t, HALF), lax.rem(t, HALF)
            got = dot(at[...], Db[s])
            for k in range(2 * LT):
                X[pl.ds((lax.rem(tt, 2) * 2 * LT + k) * SIDE_STRIDE + 8, D), :] = got[:, k * LANES : (k + 1) * LANES]
            point(kind, t, SIDE, 0)
            for v, parts in enumerate(WHOLE):

                @pl.when(tt == v)
                def _(parts=parts):
                    pack(torus, 0, X, lambda ct: ct % RING_TILES * SIDE_STRIDE + 8, parts, 0, lines, [T.at[half] for T in it.T])

        def down(kind, t, s):
            half, tt = lax.div(t, HALF), lax.rem(t, HALF)
            got = dot(Mb[...], dyv[...])
            for ct in range(D // LANES):
                X[pl.ds(DOWN_BASE + ct * DOWN_STRIDE + 8 + tt * TILE, TILE), :] = got[:, ct * LANES : (ct + 1) * LANES]
            point(kind, t, DOWN, 0)

            @pl.when(tt == HALF - 1)
            def _():
                some = lines // HALVES
                pack(torus, HALVES, X, lambda ct: DOWN_BASE + ct * DOWN_STRIDE + 8, range(ROWS // 16), half * some, some, [T.at[HALVES] for T in it.T])

        def d_a(t, s):
            for r in range(0, TOKENS, PART):
                got = dot(Db[s, pl.ds(r, PART), :], Wb[s], NT)
                for ct in range(D // LANES):
                    rows = pl.ds(ct * TOKENS + r, PART)
                    X[rows, :] = jnp.where(t == 0, 0.0, X[rows, :]) + got[:, ct * LANES : (ct + 1) * LANES]

        def norm(t, s):
            da = jnp.concatenate([X[pl.ds(ct * TOKENS + t * TILE, TILE), :] for ct in range(D // LANES)], axis=1).astype(BF16).astype(F32)
            wide = Vb[s].astype(F32)
            scale = scale_of(wide)
            inner = jnp.mean(da * wide, -1, keepdims=True)
            dyv[part(t), :] = dyv[part(t), :] + (scale * da - wide * (scale * scale * scale * inner)).astype(BF16)

        for f in fetch("last", 0, 0) + loads:
            f.start()
        barrier(me, rs.peers())
        for f in loads:
            f.wait()
        for number, kind in enumerate(PASSES):
            count = COUNT[kind]
            following = PASSES[number + 1] if number + 1 < len(PASSES) else None
            if kind == "da":
                load_at0.start()
            if kind == "norm":
                for q in range(TOKENS // PART):
                    for f in hiddens(0, q):
                        f.start()
            if kind == "first":
                load_at0.wait()

            def body(t, carry, kind=kind, count=count, following=following):
                s = lax.rem(t, 2)
                for f in fetch(kind, t, s):
                    f.wait()

                @pl.when(t + 1 < count)
                def _():
                    for f in fetch(kind, t + 1, 1 - s):
                        f.start()

                if kind == "last":

                    @pl.when(t > 1)
                    def _():
                        save(t - 2, s).wait()

                if following:

                    @pl.when(t == count - 1)
                    def _():
                        if kind == "last":
                            save(t - 1, 1 - s).wait()
                        for f in fetch(following, 0, 0):
                            f.start()

                if kind in ("last", "first"):
                    hidden(kind, t, s)
                    if kind == "last":
                        save(t, s).start()
                    point(kind, t, 0, 1)
                    side(kind, t, s)
                    point(kind, t, SIDE, 1)
                    down(kind, t, s)
                    point(kind, t, DOWN, 1)
                else:
                    (d_a if kind == "da" else norm)(t, s)
                    point(kind, t, 0, 1)
                return carry

            lax.fori_loop(0, count, body, 0)
            if kind == "last":
                save(count - 1, (count - 1) % 2).wait()
        for u in range(3):
            for c in range(3):
                it.wait_sends(u, c, flips[0, u, c])

    any_space = pl.BlockSpec(memory_space=pl.ANY)
    return pl.pallas_call(
        kernel,
        out_shape=[jax.ShapeDtypeStruct((LAYERS, 3, 3, CHUNK, LANES), F32), jax.ShapeDtypeStruct((STEPS, TOKENS, 2 * TILE), BF16)],
        in_specs=[any_space] * 10,
        out_specs=[pl.BlockSpec(memory_space=pltpu.VMEM), any_space],
        scratch_shapes=[
            pltpu.VMEM((TOKENS, D), BF16),
            pltpu.VMEM((TOKENS, D), BF16),
            pltpu.VMEM((D, TOKENS), BF16),
            pltpu.VMEM((X_ROWS, LANES), F32),
            pltpu.VMEM((TILE, TOKENS), BF16),
            pltpu.VMEM((2, TOKENS, 2 * TILE), BF16),
            pltpu.VMEM((2, D, 2 * TILE), BF16),
            pltpu.VMEM((2, TILE, D), BF16),
            pltpu.VMEM((TOKENS // PART, 2, LT, PART, LANES), F32),
            pltpu.SemaphoreType.DMA((4,)),
            pltpu.SemaphoreType.DMA((5, 2)),
            pltpu.SemaphoreType.DMA((TOKENS // PART, 2)),
            rs.scratch(),
        ],
        compiler_params=pltpu.CompilerParams(collective_id=collective_id, has_side_effects=True, vmem_limit_bytes=VMEM_ALL),
        cost_estimate=pl.CostEstimate(flops=TOKENS * D * FF * 24, bytes_accessed=TOKENS * FF * 20, transcendentals=0),
        name="backward",
    )(gate0, up0, h1, a1, at1, at0, dy, wg, wu, wd)[0]


def solution(mesh):
    torus = Torus(4, 4, 8)
    count = float(LAYERS * 3 * D * FF)

    def step(x, dy, wg, wu, wd, mg, mu, md, vg, vu, vd):
        x, dy = x[0], dy[0]
        gate0, up0, h1, a1, at1, at0 = forward(x, wg, wu, wd)
        g = backward(torus, gate0, up0, h1, a1, at1, at0, dy, wg, wu, wd, 1)
        G, m, v = step_and_gather(torus, g, (wg, wu, wd), (mg, mu, md), (vg, vu, vd), count, 2)
        return (*unpack(torus, G), *m, *v)

    P = jax.sharding.PartitionSpec
    return jax.shard_map(
        step,
        mesh=mesh,
        in_specs=(P(("rep", "dp")),) * 2 + (P(),) * 3 + (P(None, "dp"),) * 6,
        out_specs=(P("rep"),) * 3 + (P("rep", "dp"),) * 6,
        check_vma=False,
    )
```

```python
import heapq
import jax
import jax.numpy as jnp
from jax import lax
from jax.experimental import pallas as pl
from jax.experimental.pallas import tpu as pltpu

F32, BF16 = jnp.float32, jnp.bfloat16
MESH = pl.DeviceIdType.MESH
RATE, LATENCY = 46.6e3, 2.3
TURN, ADD, HOP = 0.1, 2.0e6, 0.7
WAYS = (1, -1)
TRIO = range(3)
RING, CROSS, DIRECT = TRIO
NEVER, MARGIN, SWEEPS = 1e9, 0.5, 2


class Torus:
    def __init__(self, nx, ny, nz):
        self.n = {"x": nx, "y": ny, "z": nz}
        self.size = nx * ny * nz

    def here(self):
        return Here(self)


class Here:
    def __init__(self, torus):
        p, n = lax.axis_index("dp"), torus.n
        ny, nz = n["y"], n["z"]
        mine = {"z": lax.rem(p, nz), "y": lax.rem(lax.div(p, nz), ny), "x": lax.div(p, ny * nz)}
        step = {"z": 1, "y": nz, "x": ny * nz}
        self.at = {d: [mine[d]] + [lax.rem(mine[d] + i, n[d]) for i in range(1, n[d])] for d in n}
        self.to = {d: [p + (self.at[d][i] - mine[d]) * step[d] for i in range(n[d])] for d in n}

    def peer(self, dim, delta):
        return {"dp": self.to[dim][delta % len(self.to[dim])]}

    def up(self, dim, delta):
        return self.at[dim][delta % len(self.at[dim])]


ORDERS = ("zxy", "xyz", "yxz")


def hops(n, flip):
    far, near = n // 2, n - 1 - n // 2
    return {1: near, -1: far} if flip else {1: far, -1: near}


class Balance:
    def __init__(self):
        self.load = {}

    def flip(self, dim, n, size):
        plain = [self.load.get((dim, s), 0) + size * hops(n, False)[s] for s in WAYS]
        turned = [self.load.get((dim, s), 0) + size * hops(n, True)[s] for s in WAYS]
        flip = max(turned) < max(plain)
        self.load[dim, 1], self.load[dim, -1] = turned if flip else plain
        return flip


def simulate(actions, copies):
    links, arrived, order = {}, {}, []
    waiting = {a: set(needs) for a, (needs, _, _, _) in actions.items()}
    by_need = {}
    for a, (needs, _, _, _) in actions.items():
        for c in needs:
            by_need.setdefault(c, []).append(a)
    ready = [(actions[a][3], i, a) for i, a in enumerate(actions) if not waiting[a]]
    rank = {a: i for i, a in enumerate(actions)}
    heapq.heapify(ready)
    now, done = 0.0, {}
    while ready:
        at, _, a = heapq.heappop(ready)
        now = max(now, at) + actions[a][2]
        order.append(a)
        done[a] = now
        for c in [("action", a)] + list(actions[a][1]):
            if c[0] == "action":
                end = now
            else:
                link, size, extra = copies[c]
                start = max(now, links.get(link, 0.0))
                links[link] = start + size / RATE
                end = links[link] + LATENCY + extra
            for b in by_need.get(c, ()):
                waiting[b].discard(c)
                arrived[b] = max(arrived.get(b, 0.0), end)
                if not waiting[b]:
                    heapq.heappush(ready, (max(arrived[b], actions[b][3]), rank[b], b))
    assert len(order) == len(actions), (len(order), len(actions))
    return order, now


def place(actions, copies, segments):
    links, known, left, slots, open_keys = {}, {}, dict(actions), {}, set()
    now = 0.0

    def do(a, where):
        nonlocal now
        _, sends, cost = left.pop(a)
        now += cost
        known["action", a] = now
        for c in sends:
            link, size, extra = copies[c]
            links[link] = max(now, links.get(link, 0.0)) + size / RATE
            known[c] = links[link] + LATENCY + extra
        where.append(a)

    def drain(where, allowed, wait):
        nonlocal now
        while True:
            able = [(max([known.get(c, NEVER) for c in actions[a][0]], default=0.0), i, a) for i, a in enumerate(left) if allowed(a)]
            best, _, a = min(able, default=(NEVER, 0, None))
            if best >= NEVER or not wait and best + MARGIN > now:
                return
            now = max(now, best)
            do(a, where)

    for key, cost, writes, whole in segments:
        now += cost
        slots[key] = ([], [])
        others = {(l, u, c) for (l, u), c in writes}
        drain(slots[key][0], lambda a: any(a[0][0][1] == u and a[0][1] == c and a[0][0][0] > l for l, u, c in others), True)
        open_keys |= set(whole)
        drain(slots[key][1], lambda a: a[1] != "start" or (a[0], a[2]) in open_keys, False)
    drain(slots[segments[-1][0]][1], lambda a: True, True)
    assert not left
    place.took = now
    return slots


def barrier(me, peers):
    sem = pltpu.get_barrier_semaphore()
    for dim, delta in peers:
        pl.semaphore_signal(sem, inc=1, device_id=me.peer(dim, delta), device_id_type=MESH)
    pl.semaphore_wait(sem, len(peers))


def both_ways(torus, dim):
    n = torus.n[dim]
    return [] if n == 1 else [(dim, 1)] if n == 2 else [(dim, 1), (dim, -1)]


def all_others(torus, dim):
    return [(dim, d) for d in range(1, torus.n[dim])]


class ReduceScatter:
    LANES = (2, 1, 1)

    def __init__(self, torus, rows, units):
        self.t, self.rows, self.units = torus, rows, units
        self.dims = [tuple(order) for order in ORDERS]
        self.nslots = max(self.base(c, DIRECT, 0) + self.sizes(c)[DIRECT] - 1 for c in TRIO)

    def sizes(self, c):
        return [self.t.n[d] for d in self.dims[c]]

    def here(self, c):
        return [self.me.up(d, 0) for d in self.dims[c]]

    def base(self, c, phase, lane):
        n = self.sizes(c)
        return sum((n[i] - 1) * self.LANES[i] for i in range(phase)) + lane * (n[phase] - 1)

    def peers(self):
        full = {dims[DIRECT] for dims in self.dims}
        out = []
        for dim in "xyz":
            out += all_others(self.t, dim) if dim in full else both_ways(self.t, dim)
        return out

    def credit_peers(self, c):
        a, b, d = self.dims[c]
        return both_ways(self.t, a) + both_ways(self.t, b) + all_others(self.t, d)

    def scratch(self):
        n = self.t.n
        t, r1, r2, r3, k2, k3 = [], [], [], [], [], []
        for dims in self.dims:
            n1, n2, n3 = (n[d] for d in dims)
            tail = (self.rows, 128)
            t.append(pltpu.VMEM((self.units, n1, n2 * n3) + tail, BF16))
            r1.append(pltpu.VMEM((self.units, max(n1 - 1, 1), n2 * n3) + tail, BF16))
            r2.append(pltpu.VMEM((self.units, max(n2 - 1, 1), n3) + tail, BF16))
            r3.append(pltpu.VMEM((self.units, max(n3 - 1, 1)) + tail, BF16))
            k2.append(pltpu.VMEM((self.units, n3) + tail, F32))
            k3.append(pltpu.VMEM((self.units,) + tail, F32))
        sems = [pltpu.SemaphoreType.DMA((self.units, 3, self.nslots)), pltpu.SemaphoreType.DMA((self.units, 3, self.nslots)), pltpu.SemaphoreType.REGULAR((self.units, 3))]
        return [t, r1, r2, r3, k2, k3] + sems

    def slot(self, c, phase, sign, h):
        return h if sign > 0 else self.sizes(c)[phase] - 2 - h

    def flips(self, balance, c):
        n1, n2, n3 = self.sizes(c)
        block, (a, b, d) = self.rows * 256, self.dims[c]
        for rel in range(1, n3):
            link = d, 1 if rel <= n3 // 2 else -1
            balance.load[link] = balance.load.get(link, 0) + block * min(rel, n3 - rel)
        ring = [balance.flip(a, n1, block * n2 * n3 // self.LANES[RING]) for _ in range(self.LANES[RING])]
        return ring, [balance.flip(b, n2, block * n3)]

    def plan(self, unit, c, flip):
        n = self.sizes(c)
        n1, n2, n3 = n
        block = self.rows * 256
        size = [block * n2 * n3 // self.LANES[RING], block * n3, block]
        actions, copies = {}, {}
        key = (unit, c)

        def send(phase, lane, sign, h):
            cid = ("copy", key, phase, lane, sign, h)
            copies[cid] = ((self.dims[c][phase], sign), size[phase], 0)
            return cid

        first, last = [[], []], [[], []]
        for phase in (RING, CROSS):
            for lane, turned in enumerate(flip[phase]):
                k = hops(n[phase], turned)
                ways = [s for s in WAYS if k[s]]
                first[phase] += [send(phase, lane, s, k[s] - 1) for s in ways]
                last[phase] += [("copy", key, phase, lane, s, 0) for s in ways]
                for s in ways:
                    for h in range(k[s] - 1, 0, -1):
                        actions[key, "step", phase, lane, s, h] = ([("copy", key, phase, lane, s, h)], [send(phase, lane, s, h - 1)], size[phase] / ADD)
        direct = []
        for rel in range(1, n3):
            cid = ("copy", key, DIRECT, 0, 0, rel)
            far = min(rel, n3 - rel)
            copies[cid] = ((self.dims[c][DIRECT], 1 if rel <= n3 // 2 else -1), size[DIRECT] * far, HOP * (far - 1))
            direct.append(cid)
        sends = first + [direct, []]
        for lane in range(self.LANES[RING]):
            actions[key, "start", lane] = ([], [x for x in sends[RING] if x[3] == lane], TURN)
        before = (key, "start", 0)
        for phase, needs in enumerate(last + [direct]):
            a = (key, "end", phase)
            actions[a] = (needs + [("action", before)], sends[phase + 1], size[phase] * self.LANES[phase] / ADD + TURN)
            before = a
        return actions, copies

    def bind(self, me, refs):
        self.me, (self.T, self.R1, self.R2, self.R3, self.K2, self.K3, self.ssem, self.rsem, self.credit) = me, refs
        return self

    def remote(self, u, c, phase, lane, sign, h):
        n1, n2, n3 = self.sizes(c)
        d1, d2, d3 = self.dims[c]
        up = self.me.up
        mine = self.T[c].at[u]
        slot = h - 1 if phase == DIRECT else self.slot(c, phase, sign, h)
        if phase == RING:
            part = n2 * n3 // self.LANES[RING]
            blocks = pl.ds(lane * part, part)
            src, dst = mine.at[up(d1, sign * (h + 1)), blocks], self.R1[c].at[u, slot, blocks]
        elif phase == CROSS:
            src, dst = mine.at[up(d1, 0), pl.ds(up(d2, sign * (h + 1)) * n3, n3)], self.R2[c].at[u, slot]
        else:
            sign = h
            src, dst = mine.at[up(d1, 0), up(d2, 0) * n3 + up(d3, h)], self.R3[c].at[u, slot]
        s = self.base(c, phase, lane) + slot
        to = self.me.peer(self.dims[c][phase], sign)
        return pltpu.make_async_remote_copy(src_ref=src, dst_ref=dst, send_sem=self.ssem.at[u, c, s], recv_sem=self.rsem.at[u, c, s], device_id=to, device_id_type=MESH)

    def all_sends(self, c, flip):
        n = self.sizes(c)
        out = []
        for phase in (RING, CROSS):
            for lane, turned in enumerate(flip[phase]):
                k = hops(n[phase], turned)
                out += [(phase, lane, s, h) for s in WAYS for h in range(k[s])]
        return out + [(DIRECT, 0, 0, rel) for rel in range(1, n[DIRECT])]

    def run(self, u, c, flip, what, store):
        n = self.sizes(c)
        n1, n2, n3 = n
        m1, m2, m3 = self.here(c)
        T, R1, R2, R3 = (r[c].at[u] for r in (self.T, self.R1, self.R2, self.R3))
        K2, K3 = self.K2[c].at[u], self.K3[c].at[u]
        mine = T.at[m1]
        wide = lambda v: v.astype(F32)
        go = lambda *a: self.remote(u, c, *a)

        def loop(count, body):
            def one(i, carry):
                body(i)
                return carry

            lax.fori_loop(0, count, one, 0)

        def line(q):
            return pl.ds(q * n3, n3)

        def ways(phase):
            for lane, turned in enumerate(flip[phase]):
                k = hops(n[phase], turned)
                for s in WAYS:
                    if k[s]:
                        yield lane, s, k[s]

        def sends(phase, only=None):
            for lane, s, k in ways(phase):
                if only in (None, lane):
                    go(phase, lane, s, k - 1).start()

        def arrived(phase):
            got = set()
            for lane, s, _ in ways(phase):
                go(phase, lane, s, 0).wait_recv()
                got.add(self.slot(c, phase, s, 0))
            return sorted(got)

        kind, *where = what
        if kind == "start":
            sends(RING, *where)
        elif kind == "step":
            phase, lane, s, h = where
            go(*where).wait_recv()
            slot = self.slot(c, phase, s, h)
            q = self.me.up(self.dims[c][phase], s * h)
            if phase == RING:
                lines = n2 // self.LANES[RING]

                def add(i):
                    b = line(lane * lines + i)
                    T[q, b] = (wide(T[q, b]) + wide(R1[slot, b])).astype(BF16)

                loop(lines, add)
            else:
                mine[line(q)] = (wide(mine[line(q)]) + wide(R2[slot])).astype(BF16)
            go(phase, lane, s, h - 1).start()
        elif where == [RING]:
            got = arrived(RING)

            def total(b):
                return sum((wide(R1[g, b]) for g in got), wide(mine[b]))

            def others(i):
                b = line(lax.rem(m2 + 1 + i, n2))
                mine[b] = total(b).astype(BF16)

            loop(n2 - 1, others)
            sends(CROSS)
            K2[...] = total(line(m2))
        elif where == [CROSS]:
            got = arrived(CROSS)
            total = sum((wide(R2[g]) for g in got), K2[...])
            K2[...] = total
            mine[line(m2)] = total.astype(BF16)
            for rel in range(1, n3):
                go(DIRECT, 0, 0, rel).start()
            K3[...] = K2[m3]
        else:
            for rel in range(1, n3):
                go(DIRECT, 0, 0, rel).wait_recv()
            store(sum((wide(R3[i]) for i in range(n3 - 1)), K3[...]).astype(BF16).astype(F32))

    def wait_sends(self, u, c, flip):
        for a in self.all_sends(c, flip):
            self.remote(u, c, *a).wait_send()

    def give_credit(self, u, c):
        for dim, delta in self.credit_peers(c):
            pl.semaphore_signal(self.credit.at[u, c], inc=1, device_id=self.me.peer(dim, delta), device_id_type=MESH)

    def take_credit(self, u, c):
        pl.semaphore_wait(self.credit.at[u, c], len(self.credit_peers(c)))


class AllGather:
    def __init__(self, torus, block_bytes, split=2):
        self.t, self.bytes, self.split = torus, block_bytes, split
        self.dims = [tuple(order) for order in ORDERS]
        self.flip, self.balance = {}, Balance()
        self.build()
        for key in list(self.flip) * SWEEPS:
            took = self.took
            self.flip[key] = not self.flip[key]
            self.build()
            if self.took >= took:
                self.flip[key] = not self.flip[key]
        self.build()

    def build(self):
        self.copies, self.actions, self.index = {}, {}, {}
        for c in TRIO:
            self.plan(c)
        self.order, self.took = simulate({a: (*v, 0) for a, v in self.actions.items()}, self.copies)

    def peers(self):
        return [p for dim in "xyz" for p in both_ways(self.t, dim)]

    def pieces(self, c, j):
        n3 = self.t.n[self.dims[c][DIRECT]]
        return n3 if not j else self.split if n3 % self.split == 0 else 1

    def size(self, c, phase, j):
        line = self.bytes * self.t.n[self.dims[c][DIRECT]]
        return self.bytes if phase == DIRECT else line // self.pieces(c, 1 if phase == CROSS else j)

    def k(self, c, phase, j, i):
        dim = self.dims[c][phase]
        key = (c, phase, j, i)
        if key not in self.flip:
            self.flip[key] = self.balance.flip(dim, self.t.n[dim], self.size(c, phase, j))
        return hops(self.t.n[dim], self.flip[key])

    def plan(self, c):
        n1, n2, n3 = (self.t.n[d] for d in self.dims[c])

        def send(where, s, h):
            phase, j, _ = where
            cid = (c, where, s, h)
            self.copies[cid] = ((self.dims[c][phase], s), self.size(c, phase, j), 0)
            self.index[cid] = len(self.index)
            return cid

        def own(*where):
            k = self.k(c, *where)
            return [send(where, s, 1) for s in WAYS if k[s]]

        def passing(*where):
            k = self.k(c, *where)
            for s in WAYS:
                for h in range(1, k[s] + 1):
                    yield s, h, (c, "pass", where, s, h), [(c, where, s, h)], [send(where, s, h + 1)] if h < k[s] else []

        def act(a, needs, sends):
            self.actions[a] = (needs, sends, TURN / 2)

        act((c, "start"), [], own(DIRECT, 0, 0) + own(RING, 0, 0))
        got = [("action", (c, "start"))]
        for s, h, a, needs, sends in passing(DIRECT, 0, 0):
            act(a, needs, sends + own(RING, 0, (-s * h) % n3))
            got.append(("action", a))
        parts = range(self.pieces(c, 1))
        act((c, "line"), got, [x for i in parts for x in own(CROSS, 0, i)])
        for i in parts:
            for s, h, a, needs, sends in passing(CROSS, 0, i):
                after = (-s * h) % n2, i
                if c:
                    act(a, needs, sends + own(RING, *after))
                else:
                    act(a, needs, sends)
                    act((c, "later", *after), [("action", x) for x in (a, (1, "line"), (2, "line"))], own(RING, *after))
        for j in range(n2):
            for i in range(self.pieces(c, j)):
                for _, _, a, needs, sends in passing(RING, j, i):
                    act(a, needs, sends)

    def bind(self, me, G, ssem, rsem):
        self.me, self.G, self.ssem, self.rsem = me, G, ssem, rsem
        return self

    def remote(self, cid, back):
        c, (phase, j, i), s, h = cid
        d1, d2, d3 = self.dims[c]
        n3, up = self.t.n[d3], self.me.up
        off = s * (back - h)
        G = self.G[c]
        if phase == DIRECT:
            ref = G.at[up(d1, 0), up(d2, 0) * n3 + up(d3, off)]
        elif phase == CROSS:
            size = n3 // self.pieces(c, 1)
            ref = G.at[up(d1, 0), pl.ds(up(d2, off) * n3 + i * size, size)]
        elif j == 0:
            ref = G.at[up(d1, off), up(d2, 0) * n3 + up(d3, i)]
        else:
            size = n3 // self.pieces(c, j)
            ref = G.at[up(d1, off), pl.ds(up(d2, j) * n3 + i * size, size)]
        x = self.index[cid]
        return pltpu.make_async_remote_copy(src_ref=ref, dst_ref=ref, send_sem=self.ssem.at[x], recv_sem=self.rsem.at[x], device_id=self.me.peer(self.dims[c][phase], s), device_id_type=MESH)

    def run(self, a):
        needs, sends, _ = self.actions[a]
        for cid in needs:
            if cid in self.index:
                self.remote(cid, 0).wait_recv()
        for cid in sends:
            self.remote(cid, 1).start()

    def wait_sends(self):
        for cid in self.copies:
            self.remote(cid, 1).wait_send()


MIB = 2**20
VMEM_ALL = 67043328
LAYERS, D, FF = 2, 896, 2560
LANES, ROWS, CHUNK = 128, 144, 48
HIGH = {0: 7, 1: 7, 2: 20}
WIDE = {0: FF, 1: FF, 2: D}
WINDOW = (16, 16, 24)


HALVES, RING_TILES = 2, 8
COLOURS = {0: (1, 2, 0), 1: (1, 2, 0), 2: (0, 1, 2)}
TOKENS, TILE, PART = 2048, 256, 512
LT, STEPS = TILE // LANES, FF // TILE
HALF = STEPS // HALVES


def home(u, ct):
    if u == HALVES:
        return u, ct
    t, k = divmod(ct, 2 * LT)
    m, j = divmod(k, LT)
    return m, (u * HALF + t) * LT + j


def tiles(u):
    high, wide = HIGH[u], WIDE[u] // LANES
    out = []
    for k in range(ROWS // 8):
        ct, row = divmod(8 * k, high)
        out.append((ct, row, min(8, high - row), ct + 1 < wide))
    return out


def pack(torus, u, X, base, parts, first, count, outs, colours):
    high, ny, nz = HIGH[u], torus.n["y"], torus.n["z"]
    sub = lax.broadcasted_iota(jnp.int32, (8, LANES), 0)
    got = tiles(u)

    def body(line, carry):
        x, y = lax.div(first + line, ny), lax.rem(first + line, ny)
        top = pl.multiple_of(line * (high * nz), 8)

        def piece(z, ct, row, whole, more):
            a = X[pl.ds(top + (base(ct) + high * z + row), 8), :]
            if whole == 8:
                return a
            b = X[pl.ds(top + (base(ct + 1) + high * z - whole), 8), :] if more else jnp.zeros((8, LANES), F32)
            return jnp.where(sub < whole, a, b)

        for z in range(nz):
            at = {"x": x, "y": y, "z": z}
            for j in parts:
                both = jnp.concatenate([piece(z, *got[2 * j]), piece(z, *got[2 * j + 1])], axis=0).astype(BF16)
                k, r = divmod(16 * j, CHUNK)
                c = colours[k]
                d1, d2, d3 = ORDERS[c]
                outs[c][at[d1], at[d2] * torus.n[d3] + at[d3], pl.ds(r, 16), :] = both
        return carry

    lax.fori_loop(0, count, body, 0)


def pieces_shapes(torus, dtype, *mid):
    out = []
    for order in ORDERS:
        a, b, d = (torus.n[x] for x in order)
        out.append(jax.ShapeDtypeStruct((a, b * d) + mid + (CHUNK, LANES), dtype))
    return out


def step_and_gather(torus, g, w, m, v, count, collective_id):
    ag = AllGather(torus, LAYERS * 3 * CHUNK * 256)
    dims = "zxy"
    slots = {d: torus.n[d] - 1 for d in dims}

    def window(p, x):
        rows = WINDOW[x]
        first = lax.div(p * HIGH[x], 8) * 8
        return pl.multiple_of(jnp.minimum(first, HIGH[x] * torus.size - rows), 8), rows

    def kernel(g_ref, *refs):
        w_in, m_in, v_in, G, m_out, v_out = (refs[i : i + 3] for i in range(0, 18, 3))
        flat, wflat, part, E, esend, erecv, ssem, rsem, win, wide_win, wsem = refs[18:]
        me = torus.here()
        p = lax.axis_index("dp")
        loads = []
        for x in TRIO:
            first, rows = window(p, x)
            loads.append(pltpu.make_async_copy(w_in[x].at[:, pl.ds(first, rows)], win[x], wsem.at[x]))
            loads[x].start()
        barrier(me, [p for d in "xyz" for p in all_others(torus, d)])
        for x in TRIO:
            loads[x].wait()
            for lt in range(WIDE[x] // LANES):
                wide_win[x][:, lt] = win[x][:, :, pl.ds(lt * LANES, LANES)].astype(F32)
        acc = jnp.zeros((8, LANES), F32)
        for l in range(LAYERS):
            for u in TRIO:
                for k, c in enumerate(COLOURS[u]):
                    value = g_ref[l, u, c]
                    flat[l, u, pl.ds(k * CHUNK, CHUNK), :] = value
                    for r in range(0, CHUNK, 8):
                        acc = acc + value[r : r + 8] * value[r : r + 8]
        part[0] = acc
        base = 0
        for i, d in enumerate(dims):
            n = torus.n[d]
            copies = []
            for rel in range(1, n):
                s = base + rel - 1
                copies.append(pltpu.make_async_remote_copy(src_ref=part.at[i], dst_ref=E.at[s], send_sem=esend.at[s], recv_sem=erecv.at[s], device_id=me.peer(d, rel), device_id_type=MESH))
            for copy in copies:
                copy.start()
            total = part[i]
            for rel in range(1, n):
                copies[rel - 1].wait_recv()
                total = total + E[base + rel - 1]
            part[i + 1] = total
            for copy in copies:
                copy.wait_send()
            base += n - 1
        mean = jnp.sum(part[3], keepdims=True) / count
        factor = jnp.minimum(1.0, 0.5 * lax.rsqrt(mean + 1e-30))
        for l in range(LAYERS):
            for u in TRIO:
                high = HIGH[u]
                wflat[l, u, pl.ds(ROWS - 8, 8), :] = jnp.zeros((8, LANES), F32)
                for ct in range(WIDE[u] // LANES):
                    x, lt = home(u, ct)
                    at = (slice(None), l, pl.ds(lt * LANES, LANES))
                    grad = flat[l, u, pl.ds(ct * high, high), :] * factor
                    new_m = 0.9 * m_in[x][at] + 0.1 * grad
                    new_v = 0.95 * v_in[x][at] + 0.05 * grad * grad
                    wide = wide_win[x][l, lt, pl.ds(p * high - window(p, x)[0], high), :]
                    new_w = wide - 0.02 * (new_m * lax.rsqrt(new_v + 1e-8) + 0.1 * wide)
                    m_out[x][at] = new_m
                    v_out[x][at] = new_v
                    wflat[l, u, pl.ds(ct * high, high), :] = new_w
        it = ag.bind(me, G, ssem, rsem)
        for u in TRIO:
            for k, c in enumerate(COLOURS[u]):
                a, b, d = (me.up(x, 0) for x in ORDERS[c])
                for l in range(LAYERS):
                    G[c][a, b * torus.n[ORDERS[c][DIRECT]] + d, l, u] = wflat[l, u, pl.ds(k * CHUNK, CHUNK), :].astype(BF16)
        for a in ag.order:
            it.run(a)
        it.wait_sends()

    vmem = pl.BlockSpec(memory_space=pltpu.VMEM)
    nsum = sum(slots.values())
    shapes = pieces_shapes(torus, BF16, LAYERS, 3)
    turn = lambda ts: [jnp.transpose(t, (1, 0, 2)) for t in ts]
    m, v = turn(m), turn(v)
    f32 = [jax.ShapeDtypeStruct(t.shape, F32) for t in m]
    k = len(ag.copies)
    got = pl.pallas_call(
        kernel,
        out_shape=[pltpu.MemorySpace.VMEM(s.shape, s.dtype) for s in shapes] + f32 * 2,
        in_specs=[vmem] + [pl.BlockSpec(memory_space=pl.ANY)] * 3 + [vmem] * 6,
        out_specs=[vmem] * 9,
        scratch_shapes=[
            pltpu.VMEM((LAYERS, 3, ROWS, LANES), F32),
            pltpu.VMEM((LAYERS, 3, ROWS, LANES), F32),
            pltpu.VMEM((4, 8, LANES), F32),
            pltpu.VMEM((nsum, 8, LANES), F32),
            pltpu.SemaphoreType.DMA((nsum,)),
            pltpu.SemaphoreType.DMA((nsum,)),
            pltpu.SemaphoreType.DMA((k,)),
            pltpu.SemaphoreType.DMA((k,)),
            [pltpu.VMEM((LAYERS, WINDOW[x], WIDE[x]), BF16) for x in TRIO],
            [pltpu.VMEM((LAYERS, WIDE[x] // LANES, WINDOW[x], LANES), F32) for x in TRIO],
            pltpu.SemaphoreType.DMA((3,)),
        ],
        compiler_params=pltpu.CompilerParams(collective_id=collective_id, has_side_effects=True, vmem_limit_bytes=26 * MIB),
        name="step_and_gather",
    )(g, *w, *m, *v)
    return got[:3], turn(got[3:6]), turn(got[6:])


def unpack(torus, G):
    nx, ny, nz = (torus.n[d] for d in "xyz")
    pair = 2
    group = pair * nz
    groups = torus.size // group
    pairs = ny // pair

    def kernel(g0, g1, g2, *refs):
        outs, Z, Y = refs[:3], refs[3], refs[4]
        l, s = pl.program_id(0), pl.program_id(1)
        corner = {"x": lax.div(s, pairs), "y": lax.rem(s, pairs) * pair, "z": 0}
        for u in TRIO:
            high, wide = HIGH[u], WIDE[u] // LANES
            for i in range(group):
                y, z = divmod(i, nz)
                at = corner | {"y": corner["y"] + y, "z": z}
                for k, c in enumerate(COLOURS[u]):
                    a, b, d = ORDERS[c]
                    Z[i, pl.ds(k * CHUNK, CHUNK), :] = (g0, g1, g2)[c][at[a], at[b] * torus.n[d] + at[d], l, u].astype(F32)
            for i in range(group):
                for ct in range(wide):
                    for r in range(0, high, 8):
                        Y[ct, pl.ds(high * i + r, 8), :] = Z[i, pl.ds(high * ct + r, 8), :]
            rows = high * group
            for ct in range(wide):
                x, lt = home(u, ct)
                outs[x][0, :, pl.ds(lt * LANES, LANES)] = Y[ct, pl.ds(0, rows), :].astype(BF16)

    shapes = [(LAYERS, HIGH[u] * torus.size, WIDE[u]) for u in TRIO]
    return pl.pallas_call(
        kernel,
        grid=(LAYERS, groups),
        out_shape=[jax.ShapeDtypeStruct(s, BF16) for s in shapes],
        in_specs=[pl.BlockSpec(memory_space=pltpu.VMEM)] * 3,
        out_specs=[pl.BlockSpec((1, HIGH[u] * group, WIDE[u]), lambda l, s: (l, s, 0)) for u in TRIO],
        scratch_shapes=[pltpu.VMEM((group, ROWS + 8, LANES), F32), pltpu.VMEM((FF // LANES, HIGH[2] * group + 8, LANES), F32)],
        compiler_params=pltpu.CompilerParams(vmem_limit_bytes=26 * MIB),
        name="unpack",
    )(*G)


NN, NT = ((1,), (0,)), ((1,), (1,))


def dot(a, b, dims=NN):
    return lax.dot_general(a, b, (dims, ((), ())), preferred_element_type=F32)


def scale_of(wide):
    return lax.rsqrt(jnp.mean(wide * wide, -1, keepdims=True) + 1e-6)


GAP = 24
SIDE_STRIDE, DOWN_STRIDE = D + GAP, FF // HALVES + GAP
DOWN_BASE = RING_TILES * SIDE_STRIDE
X_ROWS = DOWN_BASE + D // LANES * DOWN_STRIDE
COST = {"last": (3.8, 2.3, 1.3), "first": (1.7, 2.3, 1.3), "da": (2.4,), "norm": (0.45,)}
PACK_DOWN = 0.4
WHOLE = ((0,), (1, 2), (3, 4), (5, 6), (7, 8))
CHUNKS = {1: 0, 3: 1, 4: 2}
PASSES = ("forward", "last", "da", "norm", "first")
COUNT = {"forward": STEPS, "last": STEPS, "da": STEPS, "norm": TOKENS // TILE, "first": STEPS}
QUARTERS = TOKENS // PART
SIDE, DOWN = 1, 2


def timeline():
    out, lanes = [], ReduceScatter.LANES[RING]
    for kind in PASSES[1:]:
        layer = {"last": 1, "first": 0}.get(kind)
        for t in range(COUNT[kind]):
            half, tt = divmod(t, HALF)
            for i, cost in enumerate(COST[kind]):
                writes, whole = [], []
                if i == SIDE:
                    unit = (layer, half)
                    writes = [(unit, c) for c in TRIO] if tt == 0 else []
                    whole = [((unit, COLOURS[half][CHUNKS[tt]]), lane) for lane in range(lanes)] if tt in CHUNKS else []
                if i == DOWN and tt == HALF - 1:
                    cost += PACK_DOWN
                    mine = [((layer, HALVES), c) for c in TRIO]
                    writes = [] if half else mine
                    whole = [(key, lane) for key in mine for lane in range(lanes) if half or lane == 0 and ORDERS[key[1]][CROSS] == "x"]
                out.append(((kind, t, i), cost, writes, whole))
    return out


def hidden_back(gate, up, d):
    s = jax.nn.sigmoid(gate)
    act = gate * s
    return (act * up).astype(BF16), (d * up * (s + act * (1.0 - s))).astype(BF16), (d * act).astype(BF16)


def gradients(torus, x, dy, wg, wu, wd, collective_id):
    rs = ReduceScatter(torus, CHUNK, 3)
    actions, copies, balance, flips = {}, {}, Balance(), {}
    for l in range(LAYERS):
        for u in TRIO:
            for c in TRIO:
                flips[l, u, c] = rs.flips(balance, c)
                got, sent = rs.plan((l, u), c, flips[l, u, c])
                copies |= sent
                actions |= got
                if l:
                    key = ((l, u), c)
                    actions[key, "free"] = ([("action", (key, "end", DIRECT))], [], TURN)
    slots = place(actions, copies, timeline())
    lines = torus.n["x"] * torus.n["y"]

    def kernel(x_ref, dy_ref, wg_ref, wu_ref, wd_ref, out, both_ref, gate_ref, up_ref, h1_ref, at0_ref, dyv, av, at, X, Mb, Db, Wb, Vb, Hb, once, pair, hsem, rsem, rsc):
        me = torus.here()
        it = rs.bind(me, rsc)
        copy = pltpu.make_async_copy
        load_x = copy(x_ref, dyv, once.at[0])
        save_at0, load_at0 = copy(at, at0_ref, once.at[1]), copy(at0_ref, at, once.at[1])

        def part(i):
            return pl.ds(i * TILE if isinstance(i, int) else pl.multiple_of(i * TILE, TILE), TILE)

        def sides(layer, t, s):
            return [copy(ref.at[layer, :, part(t)], Wb.at[s, :, part(k)], pair.at[k, s]) for k, ref in enumerate((wg_ref, wu_ref))]

        def fetch(kind, t, s):
            both, rows = pair.at[2, s], pair.at[3, s]
            if kind == "forward":
                return sides(0, t, s) + [copy(wd_ref.at[0, part(t)], Vb.at[s], rows)]
            if kind == "last":
                return sides(1, t, s) + [copy(wd_ref.at[1, part(t)], Vb.at[s], rows)]
            if kind == "da":
                return sides(1, t, s) + [copy(both_ref.at[t], Db.at[s], both)]
            if kind == "norm":
                return [copy(h1_ref.at[part(t)], Vb.at[s], rows)]
            return [copy(wd_ref.at[0, part(t)], Vb.at[s], rows)]

        def save(t, s):
            return copy(Db.at[s], both_ref.at[t], pair.at[4, s])

        def hiddens(t, quarters, out=False):
            got = []
            for q in quarters:
                for k, ref in enumerate((gate_ref, up_ref)):
                    ends = ref.at[pl.ds(t * LT, LT), pl.ds(q * PART, PART)], Hb.at[q, k]
                    got.append(copy(*(ends[::-1] if out else ends), hsem.at[q, k]))
            return got

        def act(a):
            ((l, u), c), what = a[0], a[1:]
            if what[0] == "free":
                it.wait_sends(u, c, flips[l, u, c])
                it.give_credit(u, c)
                return
            if what == ("start", 0) and l == 0:
                it.take_credit(u, c)

            def store(value):
                out[l, u, c] = value

            it.run(u, c, flips[l, u, c], what, store)

        def point(kind, t, i, which):
            for k in range(COUNT[kind]):
                if slots[kind, k, i][which]:

                    @pl.when(t == k)
                    def _(k=k):
                        for a in slots[kind, k, i][which]:
                            act(a)

        def normed_into(r):
            wide = dyv[part(r), :].astype(F32)
            a = (wide * scale_of(wide)).astype(BF16)
            av[part(r), :] = a
            at[:, part(r)] = a.T

        def lanes_of(ct):
            return slice(ct * LANES, (ct + 1) * LANES)

        def forward(t, s):
            for first in range(0, QUARTERS, 2):
                quarters = range(first, first + 2)

                @pl.when(t > 0)
                def _():
                    for f in hiddens(t - 1, quarters, True):
                        f.wait()

                for q in quarters:
                    rows = pl.ds(q * PART, PART)
                    both = dot(av[rows, :], Wb[s])
                    gate, up = both[:, :TILE], both[:, TILE:]
                    for j in range(LT):
                        Hb[q, 0, j], Hb[q, 1, j] = gate[:, lanes_of(j)], up[:, lanes_of(j)]
                    got = dot((jax.nn.silu(gate) * up).astype(BF16), Vb[s])
                    for ct in range(D // LANES):
                        here = pl.ds(ct * TOKENS + q * PART, PART)
                        X[here, :] = jnp.where(t == 0, 0.0, X[here, :]) + got[:, lanes_of(ct)]
                for f in hiddens(t, quarters, True):
                    f.start()

        def turn():
            for f in hiddens(STEPS - 1, range(QUARTERS), True):
                f.wait()
            save_at0.wait()
            count = TOKENS // TILE

            def saves(r):
                return copy(dyv.at[part(r)], h1_ref.at[part(r)], rsem.at[0, r])

            def loads(r):
                return copy(dy_ref.at[part(r)], dyv.at[part(r)], rsem.at[1, r])

            @pl.loop(0, count)
            def _(r):
                total = jnp.concatenate([X[pl.ds(ct * TOKENS + r * TILE, TILE), :] for ct in range(D // LANES)], axis=1)
                dyv[part(r), :] = dyv[part(r), :] + total.astype(BF16)
                normed_into(r)
                saves(r).start()

                @pl.when(r > 0)
                def _():
                    saves(r - 1).wait()
                    loads(r - 1).start()

            saves(count - 1).wait()
            loads(count - 1).start()
            for r in range(count):
                loads(r).wait()

        def hidden(kind, t, s):
            for first in range(0, QUARTERS, 2):
                quarters = range(first, first + 2)
                if kind == "first":
                    for f in hiddens(t, quarters):
                        f.wait()
                for q in quarters:
                    rows = pl.ds(q * PART, PART)
                    if kind == "last":
                        both = dot(av[rows, :], Wb[s])
                        gate, up = both[:, :TILE], both[:, TILE:]
                    else:
                        gate, up = (jnp.concatenate([Hb[q, k, j] for j in range(LT)], axis=1) for k in range(2))
                    d = dot(dyv[rows, :], Vb[s], NT).astype(BF16).astype(F32)
                    mid, Db[s, rows, part(0)], Db[s, rows, part(1)] = hidden_back(gate, up, d)
                    Mb[:, rows] = mid.T
                if kind == "first":

                    @pl.when(t + 1 < STEPS)
                    def _():
                        for f in hiddens(t + 1, quarters):
                            f.start()

        def side(kind, t, s):
            tt = lax.rem(t, HALF)
            got = dot(at[...], Db[s])
            for k in range(2 * LT):
                X[pl.ds((lax.rem(tt, 2) * 2 * LT + k) * SIDE_STRIDE + 8, D), :] = got[:, lanes_of(k)]
            point(kind, t, SIDE, 0)
            half = lax.div(t, HALF)
            for v, parts in enumerate(WHOLE):

                @pl.when(tt == v)
                def _(parts=parts):
                    pack(torus, 0, X, lambda ct: ct % RING_TILES * SIDE_STRIDE + 8, parts, 0, lines, [T.at[half] for T in it.T], COLOURS[0])

        def down(kind, t, s):
            half, tt = lax.div(t, HALF), lax.rem(t, HALF)
            got = dot(Mb[...], dyv[...])
            for ct in range(D // LANES):
                X[pl.ds(DOWN_BASE + ct * DOWN_STRIDE + 8 + tt * TILE, TILE), :] = got[:, lanes_of(ct)]
            point(kind, t, DOWN, 0)

            @pl.when(tt == HALF - 1)
            def _():
                some = lines // HALVES
                pack(torus, HALVES, X, lambda ct: DOWN_BASE + ct * DOWN_STRIDE + 8, range(ROWS // 16), half * some, some, [T.at[HALVES] for T in it.T], COLOURS[HALVES])

        def d_a(t, s):
            for r in range(0, TOKENS, PART):
                got = dot(Db[s, pl.ds(r, PART), :], Wb[s], NT)
                for ct in range(D // LANES):
                    rows = pl.ds(ct * TOKENS + r, PART)
                    X[rows, :] = jnp.where(t == 0, 0.0, X[rows, :]) + got[:, lanes_of(ct)]

        def norm(t, s):
            da = jnp.concatenate([X[pl.ds(ct * TOKENS + t * TILE, TILE), :] for ct in range(D // LANES)], axis=1).astype(BF16).astype(F32)
            wide = Vb[s].astype(F32)
            scale = scale_of(wide)
            inner = jnp.mean(da * wide, -1, keepdims=True)
            dyv[part(t), :] = dyv[part(t), :] + (scale * da - wide * (scale * scale * scale * inner)).astype(BF16)

        for f in fetch("forward", 0, 0) + [load_x]:
            f.start()
        barrier(me, rs.peers())
        load_x.wait()

        @pl.loop(0, TOKENS // TILE)
        def _(r):
            normed_into(r)

        save_at0.start()
        for number, kind in enumerate(PASSES):
            count = COUNT[kind]
            following = PASSES[number + 1] if number + 1 < len(PASSES) else None
            if kind == "last":
                turn()
            if kind == "da":
                load_at0.start()
            if kind == "norm":
                for f in hiddens(0, range(QUARTERS)):
                    f.start()
            if kind == "first":
                load_at0.wait()

            def body(t, carry, kind=kind, count=count, following=following):
                s = lax.rem(t, 2)
                for f in fetch(kind, t, s):
                    f.wait()

                @pl.when(t + 1 < count)
                def _():
                    for f in fetch(kind, t + 1, 1 - s):
                        f.start()

                if kind == "last":

                    @pl.when(t > 1)
                    def _():
                        save(t - 2, s).wait()

                if following:

                    @pl.when(t == count - 1)
                    def _():
                        if kind == "last":
                            save(t - 1, 1 - s).wait()
                        for f in fetch(following, 0, 0):
                            f.start()

                if kind in ("last", "first"):
                    hidden(kind, t, s)
                    if kind == "last":
                        save(t, s).start()
                    point(kind, t, 0, 1)
                    side(kind, t, s)
                    point(kind, t, SIDE, 1)
                    down(kind, t, s)
                    point(kind, t, DOWN, 1)
                else:
                    {"forward": forward, "da": d_a, "norm": norm}[kind](t, s)
                    if kind != "forward":
                        point(kind, t, 0, 1)
                return carry

            lax.fori_loop(0, count, body, 0)
            if kind == "last":
                save(count - 1, (count - 1) % 2).wait()
        for u in TRIO:
            for c in TRIO:
                it.wait_sends(u, c, flips[0, u, c])

    any_space = pl.BlockSpec(memory_space=pl.ANY)
    return pl.pallas_call(
        kernel,
        out_shape=[jax.ShapeDtypeStruct((LAYERS, 3, 3, CHUNK, LANES), F32), jax.ShapeDtypeStruct((STEPS, TOKENS, 2 * TILE), BF16)]
        + [jax.ShapeDtypeStruct((FF // LANES, TOKENS, LANES), F32)] * 2
        + [jax.ShapeDtypeStruct((TOKENS, D), BF16), jax.ShapeDtypeStruct((D, TOKENS), BF16)],
        in_specs=[any_space] * 5,
        out_specs=[pl.BlockSpec(memory_space=pltpu.VMEM)] + [any_space] * 5,
        scratch_shapes=[
            pltpu.VMEM((TOKENS, D), BF16),
            pltpu.VMEM((TOKENS, D), BF16),
            pltpu.VMEM((D, TOKENS), BF16),
            pltpu.VMEM((X_ROWS, LANES), F32),
            pltpu.VMEM((TILE, TOKENS), BF16),
            pltpu.VMEM((2, TOKENS, 2 * TILE), BF16),
            pltpu.VMEM((2, D, 2 * TILE), BF16),
            pltpu.VMEM((2, TILE, D), BF16),
            pltpu.VMEM((QUARTERS, 2, LT, PART, LANES), F32),
            pltpu.SemaphoreType.DMA((2,)),
            pltpu.SemaphoreType.DMA((5, 2)),
            pltpu.SemaphoreType.DMA((QUARTERS, 2)),
            pltpu.SemaphoreType.DMA((2, TOKENS // TILE)),
            rs.scratch(),
        ],
        compiler_params=pltpu.CompilerParams(collective_id=collective_id, has_side_effects=True, vmem_limit_bytes=VMEM_ALL),
        cost_estimate=pl.CostEstimate(flops=TOKENS * D * FF * 24, bytes_accessed=TOKENS * FF * 20, transcendentals=0),
        name="gradients",
    )(x, dy, wg, wu, wd)[0]


def solution(mesh):
    torus = Torus(4, 4, 8)
    count = float(LAYERS * 3 * D * FF)

    def step(x, dy, wg, wu, wd, mg, mu, md, vg, vu, vd):
        x, dy = x[0], dy[0]
        g = gradients(torus, x, dy, wg, wu, wd, 1)
        G, m, v = step_and_gather(torus, g, (wg, wu, wd), (mg, mu, md), (vg, vu, vd), count, 2)
        return (*unpack(torus, G), *m, *v)

    P = jax.sharding.PartitionSpec
    return jax.shard_map(
        step,
        mesh=mesh,
        in_specs=(P(("rep", "dp")),) * 2 + (P(),) * 3 + (P(None, "dp"),) * 6,
        out_specs=(P("rep"),) * 3 + (P("rep", "dp"),) * 6,
        check_vma=False,
    )
```

```python
import heapq
import jax
import jax.numpy as jnp
from jax import lax
from jax.experimental import pallas as pl
from jax.experimental.pallas import tpu as pltpu

F32, BF16 = jnp.float32, jnp.bfloat16
MESH = pl.DeviceIdType.MESH
RATE, LATENCY = 46.6e3, 2.3
TURN, ADD, HOP = 0.1, 2.0e6, 0.7
WAYS = (1, -1)
TRIO = range(3)
RING, CROSS, DIRECT = TRIO
NEVER, MARGIN, SWEEPS = 1e9, (0.3, 1.2), 3


class Torus:
    def __init__(self, nx, ny, nz):
        self.n = {"x": nx, "y": ny, "z": nz}
        self.size = nx * ny * nz

    def here(self):
        return Here(self)


class Here:
    def __init__(self, torus):
        p, n = lax.axis_index("dp"), torus.n
        ny, nz = n["y"], n["z"]
        mine = {"z": lax.rem(p, nz), "y": lax.rem(lax.div(p, nz), ny), "x": lax.div(p, ny * nz)}
        step = {"z": 1, "y": nz, "x": ny * nz}
        self.at = {d: [mine[d]] + [lax.rem(mine[d] + i, n[d]) for i in range(1, n[d])] for d in n}
        self.to = {d: [p + (self.at[d][i] - mine[d]) * step[d] for i in range(n[d])] for d in n}

    def peer(self, dim, delta):
        return {"dp": self.to[dim][delta % len(self.to[dim])]}

    def up(self, dim, delta):
        return self.at[dim][delta % len(self.at[dim])]


ORDERS = ("zxy", "xyz", "yxz")


def hops(n, flip):
    far, near = n // 2, n - 1 - n // 2
    return {1: near, -1: far} if flip else {1: far, -1: near}


class Balance:
    def __init__(self):
        self.load = {}

    def flip(self, dim, n, size):
        plain = [self.load.get((dim, s), 0) + size * hops(n, False)[s] for s in WAYS]
        turned = [self.load.get((dim, s), 0) + size * hops(n, True)[s] for s in WAYS]
        flip = max(turned) < max(plain)
        self.load[dim, 1], self.load[dim, -1] = turned if flip else plain
        return flip


def simulate(actions, copies):
    links, arrived, order = {}, {}, []
    waiting = {a: set(needs) for a, (needs, _, _, _) in actions.items()}
    by_need = {}
    for a, (needs, _, _, _) in actions.items():
        for c in needs:
            by_need.setdefault(c, []).append(a)
    ready = [(actions[a][3], i, a) for i, a in enumerate(actions) if not waiting[a]]
    rank = {a: i for i, a in enumerate(actions)}
    heapq.heapify(ready)
    now, done = 0.0, {}
    while ready:
        at, _, a = heapq.heappop(ready)
        now = max(now, at) + actions[a][2]
        order.append(a)
        done[a] = now
        for c in [("action", a)] + list(actions[a][1]):
            if c[0] == "action":
                end = now
            else:
                link, size, extra = copies[c]
                start = max(now, links.get(link, 0.0))
                links[link] = start + size / RATE
                end = links[link] + LATENCY + extra
            for b in by_need.get(c, ()):
                waiting[b].discard(c)
                arrived[b] = max(arrived.get(b, 0.0), end)
                if not waiting[b]:
                    heapq.heappush(ready, (max(arrived[b], actions[b][3]), rank[b], b))
    assert len(order) == len(actions), (len(order), len(actions))
    return order, now


def place(actions, copies, segments):
    links, known, left, slots, open_keys = {}, {}, dict(actions), {}, set()
    now = 0.0

    def do(a, where):
        nonlocal now
        _, sends, cost = left.pop(a)
        now += cost
        known["action", a] = now
        for c in sends:
            link, size, extra = copies[c]
            links[link] = max(now, links.get(link, 0.0)) + size / RATE
            known[c] = links[link] + LATENCY + extra
        where.append(a)

    def drain(where, allowed, wait):
        nonlocal now
        while True:
            able = [(max([known.get(c, NEVER) for c in actions[a][0]], default=0.0), i, a) for i, a in enumerate(left) if allowed(a)]
            best, _, a = min(able, default=(NEVER, 0, None))
            if best >= NEVER or not wait and best + MARGIN[a[0][0][0]] > now:
                return
            now = max(now, best)
            do(a, where)

    for key, cost, writes, whole in segments:
        now += cost
        slots[key] = ([], [])
        others = {(l, u, c) for (l, u), c in writes}
        drain(slots[key][0], lambda a: any(a[0][0][1] == u and a[0][1] == c and a[0][0][0] > l for l, u, c in others), True)
        open_keys |= set(whole)
        drain(slots[key][1], lambda a: a[1] != "start" or (a[0], a[2]) in open_keys, False)
    drain(slots[segments[-1][0]][1], lambda a: True, True)
    assert not left
    place.took = now
    return slots


def barrier(me, peers):
    sem = pltpu.get_barrier_semaphore()
    for dim, delta in peers:
        pl.semaphore_signal(sem, inc=1, device_id=me.peer(dim, delta), device_id_type=MESH)
    pl.semaphore_wait(sem, len(peers))


def both_ways(torus, dim):
    n = torus.n[dim]
    return [] if n == 1 else [(dim, 1)] if n == 2 else [(dim, 1), (dim, -1)]


def all_others(torus, dim):
    return [(dim, d) for d in range(1, torus.n[dim])]


class ReduceScatter:
    LANES = (2, 1, 1)

    def __init__(self, torus, rows, units):
        self.t, self.rows, self.units = torus, rows, units
        self.dims = [tuple(order) for order in ORDERS]
        self.nslots = max(self.base(c, DIRECT, 0) + self.sizes(c)[DIRECT] - 1 for c in TRIO)

    def sizes(self, c):
        return [self.t.n[d] for d in self.dims[c]]

    def here(self, c):
        return [self.me.up(d, 0) for d in self.dims[c]]

    def base(self, c, phase, lane):
        n = self.sizes(c)
        return sum((n[i] - 1) * self.LANES[i] for i in range(phase)) + lane * (n[phase] - 1)

    def peers(self):
        full = {dims[DIRECT] for dims in self.dims}
        out = []
        for dim in "xyz":
            out += all_others(self.t, dim) if dim in full else both_ways(self.t, dim)
        return out

    def credit_peers(self, c):
        a, b, d = self.dims[c]
        return both_ways(self.t, a) + both_ways(self.t, b) + all_others(self.t, d)

    def scratch(self):
        n = self.t.n
        t, r1, r2, r3, k2, k3 = [], [], [], [], [], []
        for dims in self.dims:
            n1, n2, n3 = (n[d] for d in dims)
            tail = (self.rows, 128)
            t.append(pltpu.VMEM((self.units, n1, n2 * n3) + tail, BF16))
            r1.append(pltpu.VMEM((self.units, max(n1 - 1, 1), n2 * n3) + tail, BF16))
            r2.append(pltpu.VMEM((self.units, max(n2 - 1, 1), n3) + tail, BF16))
            r3.append(pltpu.VMEM((self.units, max(n3 - 1, 1)) + tail, BF16))
            k2.append(pltpu.VMEM((self.units, n3) + tail, F32))
            k3.append(pltpu.VMEM((self.units,) + tail, F32))
        sems = [pltpu.SemaphoreType.DMA((self.units, 3, self.nslots)), pltpu.SemaphoreType.DMA((self.units, 3, self.nslots)), pltpu.SemaphoreType.REGULAR((self.units, 3))]
        return [t, r1, r2, r3, k2, k3] + sems

    def slot(self, c, phase, sign, h):
        return h if sign > 0 else self.sizes(c)[phase] - 2 - h

    def flips(self, balance, c):
        n1, n2, n3 = self.sizes(c)
        block, (a, b, d) = self.rows * 256, self.dims[c]
        for rel in range(1, n3):
            link = d, 1 if rel <= n3 // 2 else -1
            balance.load[link] = balance.load.get(link, 0) + block * min(rel, n3 - rel)
        ring = [balance.flip(a, n1, block * n2 * n3 // self.LANES[RING]) for _ in range(self.LANES[RING])]
        return ring, [balance.flip(b, n2, block * n3)]

    def plan(self, unit, c, flip):
        n = self.sizes(c)
        n1, n2, n3 = n
        block = self.rows * 256
        size = [block * n2 * n3 // self.LANES[RING], block * n3, block]
        actions, copies = {}, {}
        key = (unit, c)

        def send(phase, lane, sign, h):
            cid = ("copy", key, phase, lane, sign, h)
            copies[cid] = ((self.dims[c][phase], sign), size[phase], 0)
            return cid

        first, last = [[], []], [[], []]
        for phase in (RING, CROSS):
            for lane, turned in enumerate(flip[phase]):
                k = hops(n[phase], turned)
                ways = [s for s in WAYS if k[s]]
                first[phase] += [send(phase, lane, s, k[s] - 1) for s in ways]
                last[phase] += [("copy", key, phase, lane, s, 0) for s in ways]
                for s in ways:
                    for h in range(k[s] - 1, 0, -1):
                        actions[key, "step", phase, lane, s, h] = ([("copy", key, phase, lane, s, h)], [send(phase, lane, s, h - 1)], size[phase] / ADD)
        direct = []
        for rel in range(1, n3):
            cid = ("copy", key, DIRECT, 0, 0, rel)
            far = min(rel, n3 - rel)
            copies[cid] = ((self.dims[c][DIRECT], 1 if rel <= n3 // 2 else -1), size[DIRECT] * far, HOP * (far - 1))
            direct.append(cid)
        sends = first + [direct, []]
        for lane in range(self.LANES[RING]):
            actions[key, "start", lane] = ([], [x for x in sends[RING] if x[3] == lane], TURN)
        before = (key, "start", 0)
        for phase, needs in enumerate(last + [direct]):
            a = (key, "end", phase)
            actions[a] = (needs + [("action", before)], sends[phase + 1], size[phase] * self.LANES[phase] / ADD + TURN)
            before = a
        return actions, copies

    def bind(self, me, refs):
        self.me, (self.T, self.R1, self.R2, self.R3, self.K2, self.K3, self.ssem, self.rsem, self.credit) = me, refs
        return self

    def remote(self, u, c, phase, lane, sign, h):
        n1, n2, n3 = self.sizes(c)
        d1, d2, d3 = self.dims[c]
        up = self.me.up
        mine = self.T[c].at[u]
        slot = h - 1 if phase == DIRECT else self.slot(c, phase, sign, h)
        if phase == RING:
            part = n2 * n3 // self.LANES[RING]
            blocks = pl.ds(lane * part, part)
            src, dst = mine.at[up(d1, sign * (h + 1)), blocks], self.R1[c].at[u, slot, blocks]
        elif phase == CROSS:
            src, dst = mine.at[up(d1, 0), pl.ds(up(d2, sign * (h + 1)) * n3, n3)], self.R2[c].at[u, slot]
        else:
            sign = h
            src, dst = mine.at[up(d1, 0), up(d2, 0) * n3 + up(d3, h)], self.R3[c].at[u, slot]
        s = self.base(c, phase, lane) + slot
        to = self.me.peer(self.dims[c][phase], sign)
        return pltpu.make_async_remote_copy(src_ref=src, dst_ref=dst, send_sem=self.ssem.at[u, c, s], recv_sem=self.rsem.at[u, c, s], device_id=to, device_id_type=MESH)

    def all_sends(self, c, flip):
        n = self.sizes(c)
        out = []
        for phase in (RING, CROSS):
            for lane, turned in enumerate(flip[phase]):
                k = hops(n[phase], turned)
                out += [(phase, lane, s, h) for s in WAYS for h in range(k[s])]
        return out + [(DIRECT, 0, 0, rel) for rel in range(1, n[DIRECT])]

    def run(self, u, c, flip, what, store):
        n = self.sizes(c)
        n1, n2, n3 = n
        m1, m2, m3 = self.here(c)
        T, R1, R2, R3 = (r[c].at[u] for r in (self.T, self.R1, self.R2, self.R3))
        K2, K3 = self.K2[c].at[u], self.K3[c].at[u]
        mine = T.at[m1]
        wide = lambda v: v.astype(F32)
        go = lambda *a: self.remote(u, c, *a)

        def loop(count, body):
            def one(i, carry):
                body(i)
                return carry

            lax.fori_loop(0, count, one, 0)

        def line(q):
            return pl.ds(q * n3, n3)

        def ways(phase):
            for lane, turned in enumerate(flip[phase]):
                k = hops(n[phase], turned)
                for s in WAYS:
                    if k[s]:
                        yield lane, s, k[s]

        def sends(phase, only=None):
            for lane, s, k in ways(phase):
                if only in (None, lane):
                    go(phase, lane, s, k - 1).start()

        def arrived(phase):
            got = set()
            for lane, s, _ in ways(phase):
                go(phase, lane, s, 0).wait_recv()
                got.add(self.slot(c, phase, s, 0))
            return sorted(got)

        kind, *where = what
        if kind == "start":
            sends(RING, *where)
        elif kind == "step":
            phase, lane, s, h = where
            go(*where).wait_recv()
            slot = self.slot(c, phase, s, h)
            q = self.me.up(self.dims[c][phase], s * h)
            if phase == RING:
                lines = n2 // self.LANES[RING]

                def add(i):
                    b = line(lane * lines + i)
                    T[q, b] = (wide(T[q, b]) + wide(R1[slot, b])).astype(BF16)

                loop(lines, add)
            else:
                mine[line(q)] = (wide(mine[line(q)]) + wide(R2[slot])).astype(BF16)
            go(phase, lane, s, h - 1).start()
        elif where == [RING]:
            got = arrived(RING)

            def total(b):
                return sum((wide(R1[g, b]) for g in got), wide(mine[b]))

            def others(i):
                b = line(lax.rem(m2 + 1 + i, n2))
                mine[b] = total(b).astype(BF16)

            loop(n2 - 1, others)
            sends(CROSS)
            K2[...] = total(line(m2))
        elif where == [CROSS]:
            got = arrived(CROSS)
            total = sum((wide(R2[g]) for g in got), K2[...])
            K2[...] = total
            mine[line(m2)] = total.astype(BF16)
            for rel in range(1, n3):
                go(DIRECT, 0, 0, rel).start()
            K3[...] = K2[m3]
        else:
            for rel in range(1, n3):
                go(DIRECT, 0, 0, rel).wait_recv()
            store(sum((wide(R3[i]) for i in range(n3 - 1)), K3[...]).astype(BF16).astype(F32))

    def wait_sends(self, u, c, flip):
        for a in self.all_sends(c, flip):
            self.remote(u, c, *a).wait_send()

    def give_credit(self, u, c):
        for dim, delta in self.credit_peers(c):
            pl.semaphore_signal(self.credit.at[u, c], inc=1, device_id=self.me.peer(dim, delta), device_id_type=MESH)

    def take_credit(self, u, c):
        pl.semaphore_wait(self.credit.at[u, c], len(self.credit_peers(c)))


class AllGather:
    def __init__(self, torus, block_bytes, split=4):
        self.t, self.bytes, self.split = torus, block_bytes, split
        self.dims = [tuple(order) for order in ORDERS]
        self.flip, self.balance = {}, Balance()
        self.build()
        for key in list(self.flip) * SWEEPS:
            took = self.took
            self.flip[key] = not self.flip[key]
            self.build()
            if self.took >= took:
                self.flip[key] = not self.flip[key]
        self.build()

    def build(self):
        self.copies, self.actions, self.index = {}, {}, {}
        for c in TRIO:
            self.plan(c)
        self.order, self.took = simulate({a: (*v, 0) for a, v in self.actions.items()}, self.copies)

    def peers(self):
        return [p for dim in "xyz" for p in both_ways(self.t, dim)]

    def pieces(self, c, j):
        n3 = self.t.n[self.dims[c][DIRECT]]
        return n3 if not j else self.split if n3 % self.split == 0 else 1

    def size(self, c, phase, j):
        line = self.bytes * self.t.n[self.dims[c][DIRECT]]
        return self.bytes if phase == DIRECT else line // self.pieces(c, 1 if phase == CROSS else j)

    def k(self, c, phase, j, i):
        dim = self.dims[c][phase]
        key = (c, phase, j, i)
        if key not in self.flip:
            self.flip[key] = self.balance.flip(dim, self.t.n[dim], self.size(c, phase, j))
        return hops(self.t.n[dim], self.flip[key])

    def plan(self, c):
        n1, n2, n3 = (self.t.n[d] for d in self.dims[c])

        def send(where, s, h):
            phase, j, _ = where
            cid = (c, where, s, h)
            self.copies[cid] = ((self.dims[c][phase], s), self.size(c, phase, j), 0)
            self.index[cid] = len(self.index)
            return cid

        def own(*where):
            k = self.k(c, *where)
            return [send(where, s, 1) for s in WAYS if k[s]]

        def passing(*where):
            k = self.k(c, *where)
            for s in WAYS:
                for h in range(1, k[s] + 1):
                    yield s, h, (c, "pass", where, s, h), [(c, where, s, h)], [send(where, s, h + 1)] if h < k[s] else []

        def act(a, needs, sends):
            self.actions[a] = (needs, sends, TURN / 2)

        act((c, "start"), [], own(DIRECT, 0, 0) + own(RING, 0, 0))
        got = [("action", (c, "start"))]
        for s, h, a, needs, sends in passing(DIRECT, 0, 0):
            act(a, needs, sends + own(RING, 0, (-s * h) % n3))
            got.append(("action", a))
        parts = range(self.pieces(c, 1))
        act((c, "line"), got, [x for i in parts for x in own(CROSS, 0, i)])
        for i in parts:
            for s, h, a, needs, sends in passing(CROSS, 0, i):
                after = (-s * h) % n2, i
                if c:
                    act(a, needs, sends + own(RING, *after))
                else:
                    act(a, needs, sends)
                    act((c, "later", *after), [("action", x) for x in (a, (1, "line"), (2, "line"))], own(RING, *after))
        for j in range(n2):
            for i in range(self.pieces(c, j)):
                for _, _, a, needs, sends in passing(RING, j, i):
                    act(a, needs, sends)

    def bind(self, me, G, ssem, rsem):
        self.me, self.G, self.ssem, self.rsem = me, G, ssem, rsem
        return self

    def remote(self, cid, back):
        c, (phase, j, i), s, h = cid
        d1, d2, d3 = self.dims[c]
        n3, up = self.t.n[d3], self.me.up
        off = s * (back - h)
        G = self.G[c]
        if phase == DIRECT:
            ref = G.at[up(d1, 0), up(d2, 0) * n3 + up(d3, off)]
        elif phase == CROSS:
            size = n3 // self.pieces(c, 1)
            ref = G.at[up(d1, 0), pl.ds(up(d2, off) * n3 + i * size, size)]
        elif j == 0:
            ref = G.at[up(d1, off), up(d2, 0) * n3 + up(d3, i)]
        else:
            size = n3 // self.pieces(c, j)
            ref = G.at[up(d1, off), pl.ds(up(d2, j) * n3 + i * size, size)]
        x = self.index[cid]
        return pltpu.make_async_remote_copy(src_ref=ref, dst_ref=ref, send_sem=self.ssem.at[x], recv_sem=self.rsem.at[x], device_id=self.me.peer(self.dims[c][phase], s), device_id_type=MESH)

    def run(self, a):
        needs, sends, _ = self.actions[a]
        for cid in needs:
            if cid in self.index:
                self.remote(cid, 0).wait_recv()
        for cid in sends:
            self.remote(cid, 1).start()

    def wait_sends(self):
        for cid in self.copies:
            self.remote(cid, 1).wait_send()


MIB = 2**20
VMEM_ALL = 67043328
LAYERS, D, FF = 2, 896, 2560
LANES, ROWS, CHUNK = 128, 144, 48
HIGH = {0: 7, 1: 7, 2: 20}
WIDE = {0: FF, 1: FF, 2: D}
WINDOW = (16, 16, 24)


HALVES, RING_TILES = 2, 8
COLOURS = {0: (1, 2, 0), 1: (1, 2, 0), 2: (0, 1, 2)}
TOKENS, TILE, PART = 2048, 256, 512
LT, STEPS = TILE // LANES, FF // TILE
HALF = STEPS // HALVES


def home(u, ct):
    if u == HALVES:
        return u, ct
    t, k = divmod(ct, 2 * LT)
    m, j = divmod(k, LT)
    return m, (u * HALF + t) * LT + j


def tiles(u):
    high, wide = HIGH[u], WIDE[u] // LANES
    out = []
    for k in range(ROWS // 8):
        ct, row = divmod(8 * k, high)
        out.append((ct, row, min(8, high - row), ct + 1 < wide))
    return out


def pack(torus, u, X, base, parts, first, count, outs, colours):
    high, ny, nz = HIGH[u], torus.n["y"], torus.n["z"]
    sub = lax.broadcasted_iota(jnp.int32, (8, LANES), 0)
    got = tiles(u)

    def body(line, carry):
        x, y = lax.div(first + line, ny), lax.rem(first + line, ny)
        top = pl.multiple_of(line * (high * nz), 8)

        def piece(z, ct, row, whole, more):
            a = X[pl.ds(top + (base(ct) + high * z + row), 8), :]
            if whole == 8:
                return a
            b = X[pl.ds(top + (base(ct + 1) + high * z - whole), 8), :] if more else jnp.zeros((8, LANES), F32)
            return jnp.where(sub < whole, a, b)

        for z in range(nz):
            at = {"x": x, "y": y, "z": z}
            for j in parts:
                both = jnp.concatenate([piece(z, *got[2 * j]), piece(z, *got[2 * j + 1])], axis=0).astype(BF16)
                k, r = divmod(16 * j, CHUNK)
                c = colours[k]
                d1, d2, d3 = ORDERS[c]
                outs[c][at[d1], at[d2] * torus.n[d3] + at[d3], pl.ds(r, 16), :] = both
        return carry

    lax.fori_loop(0, count, body, 0)


def pieces_shapes(torus, dtype, *mid):
    out = []
    for order in ORDERS:
        a, b, d = (torus.n[x] for x in order)
        out.append(jax.ShapeDtypeStruct((a, b * d) + mid + (CHUNK, LANES), dtype))
    return out


def step_and_gather(torus, g, w, m, v, count, collective_id):
    ag = AllGather(torus, LAYERS * 3 * CHUNK * 256)
    dims = "zxy"
    slots = {d: torus.n[d] - 1 for d in dims}

    def window(p, x):
        rows = WINDOW[x]
        first = lax.div(p * HIGH[x], 8) * 8
        return pl.multiple_of(jnp.minimum(first, HIGH[x] * torus.size - rows), 8), rows

    def kernel(g_ref, *refs):
        w_in, m_in, v_in, G, m_out, v_out = (refs[i : i + 3] for i in range(0, 18, 3))
        flat, wflat, part, E, esend, erecv, ssem, rsem, win, wide_win, wsem = refs[18:]
        me = torus.here()
        p = lax.axis_index("dp")
        loads = []
        for x in TRIO:
            first, rows = window(p, x)
            loads.append(pltpu.make_async_copy(w_in[x].at[:, pl.ds(first, rows)], win[x], wsem.at[x]))
            loads[x].start()
        barrier(me, [p for d in "xyz" for p in all_others(torus, d)])
        for x in TRIO:
            loads[x].wait()
            for lt in range(WIDE[x] // LANES):
                wide_win[x][:, lt] = win[x][:, :, pl.ds(lt * LANES, LANES)].astype(F32)
        acc = jnp.zeros((8, LANES), F32)
        for l in range(LAYERS):
            for u in TRIO:
                for k, c in enumerate(COLOURS[u]):
                    value = g_ref[l, u, c]
                    flat[l, u, pl.ds(k * CHUNK, CHUNK), :] = value
                    for r in range(0, CHUNK, 8):
                        acc = acc + value[r : r + 8] * value[r : r + 8]
        part[0] = acc
        base = 0
        for i, d in enumerate(dims):
            n = torus.n[d]
            copies = []
            for rel in range(1, n):
                s = base + rel - 1
                copies.append(pltpu.make_async_remote_copy(src_ref=part.at[i], dst_ref=E.at[s], send_sem=esend.at[s], recv_sem=erecv.at[s], device_id=me.peer(d, rel), device_id_type=MESH))
            for copy in copies:
                copy.start()
            total = part[i]
            for rel in range(1, n):
                copies[rel - 1].wait_recv()
                total = total + E[base + rel - 1]
            part[i + 1] = total
            for copy in copies:
                copy.wait_send()
            base += n - 1
        mean = jnp.sum(part[3], keepdims=True) / count
        factor = jnp.minimum(1.0, 0.5 * lax.rsqrt(mean + 1e-30))
        for l in range(LAYERS):
            for u in TRIO:
                high = HIGH[u]
                wflat[l, u, pl.ds(ROWS - 8, 8), :] = jnp.zeros((8, LANES), F32)
                for ct in range(WIDE[u] // LANES):
                    x, lt = home(u, ct)
                    at = (slice(None), l, pl.ds(lt * LANES, LANES))
                    grad = flat[l, u, pl.ds(ct * high, high), :] * factor
                    new_m = 0.9 * m_in[x][at] + 0.1 * grad
                    new_v = 0.95 * v_in[x][at] + 0.05 * grad * grad
                    wide = wide_win[x][l, lt, pl.ds(p * high - window(p, x)[0], high), :]
                    new_w = wide - 0.02 * (new_m * lax.rsqrt(new_v + 1e-8) + 0.1 * wide)
                    m_out[x][at] = new_m
                    v_out[x][at] = new_v
                    wflat[l, u, pl.ds(ct * high, high), :] = new_w
        it = ag.bind(me, G, ssem, rsem)
        for u in TRIO:
            for k, c in enumerate(COLOURS[u]):
                a, b, d = (me.up(x, 0) for x in ORDERS[c])
                for l in range(LAYERS):
                    G[c][a, b * torus.n[ORDERS[c][DIRECT]] + d, l, u] = wflat[l, u, pl.ds(k * CHUNK, CHUNK), :].astype(BF16)
        for a in ag.order:
            it.run(a)
        it.wait_sends()

    vmem = pl.BlockSpec(memory_space=pltpu.VMEM)
    nsum = sum(slots.values())
    shapes = pieces_shapes(torus, BF16, LAYERS, 3)
    turn = lambda ts: [jnp.transpose(t, (1, 0, 2)) for t in ts]
    m, v = turn(m), turn(v)
    f32 = [jax.ShapeDtypeStruct(t.shape, F32) for t in m]
    k = len(ag.copies)
    got = pl.pallas_call(
        kernel,
        out_shape=[pltpu.MemorySpace.VMEM(s.shape, s.dtype) for s in shapes + f32 * 2],
        in_specs=[vmem] + [pl.BlockSpec(memory_space=pl.ANY)] * 3 + [vmem] * 6,
        out_specs=[vmem] * 9,
        scratch_shapes=[
            pltpu.VMEM((LAYERS, 3, ROWS, LANES), F32),
            pltpu.VMEM((LAYERS, 3, ROWS, LANES), F32),
            pltpu.VMEM((4, 8, LANES), F32),
            pltpu.VMEM((nsum, 8, LANES), F32),
            pltpu.SemaphoreType.DMA((nsum,)),
            pltpu.SemaphoreType.DMA((nsum,)),
            pltpu.SemaphoreType.DMA((k,)),
            pltpu.SemaphoreType.DMA((k,)),
            [pltpu.VMEM((LAYERS, WINDOW[x], WIDE[x]), BF16) for x in TRIO],
            [pltpu.VMEM((LAYERS, WIDE[x] // LANES, WINDOW[x], LANES), F32) for x in TRIO],
            pltpu.SemaphoreType.DMA((3,)),
        ],
        compiler_params=pltpu.CompilerParams(collective_id=collective_id, has_side_effects=True, vmem_limit_bytes=26 * MIB),
        name="step_and_gather",
    )(g, *w, *m, *v)
    return got


def unpack(torus, got):
    nx, ny, nz = (torus.n[d] for d in "xyz")
    pair = 2
    group = pair * nz
    groups = torus.size // group
    pairs = ny // pair

    def kernel(g0, g1, g2, *refs):
        moments, outs, kept, (Z, Y, sem) = refs[:6], refs[6:9], refs[9:15], refs[15:]
        l, s = pl.program_id(0), pl.program_id(1)
        copies = [pltpu.make_async_copy(src, dst, sem.at[i]) for i, (src, dst) in enumerate(zip(moments, kept))]

        @pl.when(l + s == 0)
        def _():
            for copy in copies:
                copy.start()

        @pl.when(l + s == LAYERS - 1 + groups - 1)
        def _():
            for copy in copies:
                copy.wait()

        corner = {"x": lax.div(s, pairs), "y": lax.rem(s, pairs) * pair, "z": 0}
        for u in TRIO:
            high, wide = HIGH[u], WIDE[u] // LANES
            for i in range(group):
                y, z = divmod(i, nz)
                at = corner | {"y": corner["y"] + y, "z": z}
                for k, c in enumerate(COLOURS[u]):
                    a, b, d = ORDERS[c]
                    Z[i, pl.ds(k * CHUNK, CHUNK), :] = (g0, g1, g2)[c][at[a], at[b] * torus.n[d] + at[d], l, u].astype(F32)
            for i in range(group):
                for ct in range(wide):
                    for r in range(0, high, 8):
                        Y[ct, pl.ds(high * i + r, 8), :] = Z[i, pl.ds(high * ct + r, 8), :]
            rows = high * group
            for ct in range(wide):
                x, lt = home(u, ct)
                outs[x][0, :, pl.ds(lt * LANES, LANES)] = Y[ct, pl.ds(0, rows), :].astype(BF16)

    shapes = [(LAYERS, HIGH[u] * torus.size, WIDE[u]) for u in TRIO]
    return pl.pallas_call(
        kernel,
        grid=(LAYERS, groups),
        out_shape=[jax.ShapeDtypeStruct(s, BF16) for s in shapes] + [jax.ShapeDtypeStruct(m.shape, F32) for m in got[3:]],
        in_specs=[pl.BlockSpec(memory_space=pltpu.VMEM)] * 9,
        out_specs=[pl.BlockSpec((1, HIGH[u] * group, WIDE[u]), lambda l, s: (l, s, 0)) for u in TRIO] + [pl.BlockSpec(memory_space=pl.ANY)] * 6,
        scratch_shapes=[
            pltpu.VMEM((group, ROWS + 8, LANES), F32),
            pltpu.VMEM((FF // LANES, HIGH[2] * group + 8, LANES), F32),
            pltpu.SemaphoreType.DMA((6,)),
        ],
        compiler_params=pltpu.CompilerParams(vmem_limit_bytes=26 * MIB),
        name="unpack",
    )(*got)


NN, NT = ((1,), (0,)), ((1,), (1,))


def dot(a, b, dims=NN):
    return lax.dot_general(a, b, (dims, ((), ())), preferred_element_type=F32)


def scale_of(wide):
    return lax.rsqrt(jnp.mean(wide * wide, -1, keepdims=True) + 1e-6)


GAP = 24
SIDE_STRIDE, DOWN_STRIDE = D + GAP, FF // HALVES + GAP
DOWN_BASE = RING_TILES * SIDE_STRIDE
X_ROWS = DOWN_BASE + D // LANES * DOWN_STRIDE
COST = {"last": (3.5, 3.5), "first": (1.8, 3.5), "da": (2.5,), "norm": (0.45,)}
PACK_DOWN = 0.4
WHOLE = ((0,), (1, 2), (3, 4), (5, 6), (7, 8))
CHUNKS = {1: 0, 3: 1, 4: 2}
PASSES = ("forward", "last", "da", "norm", "first")
COUNT = {"forward": STEPS, "last": STEPS, "da": STEPS, "norm": TOKENS // TILE, "first": STEPS}
QUARTERS = TOKENS // PART
MAKE = 1


def timeline():
    out, lanes = [], ReduceScatter.LANES[RING]
    for kind in PASSES[1:]:
        layer = {"last": 1, "first": 0}.get(kind)
        for t in range(COUNT[kind]):
            half, tt = divmod(t, HALF)
            for i, cost in enumerate(COST[kind]):
                writes, whole = [], []
                if i == MAKE:
                    unit = (layer, half)
                    if tt == 0:
                        writes += [(unit, c) for c in TRIO]
                    if tt in CHUNKS:
                        whole += [((unit, COLOURS[half][CHUNKS[tt]]), lane) for lane in range(lanes)]
                    if tt == HALF - 1:
                        cost += PACK_DOWN
                        mine = [((layer, HALVES), c) for c in TRIO]
                        writes += [] if half else mine
                        whole += [(key, lane) for key in mine for lane in range(lanes) if half or lane == 0 and ORDERS[key[1]][CROSS] == "x"]
                out.append(((kind, t, i), cost, writes, whole))
    return out


def hidden_back(gate, up, d):
    s = jax.nn.sigmoid(gate)
    act = gate * s
    return (act * up).astype(BF16), (d * up * (s + act * (1.0 - s))).astype(BF16), (d * act).astype(BF16)


def gradients(torus, x, dy, wg, wu, wd, collective_id):
    rs = ReduceScatter(torus, CHUNK, 3)
    actions, copies, balance, flips = {}, {}, Balance(), {}
    for l in range(LAYERS):
        for u in TRIO:
            for c in TRIO:
                flips[l, u, c] = rs.flips(balance, c)
                got, sent = rs.plan((l, u), c, flips[l, u, c])
                copies |= sent
                actions |= got
                if l:
                    key = ((l, u), c)
                    actions[key, "free"] = ([("action", (key, "end", DIRECT))], [], TURN)
    slots = place(actions, copies, timeline())
    lines = torus.n["x"] * torus.n["y"]

    def kernel(x_ref, dy_ref, wg_ref, wu_ref, wd_ref, out, both_ref, gate_ref, up_ref, h1_ref, at0_ref, dyv, av, at, X, Mb, Db, Wb, Vb, Hb, once, pair, hsem, rsem, rsc):
        me = torus.here()
        it = rs.bind(me, rsc)
        copy = pltpu.make_async_copy
        load_x = copy(x_ref, dyv, once.at[0])
        save_at0, load_at0 = copy(at, at0_ref, once.at[1]), copy(at0_ref, at, once.at[1])

        def part(i):
            return pl.ds(i * TILE if isinstance(i, int) else pl.multiple_of(i * TILE, TILE), TILE)

        def sides(layer, t, s):
            return [copy(ref.at[layer, :, part(t)], Wb.at[s, :, part(k)], pair.at[k, s]) for k, ref in enumerate((wg_ref, wu_ref))]

        def fetch(kind, t, s):
            both, rows = pair.at[2, s], pair.at[3, s]
            if kind == "forward":
                return sides(0, t, s) + [copy(wd_ref.at[0, part(t)], Vb.at[s], rows)]
            if kind == "last":
                return sides(1, t, s) + [copy(wd_ref.at[1, part(t)], Vb.at[s], rows)]
            if kind == "da":
                return sides(1, t, s) + [copy(both_ref.at[t], Db.at[s], both)]
            if kind == "norm":
                return [copy(h1_ref.at[part(t)], Vb.at[s], rows)]
            return [copy(wd_ref.at[0, part(t)], Vb.at[s], rows)]

        def save(t, s):
            return copy(Db.at[s], both_ref.at[t], pair.at[4, s])

        def hiddens(t, quarters, out=False):
            got = []
            for q in quarters:
                for k, ref in enumerate((gate_ref, up_ref)):
                    ends = ref.at[pl.ds(t * LT, LT), pl.ds(q * PART, PART)], Hb.at[q, k]
                    got.append(copy(*(ends[::-1] if out else ends), hsem.at[q, k]))
            return got

        def act(a):
            ((l, u), c), what = a[0], a[1:]
            if what[0] == "free":
                it.wait_sends(u, c, flips[l, u, c])
                it.give_credit(u, c)
                return
            if what == ("start", 0) and l == 0:
                it.take_credit(u, c)

            def store(value):
                out[l, u, c] = value

            it.run(u, c, flips[l, u, c], what, store)

        def point(kind, t, i, which):
            for k in range(COUNT[kind]):
                if slots[kind, k, i][which]:

                    @pl.when(t == k)
                    def _(k=k):
                        for a in slots[kind, k, i][which]:
                            act(a)

        def normed_into(r):
            wide = dyv[part(r), :].astype(F32)
            a = (wide * scale_of(wide)).astype(BF16)
            av[part(r), :] = a
            at[:, part(r)] = a.T

        def lanes_of(ct):
            return slice(ct * LANES, (ct + 1) * LANES)

        def forward(t, s):
            for first in range(0, QUARTERS, 2):
                quarters = range(first, first + 2)

                @pl.when(t > 0)
                def _():
                    for f in hiddens(t - 1, quarters, True):
                        f.wait()

                for q in quarters:
                    rows = pl.ds(q * PART, PART)
                    both = dot(av[rows, :], Wb[s])
                    gate, up = both[:, :TILE], both[:, TILE:]
                    for j in range(LT):
                        Hb[q, 0, j], Hb[q, 1, j] = gate[:, lanes_of(j)], up[:, lanes_of(j)]
                    got = dot((jax.nn.silu(gate) * up).astype(BF16), Vb[s])
                    for ct in range(D // LANES):
                        here = pl.ds(ct * TOKENS + q * PART, PART)
                        X[here, :] = jnp.where(t == 0, 0.0, X[here, :]) + got[:, lanes_of(ct)]
                for f in hiddens(t, quarters, True):
                    f.start()

        def turn():
            for f in hiddens(STEPS - 1, range(QUARTERS), True):
                f.wait()
            save_at0.wait()
            count = TOKENS // TILE

            def saves(r):
                return copy(dyv.at[part(r)], h1_ref.at[part(r)], rsem.at[0, r])

            def loads(r):
                return copy(dy_ref.at[part(r)], dyv.at[part(r)], rsem.at[1, r])

            @pl.loop(0, count)
            def _(r):
                total = jnp.concatenate([X[pl.ds(ct * TOKENS + r * TILE, TILE), :] for ct in range(D // LANES)], axis=1)
                dyv[part(r), :] = dyv[part(r), :] + total.astype(BF16)
                normed_into(r)
                saves(r).start()

                @pl.when(r > 0)
                def _():
                    saves(r - 1).wait()
                    loads(r - 1).start()

            saves(count - 1).wait()
            loads(count - 1).start()
            for r in range(count):
                loads(r).wait()

        def hidden(kind, t, s):
            for first in range(0, QUARTERS, 2):
                quarters = range(first, first + 2)
                if kind == "first":
                    for f in hiddens(t, quarters):
                        f.wait()
                for q in quarters:
                    rows = pl.ds(q * PART, PART)
                    if kind == "last":
                        both = dot(av[rows, :], Wb[s])
                        gate, up = both[:, :TILE], both[:, TILE:]
                    else:
                        gate, up = (jnp.concatenate([Hb[q, k, j] for j in range(LT)], axis=1) for k in range(2))
                    d = dot(dyv[rows, :], Vb[s], NT).astype(BF16).astype(F32)
                    mid, Db[s, rows, part(0)], Db[s, rows, part(1)] = hidden_back(gate, up, d)
                    Mb[:, rows] = mid.T
                if kind == "first":

                    @pl.when(t + 1 < STEPS)
                    def _():
                        for f in hiddens(t + 1, quarters):
                            f.start()

        def make(kind, t, s):
            half, tt = lax.div(t, HALF), lax.rem(t, HALF)
            got = dot(at[...], Db[s])
            for k in range(2 * LT):
                X[pl.ds((lax.rem(tt, 2) * 2 * LT + k) * SIDE_STRIDE + 8, D), :] = got[:, lanes_of(k)]
            got = dot(Mb[...], dyv[...])
            for ct in range(D // LANES):
                X[pl.ds(DOWN_BASE + ct * DOWN_STRIDE + 8 + tt * TILE, TILE), :] = got[:, lanes_of(ct)]
            point(kind, t, MAKE, 0)
            for v, parts in enumerate(WHOLE):

                @pl.when(tt == v)
                def _(parts=parts):
                    pack(torus, 0, X, lambda ct: ct % RING_TILES * SIDE_STRIDE + 8, parts, 0, lines, [T.at[half] for T in it.T], COLOURS[0])

            @pl.when(tt == HALF - 1)
            def _():
                some = lines // HALVES
                pack(torus, HALVES, X, lambda ct: DOWN_BASE + ct * DOWN_STRIDE + 8, range(ROWS // 16), half * some, some, [T.at[HALVES] for T in it.T], COLOURS[HALVES])

        def d_a(t, s):
            for r in range(0, TOKENS, PART):
                got = dot(Db[s, pl.ds(r, PART), :], Wb[s], NT)
                for ct in range(D // LANES):
                    rows = pl.ds(ct * TOKENS + r, PART)
                    X[rows, :] = jnp.where(t == 0, 0.0, X[rows, :]) + got[:, lanes_of(ct)]

        def norm(t, s):
            da = jnp.concatenate([X[pl.ds(ct * TOKENS + t * TILE, TILE), :] for ct in range(D // LANES)], axis=1).astype(BF16).astype(F32)
            wide = Vb[s].astype(F32)
            scale = scale_of(wide)
            inner = jnp.mean(da * wide, -1, keepdims=True)
            dyv[part(t), :] = dyv[part(t), :] + (scale * da - wide * (scale * scale * scale * inner)).astype(BF16)

        for f in fetch("forward", 0, 0) + [load_x]:
            f.start()
        barrier(me, rs.peers())
        load_x.wait()

        @pl.loop(0, TOKENS // TILE)
        def _(r):
            normed_into(r)

        save_at0.start()
        for number, kind in enumerate(PASSES):
            count = COUNT[kind]
            following = PASSES[number + 1] if number + 1 < len(PASSES) else None
            if kind == "last":
                turn()
            if kind == "da":
                load_at0.start()
            if kind == "norm":
                for f in hiddens(0, range(QUARTERS)):
                    f.start()
            if kind == "first":
                load_at0.wait()

            def body(t, carry, kind=kind, count=count, following=following):
                s = lax.rem(t, 2)
                for f in fetch(kind, t, s):
                    f.wait()

                @pl.when(t + 1 < count)
                def _():
                    for f in fetch(kind, t + 1, 1 - s):
                        f.start()

                if kind == "last":

                    @pl.when(t > 1)
                    def _():
                        save(t - 2, s).wait()

                if following:

                    @pl.when(t == count - 1)
                    def _():
                        if kind == "last":
                            save(t - 1, 1 - s).wait()
                        for f in fetch(following, 0, 0):
                            f.start()

                if kind in ("last", "first"):
                    hidden(kind, t, s)
                    if kind == "last":
                        save(t, s).start()
                    point(kind, t, 0, 1)
                    make(kind, t, s)
                    point(kind, t, MAKE, 1)
                else:
                    {"forward": forward, "da": d_a, "norm": norm}[kind](t, s)
                    if kind != "forward":
                        point(kind, t, 0, 1)
                return carry

            lax.fori_loop(0, count, body, 0)
            if kind == "last":
                save(count - 1, (count - 1) % 2).wait()
        for u in TRIO:
            for c in TRIO:
                it.wait_sends(u, c, flips[0, u, c])

    any_space = pl.BlockSpec(memory_space=pl.ANY)
    return pl.pallas_call(
        kernel,
        out_shape=[jax.ShapeDtypeStruct((LAYERS, 3, 3, CHUNK, LANES), F32), jax.ShapeDtypeStruct((STEPS, TOKENS, 2 * TILE), BF16)]
        + [jax.ShapeDtypeStruct((FF // LANES, TOKENS, LANES), F32)] * 2
        + [jax.ShapeDtypeStruct((TOKENS, D), BF16), jax.ShapeDtypeStruct((D, TOKENS), BF16)],
        in_specs=[any_space] * 5,
        out_specs=[pl.BlockSpec(memory_space=pltpu.VMEM)] + [any_space] * 5,
        scratch_shapes=[
            pltpu.VMEM((TOKENS, D), BF16),
            pltpu.VMEM((TOKENS, D), BF16),
            pltpu.VMEM((D, TOKENS), BF16),
            pltpu.VMEM((X_ROWS, LANES), F32),
            pltpu.VMEM((TILE, TOKENS), BF16),
            pltpu.VMEM((2, TOKENS, 2 * TILE), BF16),
            pltpu.VMEM((2, D, 2 * TILE), BF16),
            pltpu.VMEM((2, TILE, D), BF16),
            pltpu.VMEM((QUARTERS, 2, LT, PART, LANES), F32),
            pltpu.SemaphoreType.DMA((2,)),
            pltpu.SemaphoreType.DMA((5, 2)),
            pltpu.SemaphoreType.DMA((QUARTERS, 2)),
            pltpu.SemaphoreType.DMA((2, TOKENS // TILE)),
            rs.scratch(),
        ],
        compiler_params=pltpu.CompilerParams(collective_id=collective_id, has_side_effects=True, vmem_limit_bytes=VMEM_ALL),
        cost_estimate=pl.CostEstimate(flops=TOKENS * D * FF * 24, bytes_accessed=TOKENS * FF * 20, transcendentals=0),
        name="gradients",
    )(x, dy, wg, wu, wd)[0]


def solution(mesh):
    torus = Torus(4, 4, 8)
    count = float(LAYERS * 3 * D * FF)

    def step(x, dy, wg, wu, wd, mg, mu, md, vg, vu, vd):
        x, dy = x[0], dy[0]
        g = gradients(torus, x, dy, wg, wu, wd, 1)
        got = step_and_gather(torus, g, (wg, wu, wd), (mg, mu, md), (vg, vu, vd), count, 2)
        new = unpack(torus, got)
        return (*new[:3], *(jnp.transpose(t, (1, 0, 2)) for t in new[3:]))

    P = jax.sharding.PartitionSpec
    return jax.shard_map(
        step,
        mesh=mesh,
        in_specs=(P(("rep", "dp")),) * 2 + (P(),) * 3 + (P(None, "dp"),) * 6,
        out_specs=(P("rep"),) * 3 + (P("rep", "dp"),) * 6,
        check_vma=False,
    )
```

```python
import heapq
import jax
import jax.numpy as jnp
from jax import lax
from jax.experimental import pallas as pl
from jax.experimental.pallas import tpu as pltpu

F32, BF16 = jnp.float32, jnp.bfloat16
MESH = pl.DeviceIdType.MESH
RATE, LATENCY = 46.6e3, 2.3
TURN, ADD, HOP = 0.1, 2.0e6, 0.7
WAYS = (1, -1)
TRIO = range(3)
RING, CROSS, DIRECT = TRIO
NEVER, MARGIN, SWEEPS = 1e9, (0.3, 1.2), 3


class Torus:
    def __init__(self, nx, ny, nz):
        self.n = {"x": nx, "y": ny, "z": nz}
        self.size = nx * ny * nz

    def here(self):
        return Here(self)


class Here:
    def __init__(self, torus):
        p, n = lax.axis_index("dp"), torus.n
        ny, nz = n["y"], n["z"]
        mine = {"z": lax.rem(p, nz), "y": lax.rem(lax.div(p, nz), ny), "x": lax.div(p, ny * nz)}
        step = {"z": 1, "y": nz, "x": ny * nz}
        self.at = {d: [mine[d]] + [lax.rem(mine[d] + i, n[d]) for i in range(1, n[d])] for d in n}
        self.to = {d: [p + (self.at[d][i] - mine[d]) * step[d] for i in range(n[d])] for d in n}

    def peer(self, dim, delta):
        return {"dp": self.to[dim][delta % len(self.to[dim])]}

    def up(self, dim, delta):
        return self.at[dim][delta % len(self.at[dim])]


ORDERS = ("zxy", "xyz", "yxz")


def hops(n, flip):
    far, near = n // 2, n - 1 - n // 2
    return {1: near, -1: far} if flip else {1: far, -1: near}


class Balance:
    def __init__(self):
        self.load = {}

    def flip(self, dim, n, size):
        plain = [self.load.get((dim, s), 0) + size * hops(n, False)[s] for s in WAYS]
        turned = [self.load.get((dim, s), 0) + size * hops(n, True)[s] for s in WAYS]
        flip = max(turned) < max(plain)
        self.load[dim, 1], self.load[dim, -1] = turned if flip else plain
        return flip


def simulate(actions, copies):
    links, arrived, order = {}, {}, []
    waiting = {a: set(needs) for a, (needs, _, _, _) in actions.items()}
    by_need = {}
    for a, (needs, _, _, _) in actions.items():
        for c in needs:
            by_need.setdefault(c, []).append(a)
    ready = [(actions[a][3], i, a) for i, a in enumerate(actions) if not waiting[a]]
    rank = {a: i for i, a in enumerate(actions)}
    heapq.heapify(ready)
    now, done = 0.0, {}
    while ready:
        at, _, a = heapq.heappop(ready)
        now = max(now, at) + actions[a][2]
        order.append(a)
        done[a] = now
        for c in [("action", a)] + list(actions[a][1]):
            if c[0] == "action":
                end = now
            else:
                link, size, extra = copies[c]
                start = max(now, links.get(link, 0.0))
                links[link] = start + size / RATE
                end = links[link] + LATENCY + extra
            for b in by_need.get(c, ()):
                waiting[b].discard(c)
                arrived[b] = max(arrived.get(b, 0.0), end)
                if not waiting[b]:
                    heapq.heappush(ready, (max(arrived[b], actions[b][3]), rank[b], b))
    assert len(order) == len(actions), (len(order), len(actions))
    return order, now


def place(actions, copies, segments):
    links, known, left, slots, open_keys = {}, {}, dict(actions), {}, set()
    now = 0.0

    def do(a, where):
        nonlocal now
        _, sends, cost = left.pop(a)
        now += cost
        known["action", a] = now
        for c in sends:
            link, size, extra = copies[c]
            links[link] = max(now, links.get(link, 0.0)) + size / RATE
            known[c] = links[link] + LATENCY + extra
        where.append(a)

    def drain(where, allowed, wait):
        nonlocal now
        while True:
            able = [(max([known.get(c, NEVER) for c in actions[a][0]], default=0.0), i, a) for i, a in enumerate(left) if allowed(a)]
            best, _, a = min(able, default=(NEVER, 0, None))
            if best >= NEVER or not wait and best + MARGIN[a[0][0][0]] > now:
                return
            now = max(now, best)
            do(a, where)

    for key, cost, writes, whole in segments:
        now += cost
        slots[key] = ([], [])
        others = {(l, u, c) for (l, u), c in writes}
        drain(slots[key][0], lambda a: any(a[0][0][1] == u and a[0][1] == c and a[0][0][0] > l for l, u, c in others), True)
        open_keys |= set(whole)
        drain(slots[key][1], lambda a: a[1] != "start" or (a[0], a[2]) in open_keys, False)
    drain(slots[segments[-1][0]][1], lambda a: True, True)
    assert not left
    place.took = now
    return slots


def arrive(me, peers):
    sem = pltpu.get_barrier_semaphore()
    for dim, delta in peers:
        pl.semaphore_signal(sem, inc=1, device_id=me.peer(dim, delta), device_id_type=MESH)


def meet(peers):
    pl.semaphore_wait(pltpu.get_barrier_semaphore(), len(peers))


def both_ways(torus, dim):
    n = torus.n[dim]
    return [] if n == 1 else [(dim, 1)] if n == 2 else [(dim, 1), (dim, -1)]


def all_others(torus, dim):
    return [(dim, d) for d in range(1, torus.n[dim])]


class ReduceScatter:
    LANES = (2, 1, 1)

    def __init__(self, torus, rows, units):
        self.t, self.rows, self.units = torus, rows, units
        self.dims = [tuple(order) for order in ORDERS]
        self.nslots = max(self.base(c, DIRECT, 0) + self.sizes(c)[DIRECT] - 1 for c in TRIO)

    def sizes(self, c):
        return [self.t.n[d] for d in self.dims[c]]

    def here(self, c):
        return [self.me.up(d, 0) for d in self.dims[c]]

    def base(self, c, phase, lane):
        n = self.sizes(c)
        return sum((n[i] - 1) * self.LANES[i] for i in range(phase)) + lane * (n[phase] - 1)

    def peers(self):
        full = {dims[DIRECT] for dims in self.dims}
        out = []
        for dim in "xyz":
            out += all_others(self.t, dim) if dim in full else both_ways(self.t, dim)
        return out

    def credit_peers(self, c):
        a, b, d = self.dims[c]
        return both_ways(self.t, a) + both_ways(self.t, b) + all_others(self.t, d)

    def scratch(self):
        n = self.t.n
        t, r1, r2, r3, k2, k3 = [], [], [], [], [], []
        for dims in self.dims:
            n1, n2, n3 = (n[d] for d in dims)
            tail = (self.rows, 128)
            t.append(pltpu.VMEM((self.units, n1, n2 * n3) + tail, BF16))
            r1.append(pltpu.VMEM((self.units, max(n1 - 1, 1), n2 * n3) + tail, BF16))
            r2.append(pltpu.VMEM((self.units, max(n2 - 1, 1), n3) + tail, BF16))
            r3.append(pltpu.VMEM((self.units, max(n3 - 1, 1)) + tail, BF16))
            k2.append(pltpu.VMEM((self.units, n3) + tail, F32))
            k3.append(pltpu.VMEM((self.units,) + tail, F32))
        sems = [pltpu.SemaphoreType.DMA((self.units, 3, self.nslots)), pltpu.SemaphoreType.DMA((self.units, 3, self.nslots)), pltpu.SemaphoreType.REGULAR((self.units, 3))]
        return [t, r1, r2, r3, k2, k3] + sems

    def slot(self, c, phase, sign, h):
        return h if sign > 0 else self.sizes(c)[phase] - 2 - h

    def flips(self, balance, c):
        n1, n2, n3 = self.sizes(c)
        block, (a, b, d) = self.rows * 256, self.dims[c]
        for rel in range(1, n3):
            link = d, 1 if rel <= n3 // 2 else -1
            balance.load[link] = balance.load.get(link, 0) + block * min(rel, n3 - rel)
        ring = [balance.flip(a, n1, block * n2 * n3 // self.LANES[RING]) for _ in range(self.LANES[RING])]
        return ring, [balance.flip(b, n2, block * n3)]

    def plan(self, unit, c, flip):
        n = self.sizes(c)
        n1, n2, n3 = n
        block = self.rows * 256
        size = [block * n2 * n3 // self.LANES[RING], block * n3, block]
        actions, copies = {}, {}
        key = (unit, c)

        def send(phase, lane, sign, h):
            cid = ("copy", key, phase, lane, sign, h)
            copies[cid] = ((self.dims[c][phase], sign), size[phase], 0)
            return cid

        first, last = [[], []], [[], []]
        for phase in (RING, CROSS):
            for lane, turned in enumerate(flip[phase]):
                k = hops(n[phase], turned)
                ways = [s for s in WAYS if k[s]]
                first[phase] += [send(phase, lane, s, k[s] - 1) for s in ways]
                last[phase] += [("copy", key, phase, lane, s, 0) for s in ways]
                for s in ways:
                    for h in range(k[s] - 1, 0, -1):
                        actions[key, "step", phase, lane, s, h] = ([("copy", key, phase, lane, s, h)], [send(phase, lane, s, h - 1)], size[phase] / ADD)
        direct = []
        for rel in range(1, n3):
            cid = ("copy", key, DIRECT, 0, 0, rel)
            far = min(rel, n3 - rel)
            copies[cid] = ((self.dims[c][DIRECT], 1 if rel <= n3 // 2 else -1), size[DIRECT] * far, HOP * (far - 1))
            direct.append(cid)
        sends = first + [direct, []]
        for lane in range(self.LANES[RING]):
            actions[key, "start", lane] = ([], [x for x in sends[RING] if x[3] == lane], TURN)
        before = (key, "start", 0)
        for phase, needs in enumerate(last + [direct]):
            a = (key, "end", phase)
            actions[a] = (needs + [("action", before)], sends[phase + 1], size[phase] * self.LANES[phase] / ADD + TURN)
            before = a
        return actions, copies

    def bind(self, me, refs):
        self.me, (self.T, self.R1, self.R2, self.R3, self.K2, self.K3, self.ssem, self.rsem, self.credit) = me, refs
        return self

    def remote(self, u, c, phase, lane, sign, h):
        n1, n2, n3 = self.sizes(c)
        d1, d2, d3 = self.dims[c]
        up = self.me.up
        mine = self.T[c].at[u]
        slot = h - 1 if phase == DIRECT else self.slot(c, phase, sign, h)
        if phase == RING:
            part = n2 * n3 // self.LANES[RING]
            blocks = pl.ds(lane * part, part)
            src, dst = mine.at[up(d1, sign * (h + 1)), blocks], self.R1[c].at[u, slot, blocks]
        elif phase == CROSS:
            src, dst = mine.at[up(d1, 0), pl.ds(up(d2, sign * (h + 1)) * n3, n3)], self.R2[c].at[u, slot]
        else:
            sign = h
            src, dst = mine.at[up(d1, 0), up(d2, 0) * n3 + up(d3, h)], self.R3[c].at[u, slot]
        s = self.base(c, phase, lane) + slot
        to = self.me.peer(self.dims[c][phase], sign)
        return pltpu.make_async_remote_copy(src_ref=src, dst_ref=dst, send_sem=self.ssem.at[u, c, s], recv_sem=self.rsem.at[u, c, s], device_id=to, device_id_type=MESH)

    def all_sends(self, c, flip):
        n = self.sizes(c)
        out = []
        for phase in (RING, CROSS):
            for lane, turned in enumerate(flip[phase]):
                k = hops(n[phase], turned)
                out += [(phase, lane, s, h) for s in WAYS for h in range(k[s])]
        return out + [(DIRECT, 0, 0, rel) for rel in range(1, n[DIRECT])]

    def run(self, u, c, flip, what, store):
        n = self.sizes(c)
        n1, n2, n3 = n
        m1, m2, m3 = self.here(c)
        T, R1, R2, R3 = (r[c].at[u] for r in (self.T, self.R1, self.R2, self.R3))
        K2, K3 = self.K2[c].at[u], self.K3[c].at[u]
        mine = T.at[m1]
        wide = lambda v: v.astype(F32)
        go = lambda *a: self.remote(u, c, *a)

        def loop(count, body):
            def one(i, carry):
                body(i)
                return carry

            lax.fori_loop(0, count, one, 0)

        def line(q):
            return pl.ds(q * n3, n3)

        def ways(phase):
            for lane, turned in enumerate(flip[phase]):
                k = hops(n[phase], turned)
                for s in WAYS:
                    if k[s]:
                        yield lane, s, k[s]

        def sends(phase, only=None):
            for lane, s, k in ways(phase):
                if only in (None, lane):
                    go(phase, lane, s, k - 1).start()

        def arrived(phase):
            got = set()
            for lane, s, _ in ways(phase):
                go(phase, lane, s, 0).wait_recv()
                got.add(self.slot(c, phase, s, 0))
            return sorted(got)

        kind, *where = what
        if kind == "start":
            sends(RING, *where)
        elif kind == "step":
            phase, lane, s, h = where
            go(*where).wait_recv()
            slot = self.slot(c, phase, s, h)
            q = self.me.up(self.dims[c][phase], s * h)
            if phase == RING:
                lines = n2 // self.LANES[RING]

                def add(i):
                    b = line(lane * lines + i)
                    T[q, b] = (wide(T[q, b]) + wide(R1[slot, b])).astype(BF16)

                loop(lines, add)
            else:
                mine[line(q)] = (wide(mine[line(q)]) + wide(R2[slot])).astype(BF16)
            go(phase, lane, s, h - 1).start()
        elif where == [RING]:
            got = arrived(RING)

            def total(b):
                return sum((wide(R1[g, b]) for g in got), wide(mine[b]))

            def others(i):
                b = line(lax.rem(m2 + 1 + i, n2))
                mine[b] = total(b).astype(BF16)

            loop(n2 - 1, others)
            sends(CROSS)
            K2[...] = total(line(m2))
        elif where == [CROSS]:
            got = arrived(CROSS)
            total = sum((wide(R2[g]) for g in got), K2[...])
            K2[...] = total
            mine[line(m2)] = total.astype(BF16)
            for rel in range(1, n3):
                go(DIRECT, 0, 0, rel).start()
            K3[...] = K2[m3]
        else:
            for rel in range(1, n3):
                go(DIRECT, 0, 0, rel).wait_recv()
            store(sum((wide(R3[i]) for i in range(n3 - 1)), K3[...]).astype(BF16).astype(F32))

    def wait_sends(self, u, c, flip):
        for a in self.all_sends(c, flip):
            self.remote(u, c, *a).wait_send()

    def give_credit(self, u, c):
        for dim, delta in self.credit_peers(c):
            pl.semaphore_signal(self.credit.at[u, c], inc=1, device_id=self.me.peer(dim, delta), device_id_type=MESH)

    def take_credit(self, u, c):
        pl.semaphore_wait(self.credit.at[u, c], len(self.credit_peers(c)))


class AllGather:
    def __init__(self, torus, block_bytes, split=4):
        self.t, self.bytes, self.split = torus, block_bytes, split
        self.dims = [tuple(order) for order in ORDERS]
        self.flip, self.balance = {}, Balance()
        self.build()
        for key in list(self.flip) * SWEEPS:
            took = self.took
            self.flip[key] = not self.flip[key]
            self.build()
            if self.took >= took:
                self.flip[key] = not self.flip[key]
        self.build()

    def build(self):
        self.copies, self.actions, self.index = {}, {}, {}
        for c in TRIO:
            self.plan(c)
        self.order, self.took = simulate({a: (*v, 0) for a, v in self.actions.items()}, self.copies)

    def peers(self):
        return [p for dim in "xyz" for p in both_ways(self.t, dim)]

    def pieces(self, c, j):
        n3 = self.t.n[self.dims[c][DIRECT]]
        return n3 if not j else self.split if n3 % self.split == 0 else 1

    def size(self, c, phase, j):
        line = self.bytes * self.t.n[self.dims[c][DIRECT]]
        return self.bytes if phase == DIRECT else line // self.pieces(c, 1 if phase == CROSS else j)

    def k(self, c, phase, j, i):
        dim = self.dims[c][phase]
        key = (c, phase, j, i)
        if key not in self.flip:
            self.flip[key] = self.balance.flip(dim, self.t.n[dim], self.size(c, phase, j))
        return hops(self.t.n[dim], self.flip[key])

    def plan(self, c):
        n1, n2, n3 = (self.t.n[d] for d in self.dims[c])

        def send(where, s, h):
            phase, j, _ = where
            cid = (c, where, s, h)
            self.copies[cid] = ((self.dims[c][phase], s), self.size(c, phase, j), 0)
            self.index[cid] = len(self.index)
            return cid

        def own(*where):
            k = self.k(c, *where)
            return [send(where, s, 1) for s in WAYS if k[s]]

        def passing(*where):
            k = self.k(c, *where)
            for s in WAYS:
                for h in range(1, k[s] + 1):
                    yield s, h, (c, "pass", where, s, h), [(c, where, s, h)], [send(where, s, h + 1)] if h < k[s] else []

        def act(a, needs, sends):
            self.actions[a] = (needs, sends, TURN / 2)

        act((c, "start"), [], own(DIRECT, 0, 0) + own(RING, 0, 0))
        got = [("action", (c, "start"))]
        for s, h, a, needs, sends in passing(DIRECT, 0, 0):
            act(a, needs, sends + own(RING, 0, (-s * h) % n3))
            got.append(("action", a))
        parts = range(self.pieces(c, 1))
        act((c, "line"), got, [x for i in parts for x in own(CROSS, 0, i)])
        for i in parts:
            for s, h, a, needs, sends in passing(CROSS, 0, i):
                after = (-s * h) % n2, i
                if c:
                    act(a, needs, sends + own(RING, *after))
                else:
                    act(a, needs, sends)
                    act((c, "later", *after), [("action", x) for x in (a, (1, "line"), (2, "line"))], own(RING, *after))
        for j in range(n2):
            for i in range(self.pieces(c, j)):
                for _, _, a, needs, sends in passing(RING, j, i):
                    act(a, needs, sends)

    def bind(self, me, G, ssem, rsem):
        self.me, self.G, self.ssem, self.rsem = me, G, ssem, rsem
        return self

    def remote(self, cid, back):
        c, (phase, j, i), s, h = cid
        d1, d2, d3 = self.dims[c]
        n3, up = self.t.n[d3], self.me.up
        off = s * (back - h)
        G = self.G[c]
        if phase == DIRECT:
            ref = G.at[up(d1, 0), up(d2, 0) * n3 + up(d3, off)]
        elif phase == CROSS:
            size = n3 // self.pieces(c, 1)
            ref = G.at[up(d1, 0), pl.ds(up(d2, off) * n3 + i * size, size)]
        elif j == 0:
            ref = G.at[up(d1, off), up(d2, 0) * n3 + up(d3, i)]
        else:
            size = n3 // self.pieces(c, j)
            ref = G.at[up(d1, off), pl.ds(up(d2, j) * n3 + i * size, size)]
        x = self.index[cid]
        return pltpu.make_async_remote_copy(src_ref=ref, dst_ref=ref, send_sem=self.ssem.at[x], recv_sem=self.rsem.at[x], device_id=self.me.peer(self.dims[c][phase], s), device_id_type=MESH)

    def run(self, a):
        needs, sends, _ = self.actions[a]
        for cid in needs:
            if cid in self.index:
                self.remote(cid, 0).wait_recv()
        for cid in sends:
            self.remote(cid, 1).start()

    def wait_sends(self):
        for cid in self.copies:
            self.remote(cid, 1).wait_send()


MIB = 2**20
VMEM_ALL = 67043328
LAYERS, D, FF = 2, 896, 2560
LANES, ROWS, CHUNK = 128, 144, 48
USED = 140
HIGH = {0: 7, 1: 7, 2: 20}
WIDE = {0: FF, 1: FF, 2: D}
WINDOW = (16, 16, 24)


HALVES, RING_TILES = 2, 8
COLOURS = {0: (1, 2, 0), 1: (1, 2, 0), 2: (0, 1, 2)}
TOKENS, TILE, PART = 2048, 256, 512
LT, STEPS = TILE // LANES, FF // TILE
HALF = STEPS // HALVES


def home(u, ct):
    if u == HALVES:
        return u, ct
    t, k = divmod(ct, 2 * LT)
    m, j = divmod(k, LT)
    return m, (u * HALF + t) * LT + j


def tiles(u):
    high, wide = HIGH[u], WIDE[u] // LANES
    out = []
    for k in range(ROWS // 8):
        ct, row = divmod(8 * k, high)
        out.append((ct, row, min(8, high - row), ct + 1 < wide))
    return out


def pack(torus, u, X, base, parts, first, count, outs, colours):
    high, ny, nz = HIGH[u], torus.n["y"], torus.n["z"]
    sub = lax.broadcasted_iota(jnp.int32, (8, LANES), 0)
    got = tiles(u)

    def body(line, carry):
        x, y = lax.div(first + line, ny), lax.rem(first + line, ny)
        top = pl.multiple_of(line * (high * nz), 8)

        def piece(z, ct, row, whole, more):
            a = X[pl.ds(top + (base(ct) + high * z + row), 8), :]
            if whole == 8:
                return a
            b = X[pl.ds(top + (base(ct + 1) + high * z - whole), 8), :] if more else jnp.zeros((8, LANES), F32)
            return jnp.where(sub < whole, a, b)

        for z in range(nz):
            at = {"x": x, "y": y, "z": z}
            for j in parts:
                both = jnp.concatenate([piece(z, *got[2 * j]), piece(z, *got[2 * j + 1])], axis=0).astype(BF16)
                k, r = divmod(16 * j, CHUNK)
                c = colours[k]
                d1, d2, d3 = ORDERS[c]
                outs[c][at[d1], at[d2] * torus.n[d3] + at[d3], pl.ds(r, 16), :] = both
        return carry

    lax.fori_loop(0, count, body, 0)


def step_and_gather(torus, g, w, m, v, count, collective_id):
    ag = AllGather(torus, LAYERS * USED * 256)
    dims = "zxy"
    slots = {d: torus.n[d] - 1 for d in dims}

    def window(p, x):
        rows = WINDOW[x]
        first = lax.div(p * HIGH[x], 8) * 8
        return pl.multiple_of(jnp.minimum(first, HIGH[x] * torus.size - rows), 8), rows

    def kernel(g_ref, *refs):
        w_in, m_in, v_in, G, m_out, v_out = (refs[i : i + 3] for i in range(0, 18, 3))
        flat, wflat, part, E, esend, erecv, ssem, rsem, win, wide_win, wsem = refs[18:]
        me = torus.here()
        p = lax.axis_index("dp")
        loads = []
        for x in TRIO:
            first, rows = window(p, x)
            loads.append(pltpu.make_async_copy(w_in[x].at[:, pl.ds(first, rows)], win[x], wsem.at[x]))
            loads[x].start()
        peers = [p for d in "xyz" for p in all_others(torus, d)]
        arrive(me, peers)
        acc = jnp.zeros((8, LANES), F32)
        for l in range(LAYERS):
            for u in TRIO:
                for k, c in enumerate(COLOURS[u]):
                    value = g_ref[l, u, c]
                    flat[l, u, pl.ds(k * CHUNK, CHUNK), :] = value
                    for r in range(0, CHUNK, 8):
                        acc = acc + value[r : r + 8] * value[r : r + 8]
        part[0] = acc
        meet(peers)
        base = 0
        for i, d in enumerate(dims):
            n = torus.n[d]
            copies = []
            for rel in range(1, n):
                s = base + rel - 1
                copies.append(pltpu.make_async_remote_copy(src_ref=part.at[i], dst_ref=E.at[s], send_sem=esend.at[s], recv_sem=erecv.at[s], device_id=me.peer(d, rel), device_id_type=MESH))
            for copy in copies:
                copy.start()
            if i == 0:
                for x in TRIO:
                    loads[x].wait()
                    for lt in range(WIDE[x] // LANES):
                        wide_win[x][:, lt] = win[x][:, :, pl.ds(lt * LANES, LANES)].astype(F32)
            total = part[i]
            for rel in range(1, n):
                copies[rel - 1].wait_recv()
                total = total + E[base + rel - 1]
            part[i + 1] = total
            for copy in copies:
                copy.wait_send()
            base += n - 1
        mean = jnp.sum(part[3], keepdims=True) / count
        factor = jnp.minimum(1.0, 0.5 * lax.rsqrt(mean + 1e-30))
        for l in range(LAYERS):
            for u in TRIO:
                high = HIGH[u]
                for ct in range(WIDE[u] // LANES):
                    x, lt = home(u, ct)
                    at = (slice(None), l, pl.ds(lt * LANES, LANES))
                    grad = flat[l, u, pl.ds(ct * high, high), :] * factor
                    new_m = 0.9 * m_in[x][at] + 0.1 * grad
                    new_v = 0.95 * v_in[x][at] + 0.05 * grad * grad
                    wide = wide_win[x][l, lt, pl.ds(p * high - window(p, x)[0], high), :]
                    new_w = wide - 0.02 * (new_m * lax.rsqrt(new_v + 1e-8) + 0.1 * wide)
                    m_out[x][at] = new_m
                    v_out[x][at] = new_v
                    wflat[u, pl.ds(l * USED + ct * high, high), :] = new_w
        it = ag.bind(me, G, ssem, rsem)
        for u in TRIO:
            a, b, d = (me.up(x, 0) for x in ORDERS[u])
            G[u][a, b * torus.n[ORDERS[u][DIRECT]] + d] = wflat[u].astype(BF16)
        for a in ag.order:
            it.run(a)
        it.wait_sends()

    vmem = pl.BlockSpec(memory_space=pltpu.VMEM)
    nsum = sum(slots.values())
    shapes = [jax.ShapeDtypeStruct((torus.n[a], torus.n[b] * torus.n[d], LAYERS * USED, LANES), BF16) for a, b, d in ORDERS]
    turn = lambda ts: [jnp.transpose(t, (1, 0, 2)) for t in ts]
    m, v = turn(m), turn(v)
    f32 = [jax.ShapeDtypeStruct(t.shape, F32) for t in m]
    k = len(ag.copies)
    got = pl.pallas_call(
        kernel,
        out_shape=[pltpu.MemorySpace.VMEM(s.shape, s.dtype) for s in shapes + f32 * 2],
        in_specs=[vmem] + [pl.BlockSpec(memory_space=pl.ANY)] * 3 + [vmem] * 6,
        out_specs=[vmem] * 9,
        scratch_shapes=[
            pltpu.VMEM((LAYERS, 3, ROWS, LANES), F32),
            pltpu.VMEM((3, LAYERS * USED, LANES), F32),
            pltpu.VMEM((4, 8, LANES), F32),
            pltpu.VMEM((nsum, 8, LANES), F32),
            pltpu.SemaphoreType.DMA((nsum,)),
            pltpu.SemaphoreType.DMA((nsum,)),
            pltpu.SemaphoreType.DMA((k,)),
            pltpu.SemaphoreType.DMA((k,)),
            [pltpu.VMEM((LAYERS, WINDOW[x], WIDE[x]), BF16) for x in TRIO],
            [pltpu.VMEM((LAYERS, WIDE[x] // LANES, WINDOW[x], LANES), F32) for x in TRIO],
            pltpu.SemaphoreType.DMA((3,)),
        ],
        compiler_params=pltpu.CompilerParams(collective_id=collective_id, has_side_effects=True, vmem_limit_bytes=26 * MIB),
        name="step_and_gather",
    )(g, *w, *m, *v)
    return got


def unpack(torus, got):
    nx, ny, nz = (torus.n[d] for d in "xyz")
    pair = 2
    group = pair * nz
    groups = torus.size // group
    pairs = ny // pair
    skip = LAYERS * USED - ROWS

    def kernel(g0, g1, g2, *refs):
        moments, outs, kept, (Z, Y, sem) = refs[:6], refs[6:9], refs[9:15], refs[15:]
        l, s = pl.program_id(0), pl.program_id(1)
        copies = [pltpu.make_async_copy(src, dst, sem.at[i]) for i, (src, dst) in enumerate(zip(moments, kept))]

        @pl.when(l + s == 0)
        def _():
            for copy in copies:
                copy.start()

        @pl.when(l + s == LAYERS - 1 + groups - 1)
        def _():
            for copy in copies:
                copy.wait()

        corner = {"x": lax.div(s, pairs), "y": lax.rem(s, pairs) * pair, "z": 0}
        for u in TRIO:
            high, wide = HIGH[u], WIDE[u] // LANES
            for i in range(group):
                y, z = divmod(i, nz)
                at = corner | {"y": corner["y"] + y, "z": z}
                a, b, d = ORDERS[u]
                Z[i, pl.ds(0, ROWS), :] = (g0, g1, g2)[u][at[a], at[b] * torus.n[d] + at[d], pl.ds(l * skip, ROWS), :].astype(F32)
            for i in range(group):
                for ct in range(wide):
                    for r in range(0, high, 8):
                        Y[ct, pl.ds(high * i + r, 8), :] = Z[i, pl.ds(l * (USED - skip) + high * ct + r, 8), :]
            rows = high * group
            for ct in range(wide):
                x, lt = home(u, ct)
                outs[x][0, :, pl.ds(lt * LANES, LANES)] = Y[ct, pl.ds(0, rows), :].astype(BF16)

    shapes = [(LAYERS, HIGH[u] * torus.size, WIDE[u]) for u in TRIO]
    return pl.pallas_call(
        kernel,
        grid=(LAYERS, groups),
        out_shape=[jax.ShapeDtypeStruct(s, BF16) for s in shapes] + [jax.ShapeDtypeStruct(m.shape, F32) for m in got[3:]],
        in_specs=[pl.BlockSpec(memory_space=pltpu.VMEM)] * 9,
        out_specs=[pl.BlockSpec((1, HIGH[u] * group, WIDE[u]), lambda l, s: (l, s, 0)) for u in TRIO] + [pl.BlockSpec(memory_space=pl.ANY)] * 6,
        scratch_shapes=[
            pltpu.VMEM((group, ROWS + 8, LANES), F32),
            pltpu.VMEM((FF // LANES, HIGH[2] * group + 8, LANES), F32),
            pltpu.SemaphoreType.DMA((6,)),
        ],
        compiler_params=pltpu.CompilerParams(vmem_limit_bytes=26 * MIB),
        name="unpack",
    )(*got)


NN, NT = ((1,), (0,)), ((1,), (1,))


def dot(a, b, dims=NN):
    return lax.dot_general(a, b, (dims, ((), ())), preferred_element_type=F32)


def scale_of(wide):
    return lax.rsqrt(jnp.mean(wide * wide, -1, keepdims=True) + 1e-6)


GAP = 24
SIDE_STRIDE, DOWN_STRIDE = D + GAP, FF // HALVES + GAP
DOWN_BASE = RING_TILES * SIDE_STRIDE
X_ROWS = DOWN_BASE + D // LANES * DOWN_STRIDE
COST = {"last": (3.5, 3.5), "first": (1.8, 3.5), "da": (2.5,), "norm": (0.45,)}
PACK_DOWN = 0.4
WHOLE = ((0,), (1, 2), (3, 4), (5, 6), (7, 8))
CHUNKS = {1: 0, 3: 1, 4: 2}
PASSES = ("forward", "last", "da", "norm", "first")
COUNT = {"forward": STEPS, "last": STEPS, "da": STEPS, "norm": TOKENS // TILE, "first": STEPS}
QUARTERS = TOKENS // PART
MAKE = 1


def timeline():
    out, lanes = [], ReduceScatter.LANES[RING]
    for kind in PASSES[1:]:
        layer = {"last": 1, "first": 0}.get(kind)
        for t in range(COUNT[kind]):
            half, tt = divmod(t, HALF)
            for i, cost in enumerate(COST[kind]):
                writes, whole = [], []
                if i == MAKE:
                    unit = (layer, half)
                    if tt == 0:
                        writes += [(unit, c) for c in TRIO]
                    if tt in CHUNKS:
                        whole += [((unit, COLOURS[half][CHUNKS[tt]]), lane) for lane in range(lanes)]
                    if tt == HALF - 1:
                        cost += PACK_DOWN
                        mine = [((layer, HALVES), c) for c in TRIO]
                        writes += [] if half else mine
                        whole += [(key, lane) for key in mine for lane in range(lanes) if half or lane == 0 and ORDERS[key[1]][CROSS] == "x"]
                out.append(((kind, t, i), cost, writes, whole))
    return out


def hidden_back(gate, up, d):
    s = jax.nn.sigmoid(gate)
    act = gate * s
    return (act * up).astype(BF16), (d * up * (s + act * (1.0 - s))).astype(BF16), (d * act).astype(BF16)


def gradients(torus, x, dy, wg, wu, wd, collective_id):
    rs = ReduceScatter(torus, CHUNK, 3)
    actions, copies, balance, flips = {}, {}, Balance(), {}
    for l in range(LAYERS):
        for u in TRIO:
            for c in TRIO:
                flips[l, u, c] = rs.flips(balance, c)
                got, sent = rs.plan((l, u), c, flips[l, u, c])
                copies |= sent
                actions |= got
                if l:
                    key = ((l, u), c)
                    actions[key, "free"] = ([("action", (key, "end", DIRECT))], [], TURN)
    slots = place(actions, copies, timeline())
    lines = torus.n["x"] * torus.n["y"]

    def kernel(x_ref, dy_ref, wg_ref, wu_ref, wd_ref, out, both_ref, gate_ref, up_ref, h1_ref, at0_ref, dyv, av, at, X, Mb, Db, Wb, Vb, Hb, once, pair, hsem, rsem, rsc):
        me = torus.here()
        it = rs.bind(me, rsc)
        copy = pltpu.make_async_copy
        load_x = copy(x_ref, dyv, once.at[0])
        save_at0, load_at0 = copy(at, at0_ref, once.at[1]), copy(at0_ref, at, once.at[1])

        def part(i):
            return pl.ds(i * TILE if isinstance(i, int) else pl.multiple_of(i * TILE, TILE), TILE)

        def sides(layer, t, s):
            return [copy(ref.at[layer, :, part(t)], Wb.at[s, :, part(k)], pair.at[k, s]) for k, ref in enumerate((wg_ref, wu_ref))]

        def fetch(kind, t, s):
            both, rows = pair.at[2, s], pair.at[3, s]
            if kind == "forward":
                return sides(0, t, s) + [copy(wd_ref.at[0, part(t)], Vb.at[s], rows)]
            if kind == "last":
                return sides(1, t, s) + [copy(wd_ref.at[1, part(t)], Vb.at[s], rows)]
            if kind == "da":
                return sides(1, t, s) + [copy(both_ref.at[t], Db.at[s], both)]
            if kind == "norm":
                return [copy(h1_ref.at[part(t)], Vb.at[s], rows)]
            return [copy(wd_ref.at[0, part(t)], Vb.at[s], rows)]

        def save(t, s):
            return copy(Db.at[s], both_ref.at[t], pair.at[4, s])

        def hiddens(t, quarters, out=False):
            got = []
            for q in quarters:
                for k, ref in enumerate((gate_ref, up_ref)):
                    ends = ref.at[pl.ds(t * LT, LT), pl.ds(q * PART, PART)], Hb.at[q, k]
                    got.append(copy(*(ends[::-1] if out else ends), hsem.at[q, k]))
            return got

        def act(a):
            ((l, u), c), what = a[0], a[1:]
            if what[0] == "free":
                it.wait_sends(u, c, flips[l, u, c])
                it.give_credit(u, c)
                return
            if what == ("start", 0) and l == 0:
                it.take_credit(u, c)

            def store(value):
                out[l, u, c] = value

            it.run(u, c, flips[l, u, c], what, store)

        def point(kind, t, i, which):
            for k in range(COUNT[kind]):
                if slots[kind, k, i][which]:

                    @pl.when(t == k)
                    def _(k=k):
                        for a in slots[kind, k, i][which]:
                            act(a)

        def normed_into(r):
            wide = dyv[part(r), :].astype(F32)
            a = (wide * scale_of(wide)).astype(BF16)
            av[part(r), :] = a
            at[:, part(r)] = a.T

        def lanes_of(ct):
            return slice(ct * LANES, (ct + 1) * LANES)

        def forward(t, s):
            for first in range(0, QUARTERS, 2):
                quarters = range(first, first + 2)

                @pl.when(t > 0)
                def _():
                    for f in hiddens(t - 1, quarters, True):
                        f.wait()

                for q in quarters:
                    rows = pl.ds(q * PART, PART)
                    both = dot(av[rows, :], Wb[s])
                    gate, up = both[:, :TILE], both[:, TILE:]
                    for j in range(LT):
                        Hb[q, 0, j], Hb[q, 1, j] = gate[:, lanes_of(j)], up[:, lanes_of(j)]
                    got = dot((jax.nn.silu(gate) * up).astype(BF16), Vb[s])
                    for ct in range(D // LANES):
                        here = pl.ds(ct * TOKENS + q * PART, PART)
                        X[here, :] = jnp.where(t == 0, 0.0, X[here, :]) + got[:, lanes_of(ct)]
                for f in hiddens(t, quarters, True):
                    f.start()

        def turn():
            for f in hiddens(STEPS - 1, range(QUARTERS), True):
                f.wait()
            save_at0.wait()
            count = TOKENS // TILE

            def saves(r):
                return copy(dyv.at[part(r)], h1_ref.at[part(r)], rsem.at[0, r])

            def loads(r):
                return copy(dy_ref.at[part(r)], dyv.at[part(r)], rsem.at[1, r])

            @pl.loop(0, count)
            def _(r):
                total = jnp.concatenate([X[pl.ds(ct * TOKENS + r * TILE, TILE), :] for ct in range(D // LANES)], axis=1)
                dyv[part(r), :] = dyv[part(r), :] + total.astype(BF16)
                normed_into(r)
                saves(r).start()

                @pl.when(r > 0)
                def _():
                    saves(r - 1).wait()
                    loads(r - 1).start()

            saves(count - 1).wait()
            loads(count - 1).start()
            for r in range(count):
                loads(r).wait()

        def hidden(kind, t, s):
            for first in range(0, QUARTERS, 2):
                quarters = range(first, first + 2)
                if kind == "first":
                    for f in hiddens(t, quarters):
                        f.wait()
                for q in quarters:
                    rows = pl.ds(q * PART, PART)
                    if kind == "last":
                        both = dot(av[rows, :], Wb[s])
                        gate, up = both[:, :TILE], both[:, TILE:]
                    else:
                        gate, up = (jnp.concatenate([Hb[q, k, j] for j in range(LT)], axis=1) for k in range(2))
                    d = dot(dyv[rows, :], Vb[s], NT).astype(BF16).astype(F32)
                    mid, Db[s, rows, part(0)], Db[s, rows, part(1)] = hidden_back(gate, up, d)
                    Mb[:, rows] = mid.T
                if kind == "first":

                    @pl.when(t + 1 < STEPS)
                    def _():
                        for f in hiddens(t + 1, quarters):
                            f.start()

        def make(kind, t, s):
            half, tt = lax.div(t, HALF), lax.rem(t, HALF)
            got = dot(at[...], Db[s])
            for k in range(2 * LT):
                X[pl.ds((lax.rem(tt, 2) * 2 * LT + k) * SIDE_STRIDE + 8, D), :] = got[:, lanes_of(k)]
            got = dot(Mb[...], dyv[...])
            for ct in range(D // LANES):
                X[pl.ds(DOWN_BASE + ct * DOWN_STRIDE + 8 + tt * TILE, TILE), :] = got[:, lanes_of(ct)]
            point(kind, t, MAKE, 0)
            for v, parts in enumerate(WHOLE):

                @pl.when(tt == v)
                def _(parts=parts):
                    pack(torus, 0, X, lambda ct: ct % RING_TILES * SIDE_STRIDE + 8, parts, 0, lines, [T.at[half] for T in it.T], COLOURS[0])

            @pl.when(tt == HALF - 1)
            def _():
                some = lines // HALVES
                pack(torus, HALVES, X, lambda ct: DOWN_BASE + ct * DOWN_STRIDE + 8, range(ROWS // 16), half * some, some, [T.at[HALVES] for T in it.T], COLOURS[HALVES])

        def d_a(t, s):
            for r in range(0, TOKENS, PART):
                got = dot(Db[s, pl.ds(r, PART), :], Wb[s], NT)
                for ct in range(D // LANES):
                    rows = pl.ds(ct * TOKENS + r, PART)
                    X[rows, :] = jnp.where(t == 0, 0.0, X[rows, :]) + got[:, lanes_of(ct)]

        def norm(t, s):
            da = jnp.concatenate([X[pl.ds(ct * TOKENS + t * TILE, TILE), :] for ct in range(D // LANES)], axis=1).astype(BF16).astype(F32)
            wide = Vb[s].astype(F32)
            scale = scale_of(wide)
            inner = jnp.mean(da * wide, -1, keepdims=True)
            dyv[part(t), :] = dyv[part(t), :] + (scale * da - wide * (scale * scale * scale * inner)).astype(BF16)

        for f in fetch("forward", 0, 0) + [load_x]:
            f.start()
        arrive(me, rs.peers())
        load_x.wait()

        @pl.loop(0, TOKENS // TILE)
        def _(r):
            normed_into(r)

        save_at0.start()
        for number, kind in enumerate(PASSES):
            count = COUNT[kind]
            following = PASSES[number + 1] if number + 1 < len(PASSES) else None
            if kind == "last":
                turn()
                meet(rs.peers())
            if kind == "da":
                load_at0.start()
            if kind == "norm":
                for f in hiddens(0, range(QUARTERS)):
                    f.start()
            if kind == "first":
                load_at0.wait()

            def body(t, carry, kind=kind, count=count, following=following):
                s = lax.rem(t, 2)
                for f in fetch(kind, t, s):
                    f.wait()

                @pl.when(t + 1 < count)
                def _():
                    for f in fetch(kind, t + 1, 1 - s):
                        f.start()

                if kind == "last":

                    @pl.when(t > 1)
                    def _():
                        save(t - 2, s).wait()

                if following:

                    @pl.when(t == count - 1)
                    def _():
                        if kind == "last":
                            save(t - 1, 1 - s).wait()
                        for f in fetch(following, 0, 0):
                            f.start()

                if kind in ("last", "first"):
                    hidden(kind, t, s)
                    if kind == "last":
                        save(t, s).start()
                    point(kind, t, 0, 1)
                    make(kind, t, s)
                    point(kind, t, MAKE, 1)
                else:
                    {"forward": forward, "da": d_a, "norm": norm}[kind](t, s)
                    if kind != "forward":
                        point(kind, t, 0, 1)
                return carry

            lax.fori_loop(0, count, body, 0)
            if kind == "last":
                save(count - 1, (count - 1) % 2).wait()
        for u in TRIO:
            for c in TRIO:
                it.wait_sends(u, c, flips[0, u, c])

    any_space = pl.BlockSpec(memory_space=pl.ANY)
    return pl.pallas_call(
        kernel,
        out_shape=[jax.ShapeDtypeStruct((LAYERS, 3, 3, CHUNK, LANES), F32), jax.ShapeDtypeStruct((STEPS, TOKENS, 2 * TILE), BF16)]
        + [jax.ShapeDtypeStruct((FF // LANES, TOKENS, LANES), F32)] * 2
        + [jax.ShapeDtypeStruct((TOKENS, D), BF16), jax.ShapeDtypeStruct((D, TOKENS), BF16)],
        in_specs=[any_space] * 5,
        out_specs=[pl.BlockSpec(memory_space=pltpu.VMEM)] + [any_space] * 5,
        scratch_shapes=[
            pltpu.VMEM((TOKENS, D), BF16),
            pltpu.VMEM((TOKENS, D), BF16),
            pltpu.VMEM((D, TOKENS), BF16),
            pltpu.VMEM((X_ROWS, LANES), F32),
            pltpu.VMEM((TILE, TOKENS), BF16),
            pltpu.VMEM((2, TOKENS, 2 * TILE), BF16),
            pltpu.VMEM((2, D, 2 * TILE), BF16),
            pltpu.VMEM((2, TILE, D), BF16),
            pltpu.VMEM((QUARTERS, 2, LT, PART, LANES), F32),
            pltpu.SemaphoreType.DMA((2,)),
            pltpu.SemaphoreType.DMA((5, 2)),
            pltpu.SemaphoreType.DMA((QUARTERS, 2)),
            pltpu.SemaphoreType.DMA((2, TOKENS // TILE)),
            rs.scratch(),
        ],
        compiler_params=pltpu.CompilerParams(collective_id=collective_id, has_side_effects=True, vmem_limit_bytes=VMEM_ALL),
        cost_estimate=pl.CostEstimate(flops=TOKENS * D * FF * 24, bytes_accessed=TOKENS * FF * 20, transcendentals=0),
        name="gradients",
    )(x, dy, wg, wu, wd)[0]


def solution(mesh):
    torus = Torus(4, 4, 8)
    count = float(LAYERS * 3 * D * FF)

    def step(x, dy, wg, wu, wd, mg, mu, md, vg, vu, vd):
        x, dy = x[0], dy[0]
        g = gradients(torus, x, dy, wg, wu, wd, 1)
        got = step_and_gather(torus, g, (wg, wu, wd), (mg, mu, md), (vg, vu, vd), count, 2)
        new = unpack(torus, got)
        return (*new[:3], *(jnp.transpose(t, (1, 0, 2)) for t in new[3:]))

    P = jax.sharding.PartitionSpec
    return jax.shard_map(
        step,
        mesh=mesh,
        in_specs=(P(("rep", "dp")),) * 2 + (P(),) * 3 + (P(None, "dp"),) * 6,
        out_specs=(P("rep"),) * 3 + (P("rep", "dp"),) * 6,
        check_vma=False,
    )
```

```python
import heapq
import jax
import jax.numpy as jnp
from jax import lax
from jax.experimental import pallas as pl
from jax.experimental.pallas import tpu as pltpu

F32, BF16 = jnp.float32, jnp.bfloat16
MESH = pl.DeviceIdType.MESH
RATE, LATENCY = 46.6e3, 2.3
TURN, ADD, HOP = 0.1, 2.0e6, 0.7
WAYS = (1, -1)
TRIO = range(3)
RING, CROSS, DIRECT = TRIO
NEVER, MARGIN, SWEEPS = 1e9, (0.3, 1.2), 3


class Torus:
    def __init__(self, nx, ny, nz):
        self.n = {"x": nx, "y": ny, "z": nz}
        self.size = nx * ny * nz

    def here(self):
        return Here(self)


class Here:
    def __init__(self, torus):
        p, n = lax.axis_index("dp"), torus.n
        ny, nz = n["y"], n["z"]
        mine = {"z": lax.rem(p, nz), "y": lax.rem(lax.div(p, nz), ny), "x": lax.div(p, ny * nz)}
        step = {"z": 1, "y": nz, "x": ny * nz}
        self.at = {d: [mine[d]] + [lax.rem(mine[d] + i, n[d]) for i in range(1, n[d])] for d in n}
        self.to = {d: [p + (self.at[d][i] - mine[d]) * step[d] for i in range(n[d])] for d in n}

    def peer(self, dim, delta):
        if dim == "xy":
            dx, dy = delta
            return {"dp": self.to["x"][dx] + self.to["y"][dy] - self.to["x"][0]}
        return {"dp": self.to[dim][delta % len(self.to[dim])]}

    def up(self, dim, delta):
        return self.at[dim][delta % len(self.at[dim])]


ORDERS = ("zxy", "xyz", "yxz")


def hops(n, flip):
    far, near = n // 2, n - 1 - n // 2
    return {1: near, -1: far} if flip else {1: far, -1: near}


class Balance:
    def __init__(self):
        self.load = {}

    def flip(self, dim, n, size):
        plain = [self.load.get((dim, s), 0) + size * hops(n, False)[s] for s in WAYS]
        turned = [self.load.get((dim, s), 0) + size * hops(n, True)[s] for s in WAYS]
        flip = max(turned) < max(plain)
        self.load[dim, 1], self.load[dim, -1] = turned if flip else plain
        return flip


def simulate(actions, copies):
    links, arrived, order = {}, {}, []
    waiting = {a: set(needs) for a, (needs, _, _, _) in actions.items()}
    by_need = {}
    for a, (needs, _, _, _) in actions.items():
        for c in needs:
            by_need.setdefault(c, []).append(a)
    ready = [(actions[a][3], i, a) for i, a in enumerate(actions) if not waiting[a]]
    rank = {a: i for i, a in enumerate(actions)}
    heapq.heapify(ready)
    now, done = 0.0, {}
    while ready:
        at, _, a = heapq.heappop(ready)
        now = max(now, at) + actions[a][2]
        order.append(a)
        done[a] = now
        for c in [("action", a)] + list(actions[a][1]):
            if c[0] == "action":
                end = now
            else:
                link, size, extra = copies[c]
                start = max(now, links.get(link, 0.0))
                links[link] = start + size / RATE
                end = links[link] + LATENCY + extra
            for b in by_need.get(c, ()):
                waiting[b].discard(c)
                arrived[b] = max(arrived.get(b, 0.0), end)
                if not waiting[b]:
                    heapq.heappush(ready, (max(arrived[b], actions[b][3]), rank[b], b))
    assert len(order) == len(actions), (len(order), len(actions))
    return order, now


def place(actions, copies, segments):
    links, known, left, slots, open_keys = {}, {}, dict(actions), {}, set()
    now = 0.0

    def do(a, where):
        nonlocal now
        _, sends, cost = left.pop(a)
        now += cost
        known["action", a] = now
        for c in sends:
            link, size, extra = copies[c]
            links[link] = max(now, links.get(link, 0.0)) + size / RATE
            known[c] = links[link] + LATENCY + extra
        where.append(a)

    def drain(where, allowed, wait):
        nonlocal now
        while True:
            able = [(max([known.get(c, NEVER) for c in actions[a][0]], default=0.0), i, a) for i, a in enumerate(left) if allowed(a)]
            best, _, a = min(able, default=(NEVER, 0, None))
            if best >= NEVER or not wait and best + MARGIN[a[0][0][0]] > now:
                return
            now = max(now, best)
            do(a, where)

    for key, cost, writes, whole in segments:
        now += cost
        slots[key] = ([], [])
        others = {(l, u, c) for (l, u), c in writes}
        drain(slots[key][0], lambda a: any(a[0][0][1] == u and a[0][1] == c and a[0][0][0] > l for l, u, c in others), True)
        open_keys |= set(whole)
        drain(slots[key][1], lambda a: a[1] != "start" or (a[0], a[2]) in open_keys, False)
    drain(slots[segments[-1][0]][1], lambda a: True, True)
    assert not left
    place.took = now
    return slots


def arrive(me, peers):
    sem = pltpu.get_barrier_semaphore()
    for dim, delta in peers:
        pl.semaphore_signal(sem, inc=1, device_id=me.peer(dim, delta), device_id_type=MESH)


def meet(peers):
    pl.semaphore_wait(pltpu.get_barrier_semaphore(), len(peers))


def both_ways(torus, dim):
    n = torus.n[dim]
    return [] if n == 1 else [(dim, 1)] if n == 2 else [(dim, 1), (dim, -1)]


def all_others(torus, dim):
    return [(dim, d) for d in range(1, torus.n[dim])]


class ReduceScatter:
    LANES = (2, 1, 1)

    def __init__(self, torus, rows, units):
        self.t, self.rows, self.units = torus, rows, units
        self.dims = [tuple(order) for order in ORDERS]
        self.nslots = max(self.base(c, DIRECT, 0) + self.sizes(c)[DIRECT] - 1 for c in TRIO)

    def sizes(self, c):
        return [self.t.n[d] for d in self.dims[c]]

    def here(self, c):
        return [self.me.up(d, 0) for d in self.dims[c]]

    def base(self, c, phase, lane):
        n = self.sizes(c)
        return sum((n[i] - 1) * self.LANES[i] for i in range(phase)) + lane * (n[phase] - 1)

    def peers(self):
        full = {dims[DIRECT] for dims in self.dims}
        out = []
        for dim in "xyz":
            out += all_others(self.t, dim) if dim in full else both_ways(self.t, dim)
        return out

    def credit_peers(self, c):
        a, b, d = self.dims[c]
        return both_ways(self.t, a) + both_ways(self.t, b) + all_others(self.t, d)

    def scratch(self):
        n = self.t.n
        t, r1, r2, r3, k2, k3 = [], [], [], [], [], []
        for dims in self.dims:
            n1, n2, n3 = (n[d] for d in dims)
            tail = (self.rows, 128)
            t.append(pltpu.VMEM((self.units, n1, n2 * n3) + tail, BF16))
            r1.append(pltpu.VMEM((self.units, max(n1 - 1, 1), n2 * n3) + tail, BF16))
            r2.append(pltpu.VMEM((self.units, max(n2 - 1, 1), n3) + tail, BF16))
            r3.append(pltpu.VMEM((self.units, max(n3 - 1, 1)) + tail, BF16))
            k2.append(pltpu.VMEM((self.units, n3) + tail, F32))
            k3.append(pltpu.VMEM((self.units,) + tail, F32))
        sems = [pltpu.SemaphoreType.DMA((self.units, 3, self.nslots)), pltpu.SemaphoreType.DMA((self.units, 3, self.nslots)), pltpu.SemaphoreType.REGULAR((self.units, 3))]
        return [t, r1, r2, r3, k2, k3] + sems

    def slot(self, c, phase, sign, h):
        return h if sign > 0 else self.sizes(c)[phase] - 2 - h

    def flips(self, balance, c):
        n1, n2, n3 = self.sizes(c)
        block, (a, b, d) = self.rows * 256, self.dims[c]
        for rel in range(1, n3):
            link = d, 1 if rel <= n3 // 2 else -1
            balance.load[link] = balance.load.get(link, 0) + block * min(rel, n3 - rel)
        ring = [balance.flip(a, n1, block * n2 * n3 // self.LANES[RING]) for _ in range(self.LANES[RING])]
        return ring, [balance.flip(b, n2, block * n3)]

    def plan(self, unit, c, flip):
        n = self.sizes(c)
        n1, n2, n3 = n
        block = self.rows * 256
        size = [block * n2 * n3 // self.LANES[RING], block * n3, block]
        actions, copies = {}, {}
        key = (unit, c)

        def send(phase, lane, sign, h):
            cid = ("copy", key, phase, lane, sign, h)
            copies[cid] = ((self.dims[c][phase], sign), size[phase], 0)
            return cid

        first, last = [[], []], [[], []]
        for phase in (RING, CROSS):
            for lane, turned in enumerate(flip[phase]):
                k = hops(n[phase], turned)
                ways = [s for s in WAYS if k[s]]
                first[phase] += [send(phase, lane, s, k[s] - 1) for s in ways]
                last[phase] += [("copy", key, phase, lane, s, 0) for s in ways]
                for s in ways:
                    for h in range(k[s] - 1, 0, -1):
                        actions[key, "step", phase, lane, s, h] = ([("copy", key, phase, lane, s, h)], [send(phase, lane, s, h - 1)], size[phase] / ADD)
        direct = []
        for rel in range(1, n3):
            cid = ("copy", key, DIRECT, 0, 0, rel)
            far = min(rel, n3 - rel)
            copies[cid] = ((self.dims[c][DIRECT], 1 if rel <= n3 // 2 else -1), size[DIRECT] * far, HOP * (far - 1))
            direct.append(cid)
        sends = first + [direct, []]
        for lane in range(self.LANES[RING]):
            actions[key, "start", lane] = ([], [x for x in sends[RING] if x[3] == lane], TURN)
        before = (key, "start", 0)
        for phase, needs in enumerate(last + [direct]):
            a = (key, "end", phase)
            actions[a] = (needs + [("action", before)], sends[phase + 1], size[phase] * self.LANES[phase] / ADD + TURN)
            before = a
        return actions, copies

    def bind(self, me, refs):
        self.me, (self.T, self.R1, self.R2, self.R3, self.K2, self.K3, self.ssem, self.rsem, self.credit) = me, refs
        return self

    def remote(self, u, c, phase, lane, sign, h):
        n1, n2, n3 = self.sizes(c)
        d1, d2, d3 = self.dims[c]
        up = self.me.up
        mine = self.T[c].at[u]
        slot = h - 1 if phase == DIRECT else self.slot(c, phase, sign, h)
        if phase == RING:
            part = n2 * n3 // self.LANES[RING]
            blocks = pl.ds(lane * part, part)
            src, dst = mine.at[up(d1, sign * (h + 1)), blocks], self.R1[c].at[u, slot, blocks]
        elif phase == CROSS:
            src, dst = mine.at[up(d1, 0), pl.ds(up(d2, sign * (h + 1)) * n3, n3)], self.R2[c].at[u, slot]
        else:
            sign = h
            src, dst = mine.at[up(d1, 0), up(d2, 0) * n3 + up(d3, h)], self.R3[c].at[u, slot]
        s = self.base(c, phase, lane) + slot
        to = self.me.peer(self.dims[c][phase], sign)
        return pltpu.make_async_remote_copy(src_ref=src, dst_ref=dst, send_sem=self.ssem.at[u, c, s], recv_sem=self.rsem.at[u, c, s], device_id=to, device_id_type=MESH)

    def all_sends(self, c, flip):
        n = self.sizes(c)
        out = []
        for phase in (RING, CROSS):
            for lane, turned in enumerate(flip[phase]):
                k = hops(n[phase], turned)
                out += [(phase, lane, s, h) for s in WAYS for h in range(k[s])]
        return out + [(DIRECT, 0, 0, rel) for rel in range(1, n[DIRECT])]

    def run(self, u, c, flip, what, store):
        n = self.sizes(c)
        n1, n2, n3 = n
        m1, m2, m3 = self.here(c)
        T, R1, R2, R3 = (r[c].at[u] for r in (self.T, self.R1, self.R2, self.R3))
        K2, K3 = self.K2[c].at[u], self.K3[c].at[u]
        mine = T.at[m1]
        wide = lambda v: v.astype(F32)
        go = lambda *a: self.remote(u, c, *a)

        def loop(count, body):
            def one(i, carry):
                body(i)
                return carry

            lax.fori_loop(0, count, one, 0)

        def line(q):
            return pl.ds(q * n3, n3)

        def ways(phase):
            for lane, turned in enumerate(flip[phase]):
                k = hops(n[phase], turned)
                for s in WAYS:
                    if k[s]:
                        yield lane, s, k[s]

        def sends(phase, only=None):
            for lane, s, k in ways(phase):
                if only in (None, lane):
                    go(phase, lane, s, k - 1).start()

        def arrived(phase):
            got = set()
            for lane, s, _ in ways(phase):
                go(phase, lane, s, 0).wait_recv()
                got.add(self.slot(c, phase, s, 0))
            return sorted(got)

        kind, *where = what
        if kind == "start":
            sends(RING, *where)
        elif kind == "step":
            phase, lane, s, h = where
            go(*where).wait_recv()
            slot = self.slot(c, phase, s, h)
            q = self.me.up(self.dims[c][phase], s * h)
            if phase == RING:
                lines = n2 // self.LANES[RING]

                def add(i):
                    b = line(lane * lines + i)
                    T[q, b] = (wide(T[q, b]) + wide(R1[slot, b])).astype(BF16)

                loop(lines, add)
            else:
                mine[line(q)] = (wide(mine[line(q)]) + wide(R2[slot])).astype(BF16)
            go(phase, lane, s, h - 1).start()
        elif where == [RING]:
            got = arrived(RING)

            def total(b):
                return sum((wide(R1[g, b]) for g in got), wide(mine[b]))

            def others(i):
                b = line(lax.rem(m2 + 1 + i, n2))
                mine[b] = total(b).astype(BF16)

            loop(n2 - 1, others)
            sends(CROSS)
            K2[...] = total(line(m2))
        elif where == [CROSS]:
            got = arrived(CROSS)
            total = sum((wide(R2[g]) for g in got), K2[...])
            K2[...] = total
            mine[line(m2)] = total.astype(BF16)
            for rel in range(1, n3):
                go(DIRECT, 0, 0, rel).start()
            K3[...] = K2[m3]
        else:
            for rel in range(1, n3):
                go(DIRECT, 0, 0, rel).wait_recv()
            store(sum((wide(R3[i]) for i in range(n3 - 1)), K3[...]).astype(BF16).astype(F32))

    def wait_sends(self, u, c, flip):
        for a in self.all_sends(c, flip):
            self.remote(u, c, *a).wait_send()

    def give_credit(self, u, c):
        for dim, delta in self.credit_peers(c):
            pl.semaphore_signal(self.credit.at[u, c], inc=1, device_id=self.me.peer(dim, delta), device_id_type=MESH)

    def take_credit(self, u, c):
        pl.semaphore_wait(self.credit.at[u, c], len(self.credit_peers(c)))


class AllGather:
    def __init__(self, torus, block_bytes, split=4):
        self.t, self.bytes, self.split = torus, block_bytes, split
        self.dims = [tuple(order) for order in ORDERS]
        self.flip, self.balance = {}, Balance()
        self.build()
        for key in list(self.flip) * SWEEPS:
            took = self.took
            self.flip[key] = not self.flip[key]
            self.build()
            if self.took >= took:
                self.flip[key] = not self.flip[key]
        self.build()

    def build(self):
        self.copies, self.actions, self.index = {}, {}, {}
        for c in TRIO:
            self.plan(c)
        self.order, self.took = simulate({a: (*v, 0) for a, v in self.actions.items()}, self.copies)

    def peers(self):
        return [p for dim in "xyz" for p in both_ways(self.t, dim)]

    def pieces(self, c, j):
        n3 = self.t.n[self.dims[c][DIRECT]]
        return n3 if not j else self.split if n3 % self.split == 0 else 1

    def size(self, c, phase, j):
        line = self.bytes * self.t.n[self.dims[c][DIRECT]]
        return self.bytes if phase == DIRECT else line // self.pieces(c, 1 if phase == CROSS else j)

    def k(self, c, phase, j, i):
        dim = self.dims[c][phase]
        key = (c, phase, j, i)
        if key not in self.flip:
            self.flip[key] = self.balance.flip(dim, self.t.n[dim], self.size(c, phase, j))
        return hops(self.t.n[dim], self.flip[key])

    def plan(self, c):
        n1, n2, n3 = (self.t.n[d] for d in self.dims[c])

        def send(where, s, h):
            phase, j, _ = where
            cid = (c, where, s, h)
            self.copies[cid] = ((self.dims[c][phase], s), self.size(c, phase, j), 0)
            self.index[cid] = len(self.index)
            return cid

        def own(*where):
            k = self.k(c, *where)
            return [send(where, s, 1) for s in WAYS if k[s]]

        def passing(*where):
            k = self.k(c, *where)
            for s in WAYS:
                for h in range(1, k[s] + 1):
                    yield s, h, (c, "pass", where, s, h), [(c, where, s, h)], [send(where, s, h + 1)] if h < k[s] else []

        def act(a, needs, sends):
            self.actions[a] = (needs, sends, TURN / 2)

        act((c, "start"), [], own(DIRECT, 0, 0) + own(RING, 0, 0))
        got = [("action", (c, "start"))]
        for s, h, a, needs, sends in passing(DIRECT, 0, 0):
            act(a, needs, sends + own(RING, 0, (-s * h) % n3))
            got.append(("action", a))
        parts = range(self.pieces(c, 1))
        act((c, "line"), got, [x for i in parts for x in own(CROSS, 0, i)])
        for i in parts:
            for s, h, a, needs, sends in passing(CROSS, 0, i):
                after = (-s * h) % n2, i
                if c:
                    act(a, needs, sends + own(RING, *after))
                else:
                    act(a, needs, sends)
                    act((c, "later", *after), [("action", x) for x in (a, (1, "line"), (2, "line"))], own(RING, *after))
        for j in range(n2):
            for i in range(self.pieces(c, j)):
                for _, _, a, needs, sends in passing(RING, j, i):
                    act(a, needs, sends)

    def bind(self, me, G, ssem, rsem):
        self.me, self.G, self.ssem, self.rsem = me, G, ssem, rsem
        return self

    def remote(self, cid, back):
        c, (phase, j, i), s, h = cid
        d1, d2, d3 = self.dims[c]
        n3, up = self.t.n[d3], self.me.up
        off = s * (back - h)
        G = self.G[c]
        if phase == DIRECT:
            ref = G.at[up(d1, 0), up(d2, 0) * n3 + up(d3, off)]
        elif phase == CROSS:
            size = n3 // self.pieces(c, 1)
            ref = G.at[up(d1, 0), pl.ds(up(d2, off) * n3 + i * size, size)]
        elif j == 0:
            ref = G.at[up(d1, off), up(d2, 0) * n3 + up(d3, i)]
        else:
            size = n3 // self.pieces(c, j)
            ref = G.at[up(d1, off), pl.ds(up(d2, j) * n3 + i * size, size)]
        x = self.index[cid]
        return pltpu.make_async_remote_copy(src_ref=ref, dst_ref=ref, send_sem=self.ssem.at[x], recv_sem=self.rsem.at[x], device_id=self.me.peer(self.dims[c][phase], s), device_id_type=MESH)

    def run(self, a):
        needs, sends, _ = self.actions[a]
        for cid in needs:
            if cid in self.index:
                self.remote(cid, 0).wait_recv()
        for cid in sends:
            self.remote(cid, 1).start()

    def wait_sends(self):
        for cid in self.copies:
            self.remote(cid, 1).wait_send()


MIB = 2**20
VMEM_ALL = 67043328
LAYERS, D, FF = 2, 896, 2560
LANES, SUB, ROWS, CHUNK = 128, 8, 144, 48
HIGH = {0: 7, 1: 7, 2: 20}
WIDE = {0: FF, 1: FF, 2: D}
WINDOW = (16, 16, 24)


HALVES, RING_TILES = 2, 8
COLOURS = {0: (1, 2, 0), 1: (1, 2, 0), 2: (0, 1, 2)}
TOKENS, TILE, PART = 2048, 256, 512
LT, STEPS = TILE // LANES, FF // TILE
HALF = STEPS // HALVES


def home(u, ct):
    if u == HALVES:
        return u, ct
    t, k = divmod(ct, 2 * LT)
    m, j = divmod(k, LT)
    return m, (u * HALF + t) * LT + j


def tiles(u):
    high, wide = HIGH[u], WIDE[u] // LANES
    out = []
    for k in range(ROWS // SUB):
        ct, row = divmod(SUB * k, high)
        out.append((ct, row, min(SUB, high - row), ct + 1 < wide))
    return out


def pack(torus, u, X, base, parts, first, count, outs, colours):
    high, ny, nz = HIGH[u], torus.n["y"], torus.n["z"]
    sub = lax.broadcasted_iota(jnp.int32, (SUB, LANES), 0)
    got = tiles(u)

    def body(line, carry):
        x, y = lax.div(first + line, ny), lax.rem(first + line, ny)
        top = pl.multiple_of(line * (high * nz), SUB)

        def piece(z, ct, row, whole, more):
            a = X[pl.ds(top + (base(ct) + high * z + row), SUB), :]
            if whole == SUB:
                return a
            b = X[pl.ds(top + (base(ct + 1) + high * z - whole), SUB), :] if more else jnp.zeros((SUB, LANES), F32)
            return jnp.where(sub < whole, a, b)

        for z in range(nz):
            at = {"x": x, "y": y, "z": z}
            for j in parts:
                both = jnp.concatenate([piece(z, *got[2 * j]), piece(z, *got[2 * j + 1])], axis=0).astype(BF16)
                k, r = divmod(16 * j, CHUNK)
                c = colours[k]
                d1, d2, d3 = ORDERS[c]
                outs[c][at[d1], at[d2] * torus.n[d3] + at[d3], pl.ds(r, 16), :] = both
        return carry

    lax.fori_loop(0, count, body, 0)


def step_and_gather(torus, g, w, m, v, count, collective_id):
    ag = AllGather(torus, LAYERS * 3 * CHUNK * 256)
    plane = [("xy", (i, j)) for i in range(torus.n["x"]) for j in range(torus.n["y"]) if i + j]
    rounds = all_others(torus, "z"), plane

    def window(p, x):
        rows = WINDOW[x]
        first = lax.div(p * HIGH[x], SUB) * SUB
        return pl.multiple_of(jnp.minimum(first, HIGH[x] * torus.size - rows), SUB), rows

    def kernel(g_ref, *refs):
        w_in, m_in, v_in, G, m_out, v_out = (refs[i : i + 3] for i in range(0, 18, 3))
        flat, wflat, part, E, esend, erecv, ssem, rsem, win, wide_win, wsem = refs[18:]
        me = torus.here()
        p = lax.axis_index("dp")
        loads = []
        for x in TRIO:
            first, rows = window(p, x)
            loads.append(pltpu.make_async_copy(w_in[x].at[:, pl.ds(first, rows)], win[x], wsem.at[x]))
            loads[x].start()
        peers = rounds[0] + rounds[1]
        arrive(me, peers)
        acc = jnp.zeros((SUB, LANES), F32)
        for l in range(LAYERS):
            for u in TRIO:
                for k, c in enumerate(COLOURS[u]):
                    value = g_ref[l, u, c]
                    flat[l, u, pl.ds(k * CHUNK, CHUNK), :] = value
                    for r in range(0, CHUNK, SUB):
                        acc = acc + value[r : r + SUB] * value[r : r + SUB]
        part[0] = acc
        meet(peers)
        base = 0
        for i, others in enumerate(rounds):
            copies = []
            for s, (d, rel) in enumerate(others, base):
                copies.append(pltpu.make_async_remote_copy(src_ref=part.at[i], dst_ref=E.at[s], send_sem=esend.at[s], recv_sem=erecv.at[s], device_id=me.peer(d, rel), device_id_type=MESH))
            for copy in copies:
                copy.start()
            if i == 0:
                for x in TRIO:
                    loads[x].wait()
                    for lt in range(WIDE[x] // LANES):
                        wide_win[x][:, lt] = win[x][:, :, pl.ds(lt * LANES, LANES)].astype(F32)
            total = part[i]
            for s, copy in enumerate(copies, base):
                copy.wait_recv()
                total = total + E[s]
            part[i + 1] = total
            for copy in copies:
                copy.wait_send()
            base += len(others)
        mean = jnp.sum(part[2], keepdims=True) / count
        factor = jnp.minimum(1.0, 0.5 * lax.rsqrt(mean + 1e-30))
        for l in range(LAYERS):
            for u in TRIO:
                high = HIGH[u]
                wflat[l, u, pl.ds(ROWS - SUB, SUB), :] = jnp.zeros((SUB, LANES), F32)
                for ct in range(WIDE[u] // LANES):
                    x, lt = home(u, ct)
                    at = (slice(None), l, pl.ds(lt * LANES, LANES))
                    grad = flat[l, u, pl.ds(ct * high, high), :] * factor
                    new_m = 0.9 * m_in[x][at] + 0.1 * grad
                    new_v = 0.95 * v_in[x][at] + 0.05 * grad * grad
                    wide = wide_win[x][l, lt, pl.ds(p * high - window(p, x)[0], high), :]
                    new_w = wide - 0.02 * (new_m * lax.rsqrt(new_v + 1e-8) + 0.1 * wide)
                    m_out[x][at] = new_m
                    v_out[x][at] = new_v
                    wflat[l, u, pl.ds(ct * high, high), :] = new_w
        it = ag.bind(me, G, ssem, rsem)
        for u in TRIO:
            for c in TRIO:
                a, b, d = (me.up(x, 0) for x in ORDERS[c])
                for l in range(LAYERS):
                    G[c][a, b * torus.n[ORDERS[c][DIRECT]] + d, l, u] = wflat[l, u, pl.ds(c * CHUNK, CHUNK), :].astype(BF16)
        for a in ag.order:
            it.run(a)
        it.wait_sends()

    vmem = pl.BlockSpec(memory_space=pltpu.VMEM)
    nsum = len(rounds[0]) + len(rounds[1])
    shapes = [jax.ShapeDtypeStruct((torus.n[a], torus.n[b] * torus.n[d], LAYERS, 3, CHUNK, LANES), BF16) for a, b, d in ORDERS]
    turn = lambda ts: [jnp.transpose(t, (1, 0, 2)) for t in ts]
    m, v = turn(m), turn(v)
    f32 = [jax.ShapeDtypeStruct(t.shape, F32) for t in m]
    k = len(ag.copies)
    got = pl.pallas_call(
        kernel,
        out_shape=[pltpu.MemorySpace.VMEM(s.shape, s.dtype) for s in shapes + f32 * 2],
        in_specs=[vmem] + [pl.BlockSpec(memory_space=pl.ANY)] * 3 + [vmem] * 6,
        out_specs=[vmem] * 9,
        scratch_shapes=[
            pltpu.VMEM((LAYERS, 3, ROWS, LANES), F32),
            pltpu.VMEM((LAYERS, 3, ROWS, LANES), F32),
            pltpu.VMEM((3, SUB, LANES), F32),
            pltpu.VMEM((nsum, SUB, LANES), F32),
            pltpu.SemaphoreType.DMA((nsum,)),
            pltpu.SemaphoreType.DMA((nsum,)),
            pltpu.SemaphoreType.DMA((k,)),
            pltpu.SemaphoreType.DMA((k,)),
            [pltpu.VMEM((LAYERS, WINDOW[x], WIDE[x]), BF16) for x in TRIO],
            [pltpu.VMEM((LAYERS, WIDE[x] // LANES, WINDOW[x], LANES), F32) for x in TRIO],
            pltpu.SemaphoreType.DMA((3,)),
        ],
        compiler_params=pltpu.CompilerParams(collective_id=collective_id, has_side_effects=True, vmem_limit_bytes=26 * MIB),
        name="step_and_gather",
    )(g, *w, *m, *v)
    return got


def unpack(torus, got):
    nx, ny, nz = (torus.n[d] for d in "xyz")
    pair = 2
    group = pair * nz
    groups = torus.size // group
    pairs = ny // pair

    def kernel(g0, g1, g2, *refs):
        moments, outs, kept, (Z, Y, sem) = refs[:6], refs[6:9], refs[9:15], refs[15:]
        l, s = pl.program_id(0), pl.program_id(1)
        copies = [pltpu.make_async_copy(src, dst, sem.at[i]) for i, (src, dst) in enumerate(zip(moments, kept))]

        @pl.when(l + s == 0)
        def _():
            for copy in copies:
                copy.start()

        @pl.when(l + s == LAYERS - 1 + groups - 1)
        def _():
            for copy in copies:
                copy.wait()

        corner = {"x": lax.div(s, pairs), "y": lax.rem(s, pairs) * pair, "z": 0}
        for u in TRIO:
            high, wide = HIGH[u], WIDE[u] // LANES
            for i in range(group):
                y, z = divmod(i, nz)
                at = corner | {"y": corner["y"] + y, "z": z}
                for c, ref in enumerate((g0, g1, g2)):
                    a, b, d = ORDERS[c]
                    chunk = ref[at[a], at[b] * torus.n[d] + at[d], l, u].astype(F32)
                    if high > SUB:
                        for k, (ct, row, whole, more) in enumerate(tiles(u)[c * CHUNK // SUB : (c + 1) * CHUNK // SUB]):
                            Y[ct, pl.ds(high * i + row, whole), :] = chunk[SUB * k : SUB * k + whole]
                            if more and whole < SUB:
                                Y[ct + 1, pl.ds(high * i, SUB - whole), :] = chunk[SUB * k + whole : SUB * k + SUB]
                    else:
                        Z[i, pl.ds(c * CHUNK, CHUNK), :] = chunk
            for i in range(group):
                for ct in range(wide if high <= SUB else 0):
                    Y[ct, pl.ds(high * i, SUB), :] = Z[i, pl.ds(high * ct, SUB), :]
            rows = high * group
            for ct in range(wide):
                x, lt = home(u, ct)
                outs[x][0, :, pl.ds(lt * LANES, LANES)] = Y[ct, pl.ds(0, rows), :].astype(BF16)

    shapes = [(LAYERS, HIGH[u] * torus.size, WIDE[u]) for u in TRIO]
    return pl.pallas_call(
        kernel,
        grid=(LAYERS, groups),
        out_shape=[jax.ShapeDtypeStruct(s, BF16) for s in shapes] + [jax.ShapeDtypeStruct(m.shape, F32) for m in got[3:]],
        in_specs=[pl.BlockSpec(memory_space=pltpu.VMEM)] * 9,
        out_specs=[pl.BlockSpec((1, HIGH[u] * group, WIDE[u]), lambda l, s: (l, s, 0)) for u in TRIO] + [pl.BlockSpec(memory_space=pl.ANY)] * 6,
        scratch_shapes=[
            pltpu.VMEM((group, ROWS + SUB, LANES), F32),
            pltpu.VMEM((FF // LANES, HIGH[2] * group + SUB, LANES), F32),
            pltpu.SemaphoreType.DMA((6,)),
        ],
        compiler_params=pltpu.CompilerParams(vmem_limit_bytes=26 * MIB),
        name="unpack",
    )(*got)


NN, NT = ((1,), (0,)), ((1,), (1,))


def dot(a, b, dims=NN):
    return lax.dot_general(a, b, (dims, ((), ())), preferred_element_type=F32)


def scale_of(wide):
    return lax.rsqrt(jnp.mean(wide * wide, -1, keepdims=True) + 1e-6)


GAP = 24
SIDE_STRIDE, DOWN_STRIDE = D + GAP, FF // HALVES + GAP
DOWN_BASE = RING_TILES * SIDE_STRIDE
X_ROWS = DOWN_BASE + D // LANES * DOWN_STRIDE
COST = {"last": (3.5, 3.5), "first": (1.8, 3.5), "da": (2.5,), "norm": (0.45,)}
PACK_DOWN = 0.4
WHOLE = ((0,), (1, 2), (3, 4), (5, 6), (7, 8))
CHUNKS = {1: 0, 3: 1, 4: 2}
PASSES = ("forward", "last", "da", "norm", "first")
COUNT = {"forward": STEPS, "last": STEPS, "da": STEPS, "norm": TOKENS // TILE, "first": STEPS}
QUARTERS = TOKENS // PART
MAKE = 1


def timeline():
    out, lanes = [], ReduceScatter.LANES[RING]
    for kind in PASSES[1:]:
        layer = {"last": 1, "first": 0}.get(kind)
        for t in range(COUNT[kind]):
            half, tt = divmod(t, HALF)
            for i, cost in enumerate(COST[kind]):
                writes, whole = [], []
                if i == MAKE:
                    unit = (layer, half)
                    if tt == 0:
                        writes += [(unit, c) for c in TRIO]
                    if tt in CHUNKS:
                        whole += [((unit, COLOURS[half][CHUNKS[tt]]), lane) for lane in range(lanes)]
                    if tt == HALF - 1:
                        cost += PACK_DOWN
                        mine = [((layer, HALVES), c) for c in TRIO]
                        writes += [] if half else mine
                        whole += [(key, lane) for key in mine for lane in range(lanes) if half or lane == 0 and ORDERS[key[1]][CROSS] == "x"]
                out.append(((kind, t, i), cost, writes, whole))
    return out


def hidden_back(gate, up, d):
    s = jax.nn.sigmoid(gate)
    act = gate * s
    return (act * up).astype(BF16), (d * up * (s + act * (1.0 - s))).astype(BF16), (d * act).astype(BF16)


def gradients(torus, x, dy, wg, wu, wd, collective_id):
    rs = ReduceScatter(torus, CHUNK, 3)
    actions, copies, balance, flips = {}, {}, Balance(), {}
    for l in range(LAYERS):
        for u in TRIO:
            for c in TRIO:
                flips[l, u, c] = rs.flips(balance, c)
                got, sent = rs.plan((l, u), c, flips[l, u, c])
                copies |= sent
                actions |= got
                if l:
                    key = ((l, u), c)
                    actions[key, "free"] = ([("action", (key, "end", DIRECT))], [], TURN)
    slots = place(actions, copies, timeline())
    lines = torus.n["x"] * torus.n["y"]

    def kernel(x_ref, dy_ref, wg_ref, wu_ref, wd_ref, out, both_ref, gate_ref, up_ref, h1_ref, at0_ref, dyv, av, at, X, Mb, Db, Wb, Vb, Hb, once, pair, hsem, rsem, rsc):
        me = torus.here()
        it = rs.bind(me, rsc)
        copy = pltpu.make_async_copy
        save_at0, load_at0 = copy(at, at0_ref, once.at[1]), copy(at0_ref, at, once.at[1])

        def part(i):
            return pl.ds(i * TILE if isinstance(i, int) else pl.multiple_of(i * TILE, TILE), TILE)

        def sides(layer, t, s):
            return [copy(ref.at[layer, :, part(t)], Wb.at[s, :, part(k)], pair.at[k, s]) for k, ref in enumerate((wg_ref, wu_ref))]

        def fetch(kind, t, s):
            both, rows = pair.at[2, s], pair.at[3, s]
            if kind == "forward":
                return sides(0, t, s) + [copy(wd_ref.at[0, part(t)], Vb.at[s], rows)]
            if kind == "last":
                return sides(1, t, s) + [copy(wd_ref.at[1, part(t)], Vb.at[s], rows)]
            if kind == "da":
                return sides(1, t, s) + [copy(both_ref.at[t], Db.at[s], both)]
            if kind == "norm":
                return [copy(h1_ref.at[part(t)], Vb.at[s], rows)]
            return [copy(wd_ref.at[0, part(t)], Vb.at[s], rows)]

        def save(t, s):
            return copy(Db.at[s], both_ref.at[t], pair.at[4, s])

        def hiddens(t, quarters, out=False):
            got = []
            for q in quarters:
                for k, ref in enumerate((gate_ref, up_ref)):
                    ends = ref.at[pl.ds(t * LT, LT), pl.ds(q * PART, PART)], Hb.at[q, k]
                    got.append(copy(*(ends[::-1] if out else ends), hsem.at[q, k]))
            return got

        def act(a):
            ((l, u), c), what = a[0], a[1:]
            if what[0] == "free":
                it.wait_sends(u, c, flips[l, u, c])
                it.give_credit(u, c)
                return
            if what == ("start", 0) and l == 0:
                it.take_credit(u, c)

            def store(value):
                out[l, u, c] = value

            it.run(u, c, flips[l, u, c], what, store)

        def point(kind, t, i, which):
            for k in range(COUNT[kind]):
                if slots[kind, k, i][which]:

                    @pl.when(t == k)
                    def _(k=k):
                        for a in slots[kind, k, i][which]:
                            act(a)

        def normed_into(r):
            wide = dyv[part(r), :].astype(F32)
            a = (wide * scale_of(wide)).astype(BF16)
            av[part(r), :] = a
            at[:, part(r)] = a.T

        def lanes_of(ct):
            return slice(ct * LANES, (ct + 1) * LANES)

        def forward(t, s):
            for first in range(0, QUARTERS, 2):
                quarters = range(first, first + 2)

                @pl.when(t > 0)
                def _():
                    for f in hiddens(t - 1, quarters, True):
                        f.wait()

                for q in quarters:
                    rows = pl.ds(q * PART, PART)
                    both = dot(av[rows, :], Wb[s])
                    gate, up = both[:, :TILE], both[:, TILE:]
                    for j in range(LT):
                        Hb[q, 0, j], Hb[q, 1, j] = gate[:, lanes_of(j)], up[:, lanes_of(j)]
                    got = dot((jax.nn.silu(gate) * up).astype(BF16), Vb[s])
                    for ct in range(D // LANES):
                        here = pl.ds(ct * TOKENS + q * PART, PART)
                        X[here, :] = jnp.where(t == 0, 0.0, X[here, :]) + got[:, lanes_of(ct)]
                for f in hiddens(t, quarters, True):
                    f.start()

        def turn():
            for f in hiddens(STEPS - 1, range(QUARTERS), True):
                f.wait()
            save_at0.wait()
            count = TOKENS // TILE

            def saves(r):
                return copy(dyv.at[part(r)], h1_ref.at[part(r)], rsem.at[0, r])

            def loads(r):
                return copy(dy_ref.at[part(r)], dyv.at[part(r)], rsem.at[1, r])

            @pl.loop(0, count)
            def _(r):
                total = jnp.concatenate([X[pl.ds(ct * TOKENS + r * TILE, TILE), :] for ct in range(D // LANES)], axis=1)
                dyv[part(r), :] = dyv[part(r), :] + total.astype(BF16)
                normed_into(r)
                saves(r).start()

                @pl.when(r > 0)
                def _():
                    saves(r - 1).wait()
                    loads(r - 1).start()

            saves(count - 1).wait()
            loads(count - 1).start()
            for r in range(count):
                loads(r).wait()

        def hidden(kind, t, s):
            for first in range(0, QUARTERS, 2):
                quarters = range(first, first + 2)
                if kind == "first":
                    for f in hiddens(t, quarters):
                        f.wait()
                for q in quarters:
                    rows = pl.ds(q * PART, PART)
                    if kind == "last":
                        both = dot(av[rows, :], Wb[s])
                        gate, up = both[:, :TILE], both[:, TILE:]
                    else:
                        gate, up = (jnp.concatenate([Hb[q, k, j] for j in range(LT)], axis=1) for k in range(2))
                    d = dot(dyv[rows, :], Vb[s], NT).astype(BF16).astype(F32)
                    mid, Db[s, rows, part(0)], Db[s, rows, part(1)] = hidden_back(gate, up, d)
                    Mb[:, rows] = mid.T
                if kind == "first":

                    @pl.when(t + 1 < STEPS)
                    def _():
                        for f in hiddens(t + 1, quarters):
                            f.start()

        def make(kind, t, s):
            half, tt = lax.div(t, HALF), lax.rem(t, HALF)
            got = dot(at[...], Db[s])
            for k in range(2 * LT):
                X[pl.ds((lax.rem(tt, 2) * 2 * LT + k) * SIDE_STRIDE + 8, D), :] = got[:, lanes_of(k)]
            got = dot(Mb[...], dyv[...])
            for ct in range(D // LANES):
                X[pl.ds(DOWN_BASE + ct * DOWN_STRIDE + 8 + tt * TILE, TILE), :] = got[:, lanes_of(ct)]
            point(kind, t, MAKE, 0)
            for v, parts in enumerate(WHOLE):

                @pl.when(tt == v)
                def _(parts=parts):
                    pack(torus, 0, X, lambda ct: ct % RING_TILES * SIDE_STRIDE + 8, parts, 0, lines, [T.at[half] for T in it.T], COLOURS[0])

            @pl.when(tt == HALF - 1)
            def _():
                some = lines // HALVES
                pack(torus, HALVES, X, lambda ct: DOWN_BASE + ct * DOWN_STRIDE + 8, range(ROWS // 16), half * some, some, [T.at[HALVES] for T in it.T], COLOURS[HALVES])

        def d_a(t, s):
            for r in range(0, TOKENS, PART):
                got = dot(Db[s, pl.ds(r, PART), :], Wb[s], NT)
                for ct in range(D // LANES):
                    rows = pl.ds(ct * TOKENS + r, PART)
                    X[rows, :] = jnp.where(t == 0, 0.0, X[rows, :]) + got[:, lanes_of(ct)]

        def norm(t, s):
            da = jnp.concatenate([X[pl.ds(ct * TOKENS + t * TILE, TILE), :] for ct in range(D // LANES)], axis=1).astype(BF16).astype(F32)
            wide = Vb[s].astype(F32)
            scale = scale_of(wide)
            inner = jnp.mean(da * wide, -1, keepdims=True)
            dyv[part(t), :] = dyv[part(t), :] + (scale * da - wide * (scale * scale * scale * inner)).astype(BF16)

        def load_x(r):
            return copy(x_ref.at[part(r)], dyv.at[part(r)], rsem.at[0, r])

        for f in [load_x(r) for r in range(TOKENS // TILE)] + fetch("forward", 0, 0):
            f.start()
        arrive(me, rs.peers())

        @pl.loop(0, TOKENS // TILE)
        def _(r):
            load_x(r).wait()
            normed_into(r)

        save_at0.start()
        for number, kind in enumerate(PASSES):
            count = COUNT[kind]
            following = PASSES[number + 1] if number + 1 < len(PASSES) else None
            if kind == "last":
                turn()
                meet(rs.peers())
            if kind == "da":
                load_at0.start()
            if kind == "norm":
                for f in hiddens(0, range(QUARTERS)):
                    f.start()
            if kind == "first":
                load_at0.wait()

            def body(t, carry, kind=kind, count=count, following=following):
                s = lax.rem(t, 2)
                for f in fetch(kind, t, s):
                    f.wait()

                @pl.when(t + 1 < count)
                def _():
                    for f in fetch(kind, t + 1, 1 - s):
                        f.start()

                if kind == "last":

                    @pl.when(t > 1)
                    def _():
                        save(t - 2, s).wait()

                if following:

                    @pl.when(t == count - 1)
                    def _():
                        if kind == "last":
                            save(t - 1, 1 - s).wait()
                        for f in fetch(following, 0, 0):
                            f.start()

                if kind in ("last", "first"):
                    hidden(kind, t, s)
                    if kind == "last":
                        save(t, s).start()
                    point(kind, t, 0, 1)
                    make(kind, t, s)
                    point(kind, t, MAKE, 1)
                else:
                    {"forward": forward, "da": d_a, "norm": norm}[kind](t, s)
                    if kind != "forward":
                        point(kind, t, 0, 1)
                return carry

            lax.fori_loop(0, count, body, 0)
            if kind == "last":
                save(count - 1, (count - 1) % 2).wait()
        for u in TRIO:
            for c in TRIO:
                it.wait_sends(u, c, flips[0, u, c])

    any_space = pl.BlockSpec(memory_space=pl.ANY)
    return pl.pallas_call(
        kernel,
        out_shape=[jax.ShapeDtypeStruct((LAYERS, 3, 3, CHUNK, LANES), F32), jax.ShapeDtypeStruct((STEPS, TOKENS, 2 * TILE), BF16)]
        + [jax.ShapeDtypeStruct((FF // LANES, TOKENS, LANES), F32)] * 2
        + [jax.ShapeDtypeStruct((TOKENS, D), BF16), jax.ShapeDtypeStruct((D, TOKENS), BF16)],
        in_specs=[any_space] * 5,
        out_specs=[pl.BlockSpec(memory_space=pltpu.VMEM)] + [any_space] * 5,
        scratch_shapes=[
            pltpu.VMEM((TOKENS, D), BF16),
            pltpu.VMEM((TOKENS, D), BF16),
            pltpu.VMEM((D, TOKENS), BF16),
            pltpu.VMEM((X_ROWS, LANES), F32),
            pltpu.VMEM((TILE, TOKENS), BF16),
            pltpu.VMEM((2, TOKENS, 2 * TILE), BF16),
            pltpu.VMEM((2, D, 2 * TILE), BF16),
            pltpu.VMEM((2, TILE, D), BF16),
            pltpu.VMEM((QUARTERS, 2, LT, PART, LANES), F32),
            pltpu.SemaphoreType.DMA((2,)),
            pltpu.SemaphoreType.DMA((5, 2)),
            pltpu.SemaphoreType.DMA((QUARTERS, 2)),
            pltpu.SemaphoreType.DMA((2, TOKENS // TILE)),
            rs.scratch(),
        ],
        compiler_params=pltpu.CompilerParams(collective_id=collective_id, has_side_effects=True, vmem_limit_bytes=VMEM_ALL),
        cost_estimate=pl.CostEstimate(flops=TOKENS * D * FF * 24, bytes_accessed=TOKENS * FF * 20, transcendentals=0),
        name="gradients",
    )(x, dy, wg, wu, wd)[0]


def solution(mesh):
    torus = Torus(4, 4, 8)
    count = float(LAYERS * 3 * D * FF)

    def step(x, dy, wg, wu, wd, mg, mu, md, vg, vu, vd):
        x, dy = x[0], dy[0]
        g = gradients(torus, x, dy, wg, wu, wd, 1)
        got = step_and_gather(torus, g, (wg, wu, wd), (mg, mu, md), (vg, vu, vd), count, 2)
        new = unpack(torus, got)
        return (*new[:3], *(jnp.transpose(t, (1, 0, 2)) for t in new[3:]))

    P = jax.sharding.PartitionSpec
    return jax.shard_map(
        step,
        mesh=mesh,
        in_specs=(P(("rep", "dp")),) * 2 + (P(),) * 3 + (P(None, "dp"),) * 6,
        out_specs=(P("rep"),) * 3 + (P("rep", "dp"),) * 6,
        check_vma=False,
    )
```

```python
import heapq
import jax
import jax.numpy as jnp
from jax import lax
from jax.experimental import pallas as pl
from jax.experimental.pallas import tpu as pltpu

F32, BF16 = jnp.float32, jnp.bfloat16
MESH = pl.DeviceIdType.MESH
RATE, LATENCY, SLACK = 46.6e3, 2.9, 0.6
TURN, ADD, HOP = 0.1, 2.0e6, 0.7
WAYS = (1, -1)
TRIO = range(3)
RING, CROSS, DIRECT = TRIO
NEVER, MARGIN, SWEEPS = 1e9, (0.3, 1.2), 3


class Torus:
    def __init__(self, nx, ny, nz):
        self.n = {"x": nx, "y": ny, "z": nz}
        self.size = nx * ny * nz

    def here(self):
        return Here(self)


class Here:
    def __init__(self, torus):
        p, n = lax.axis_index("dp"), torus.n
        ny, nz = n["y"], n["z"]
        mine = {"z": lax.rem(p, nz), "y": lax.rem(lax.div(p, nz), ny), "x": lax.div(p, ny * nz)}
        step = {"z": 1, "y": nz, "x": ny * nz}
        self.at = {d: [mine[d]] + [lax.rem(mine[d] + i, n[d]) for i in range(1, n[d])] for d in n}
        self.to = {d: [p + (self.at[d][i] - mine[d]) * step[d] for i in range(n[d])] for d in n}

    def peer(self, dim, delta):
        if dim == "xy":
            dx, dy = delta
            return {"dp": self.to["x"][dx] + self.to["y"][dy] - self.to["x"][0]}
        return {"dp": self.to[dim][delta % len(self.to[dim])]}

    def up(self, dim, delta):
        return self.at[dim][delta % len(self.at[dim])]


ORDERS = ("zxy", "xyz", "yxz")


def hops(n, flip):
    far, near = n // 2, n - 1 - n // 2
    return {1: near, -1: far} if flip else {1: far, -1: near}


class Balance:
    def __init__(self):
        self.load = {}

    def flip(self, dim, n, size):
        plain = [self.load.get((dim, s), 0) + size * hops(n, False)[s] for s in WAYS]
        turned = [self.load.get((dim, s), 0) + size * hops(n, True)[s] for s in WAYS]
        flip = max(turned) < max(plain)
        self.load[dim, 1], self.load[dim, -1] = turned if flip else plain
        return flip


def simulate(actions, copies):
    links, arrived, order = {}, {}, []
    waiting = {a: set(needs) for a, (needs, _, _, _) in actions.items()}
    by_need = {}
    for a, (needs, _, _, _) in actions.items():
        for c in needs:
            by_need.setdefault(c, []).append(a)
    ready = [(actions[a][3], i, a) for i, a in enumerate(actions) if not waiting[a]]
    rank = {a: i for i, a in enumerate(actions)}
    heapq.heapify(ready)
    now, done = 0.0, {}
    while ready:
        at, _, a = heapq.heappop(ready)
        now = max(now, at) + actions[a][2]
        order.append(a)
        done[a] = now
        for c in [("action", a)] + list(actions[a][1]):
            if c[0] == "action":
                end = now
            else:
                link, size, extra = copies[c]
                start = max(now, links.get(link, 0.0))
                links[link] = start + size / RATE
                end = links[link] + LATENCY + SLACK + extra
            for b in by_need.get(c, ()):
                waiting[b].discard(c)
                arrived[b] = max(arrived.get(b, 0.0), end)
                if not waiting[b]:
                    heapq.heappush(ready, (max(arrived[b], actions[b][3]), rank[b], b))
    assert len(order) == len(actions), (len(order), len(actions))
    return order, now


def place(actions, copies, segments):
    links, known, left, slots, open_keys = {}, {}, dict(actions), {}, set()
    now = 0.0

    def do(a, where):
        nonlocal now
        _, sends, cost = left.pop(a)
        now += cost
        known["action", a] = now
        for c in sends:
            link, size, extra = copies[c]
            links[link] = max(now, links.get(link, 0.0)) + size / RATE
            known[c] = links[link] + LATENCY + extra
        where.append(a)

    def drain(where, allowed, wait):
        nonlocal now
        while True:
            able = [(max([known.get(c, NEVER) for c in actions[a][0]], default=0.0), i, a) for i, a in enumerate(left) if allowed(a)]
            best, _, a = min(able, default=(NEVER, 0, None))
            if best >= NEVER or not wait and best + MARGIN[a[0][0][0]] > now:
                return
            now = max(now, best)
            do(a, where)

    for key, cost, writes, whole in segments:
        now += cost
        slots[key] = ([], [])
        others = {(l, u, c) for (l, u), c in writes}
        drain(slots[key][0], lambda a: any(a[0][0][1] == u and a[0][1] == c and a[0][0][0] > l for l, u, c in others), True)
        open_keys |= set(whole)
        drain(slots[key][1], lambda a: a[1] != "start" or (a[0], a[2]) in open_keys, False)
    drain(slots[segments[-1][0]][1], lambda a: True, True)
    assert not left
    place.took = now
    return slots


def arrive(me, peers):
    sem = pltpu.get_barrier_semaphore()
    for dim, delta in peers:
        pl.semaphore_signal(sem, inc=1, device_id=me.peer(dim, delta), device_id_type=MESH)


def meet(peers):
    pl.semaphore_wait(pltpu.get_barrier_semaphore(), len(peers))


def both_ways(torus, dim):
    n = torus.n[dim]
    return [] if n == 1 else [(dim, 1)] if n == 2 else [(dim, 1), (dim, -1)]


def all_others(torus, dim):
    return [(dim, d) for d in range(1, torus.n[dim])]


class ReduceScatter:
    LANES = (2, 1, 1)

    def __init__(self, torus, rows, units):
        self.t, self.rows, self.units = torus, rows, units
        self.dims = [tuple(order) for order in ORDERS]
        self.nslots = max(self.base(c, DIRECT, 0) + self.sizes(c)[DIRECT] - 1 for c in TRIO)

    def sizes(self, c):
        return [self.t.n[d] for d in self.dims[c]]

    def here(self, c):
        return [self.me.up(d, 0) for d in self.dims[c]]

    def base(self, c, phase, lane):
        n = self.sizes(c)
        return sum((n[i] - 1) * self.LANES[i] for i in range(phase)) + lane * (n[phase] - 1)

    def peers(self):
        full = {dims[DIRECT] for dims in self.dims}
        out = []
        for dim in "xyz":
            out += all_others(self.t, dim) if dim in full else both_ways(self.t, dim)
        return out

    def credit_peers(self, c):
        a, b, d = self.dims[c]
        return both_ways(self.t, a) + both_ways(self.t, b) + all_others(self.t, d)

    def scratch(self):
        n = self.t.n
        t, r1, r2, r3, k2, k3 = [], [], [], [], [], []
        for dims in self.dims:
            n1, n2, n3 = (n[d] for d in dims)
            tail = (self.rows, 128)
            t.append(pltpu.VMEM((self.units, n1, n2 * n3) + tail, BF16))
            r1.append(pltpu.VMEM((self.units, max(n1 - 1, 1), n2 * n3) + tail, BF16))
            r2.append(pltpu.VMEM((self.units, max(n2 - 1, 1), n3) + tail, BF16))
            r3.append(pltpu.VMEM((self.units, max(n3 - 1, 1)) + tail, BF16))
            k2.append(pltpu.VMEM((self.units, n3) + tail, F32))
            k3.append(pltpu.VMEM((self.units,) + tail, F32))
        sems = [pltpu.SemaphoreType.DMA((self.units, 3, self.nslots)), pltpu.SemaphoreType.DMA((self.units, 3, self.nslots)), pltpu.SemaphoreType.REGULAR((self.units, 3))]
        return [t, r1, r2, r3, k2, k3] + sems

    def slot(self, c, phase, sign, h):
        return h if sign > 0 else self.sizes(c)[phase] - 2 - h

    def flips(self, balance, c):
        n1, n2, n3 = self.sizes(c)
        block, (a, b, d) = self.rows * 256, self.dims[c]
        for rel in range(1, n3):
            link = d, 1 if rel <= n3 // 2 else -1
            balance.load[link] = balance.load.get(link, 0) + block * min(rel, n3 - rel)
        ring = [balance.flip(a, n1, block * n2 * n3 // self.LANES[RING]) for _ in range(self.LANES[RING])]
        return ring, [balance.flip(b, n2, block * n3)]

    def plan(self, unit, c, flip):
        n = self.sizes(c)
        n1, n2, n3 = n
        block = self.rows * 256
        size = [block * n2 * n3 // self.LANES[RING], block * n3, block]
        actions, copies = {}, {}
        key = (unit, c)

        def send(phase, lane, sign, h):
            cid = ("copy", key, phase, lane, sign, h)
            copies[cid] = ((self.dims[c][phase], sign), size[phase], 0)
            return cid

        first, last = [[], []], [[], []]
        for phase in (RING, CROSS):
            for lane, turned in enumerate(flip[phase]):
                k = hops(n[phase], turned)
                ways = [s for s in WAYS if k[s]]
                first[phase] += [send(phase, lane, s, k[s] - 1) for s in ways]
                last[phase] += [("copy", key, phase, lane, s, 0) for s in ways]
                for s in ways:
                    for h in range(k[s] - 1, 0, -1):
                        actions[key, "step", phase, lane, s, h] = ([("copy", key, phase, lane, s, h)], [send(phase, lane, s, h - 1)], size[phase] / ADD)
        direct = []
        for rel in range(1, n3):
            cid = ("copy", key, DIRECT, 0, 0, rel)
            far = min(rel, n3 - rel)
            copies[cid] = ((self.dims[c][DIRECT], 1 if rel <= n3 // 2 else -1), size[DIRECT] * far, HOP * (far - 1))
            direct.append(cid)
        sends = first + [direct, []]
        for lane in range(self.LANES[RING]):
            actions[key, "start", lane] = ([], [x for x in sends[RING] if x[3] == lane], TURN)
        before = (key, "start", 0)
        for phase, needs in enumerate(last + [direct]):
            a = (key, "end", phase)
            actions[a] = (needs + [("action", before)], sends[phase + 1], size[phase] * self.LANES[phase] / ADD + TURN)
            before = a
        return actions, copies

    def bind(self, me, refs):
        self.me, (self.T, self.R1, self.R2, self.R3, self.K2, self.K3, self.ssem, self.rsem, self.credit) = me, refs
        return self

    def remote(self, u, c, phase, lane, sign, h):
        n1, n2, n3 = self.sizes(c)
        d1, d2, d3 = self.dims[c]
        up = self.me.up
        mine = self.T[c].at[u]
        slot = h - 1 if phase == DIRECT else self.slot(c, phase, sign, h)
        if phase == RING:
            part = n2 * n3 // self.LANES[RING]
            blocks = pl.ds(lane * part, part)
            src, dst = mine.at[up(d1, sign * (h + 1)), blocks], self.R1[c].at[u, slot, blocks]
        elif phase == CROSS:
            src, dst = mine.at[up(d1, 0), pl.ds(up(d2, sign * (h + 1)) * n3, n3)], self.R2[c].at[u, slot]
        else:
            sign = h
            src, dst = mine.at[up(d1, 0), up(d2, 0) * n3 + up(d3, h)], self.R3[c].at[u, slot]
        s = self.base(c, phase, lane) + slot
        to = self.me.peer(self.dims[c][phase], sign)
        return pltpu.make_async_remote_copy(src_ref=src, dst_ref=dst, send_sem=self.ssem.at[u, c, s], recv_sem=self.rsem.at[u, c, s], device_id=to, device_id_type=MESH)

    def all_sends(self, c, flip):
        n = self.sizes(c)
        out = []
        for phase in (RING, CROSS):
            for lane, turned in enumerate(flip[phase]):
                k = hops(n[phase], turned)
                out += [(phase, lane, s, h) for s in WAYS for h in range(k[s])]
        return out + [(DIRECT, 0, 0, rel) for rel in range(1, n[DIRECT])]

    def run(self, u, c, flip, what, store):
        n = self.sizes(c)
        n1, n2, n3 = n
        m1, m2, m3 = self.here(c)
        T, R1, R2, R3 = (r[c].at[u] for r in (self.T, self.R1, self.R2, self.R3))
        K2, K3 = self.K2[c].at[u], self.K3[c].at[u]
        mine = T.at[m1]
        wide = lambda v: v.astype(F32)
        go = lambda *a: self.remote(u, c, *a)

        def loop(count, body):
            def one(i, carry):
                body(i)
                return carry

            lax.fori_loop(0, count, one, 0)

        def line(q):
            return pl.ds(q * n3, n3)

        def ways(phase):
            for lane, turned in enumerate(flip[phase]):
                k = hops(n[phase], turned)
                for s in WAYS:
                    if k[s]:
                        yield lane, s, k[s]

        def sends(phase, only=None):
            for lane, s, k in ways(phase):
                if only in (None, lane):
                    go(phase, lane, s, k - 1).start()

        def arrived(phase):
            got = set()
            for lane, s, _ in ways(phase):
                go(phase, lane, s, 0).wait_recv()
                got.add(self.slot(c, phase, s, 0))
            return sorted(got)

        kind, *where = what
        if kind == "start":
            sends(RING, *where)
        elif kind == "step":
            phase, lane, s, h = where
            go(*where).wait_recv()
            slot = self.slot(c, phase, s, h)
            q = self.me.up(self.dims[c][phase], s * h)
            if phase == RING:
                lines = n2 // self.LANES[RING]

                def add(i):
                    b = line(lane * lines + i)
                    T[q, b] = (wide(T[q, b]) + wide(R1[slot, b])).astype(BF16)

                loop(lines, add)
            else:
                mine[line(q)] = (wide(mine[line(q)]) + wide(R2[slot])).astype(BF16)
            go(phase, lane, s, h - 1).start()
        elif where == [RING]:
            got = arrived(RING)

            def total(b):
                return sum((wide(R1[g, b]) for g in got), wide(mine[b]))

            def others(i):
                b = line(lax.rem(m2 + 1 + i, n2))
                mine[b] = total(b).astype(BF16)

            loop(n2 - 1, others)
            sends(CROSS)
            K2[...] = total(line(m2))
        elif where == [CROSS]:
            got = arrived(CROSS)
            total = sum((wide(R2[g]) for g in got), K2[...])
            K2[...] = total
            mine[line(m2)] = total.astype(BF16)
            for rel in range(1, n3):
                go(DIRECT, 0, 0, rel).start()
            K3[...] = K2[m3]
        else:
            for rel in range(1, n3):
                go(DIRECT, 0, 0, rel).wait_recv()
            store(sum((wide(R3[i]) for i in range(n3 - 1)), K3[...]).astype(BF16).astype(F32))

    def wait_sends(self, u, c, flip):
        for a in self.all_sends(c, flip):
            self.remote(u, c, *a).wait_send()

    def give_credit(self, u, c):
        for dim, delta in self.credit_peers(c):
            pl.semaphore_signal(self.credit.at[u, c], inc=1, device_id=self.me.peer(dim, delta), device_id_type=MESH)

    def take_credit(self, u, c):
        pl.semaphore_wait(self.credit.at[u, c], len(self.credit_peers(c)))


class AllGather:
    def __init__(self, torus, block_bytes, split=4):
        self.t, self.bytes, self.split = torus, block_bytes, split
        self.dims = [tuple(order) for order in ORDERS]
        self.flip, self.balance = {}, Balance()
        self.build()
        for key in list(self.flip) * SWEEPS:
            took = self.took
            self.flip[key] = not self.flip[key]
            self.build()
            if self.took >= took:
                self.flip[key] = not self.flip[key]
        self.build()

    def build(self):
        self.copies, self.actions, self.index = {}, {}, {}
        for c in TRIO:
            self.plan(c)
        self.order, self.took = simulate({a: (*v, 0) for a, v in self.actions.items()}, self.copies)

    def peers(self):
        return [p for dim in "xyz" for p in both_ways(self.t, dim)]

    def pieces(self, c, j):
        n3 = self.t.n[self.dims[c][DIRECT]]
        return n3 if not j else self.split if n3 % self.split == 0 else 1

    def size(self, c, phase, j):
        line = self.bytes * self.t.n[self.dims[c][DIRECT]]
        return self.bytes if phase == DIRECT else line // self.pieces(c, 1 if phase == CROSS else j)

    def k(self, c, phase, j, i):
        dim = self.dims[c][phase]
        key = (c, phase, j, i)
        if key not in self.flip:
            self.flip[key] = self.balance.flip(dim, self.t.n[dim], self.size(c, phase, j))
        return hops(self.t.n[dim], self.flip[key])

    def plan(self, c):
        n1, n2, n3 = (self.t.n[d] for d in self.dims[c])

        def send(where, s, h):
            phase, j, _ = where
            cid = (c, where, s, h)
            self.copies[cid] = ((self.dims[c][phase], s), self.size(c, phase, j), 0)
            self.index[cid] = len(self.index)
            return cid

        def own(*where):
            k = self.k(c, *where)
            return [send(where, s, 1) for s in WAYS if k[s]]

        def passing(*where):
            k = self.k(c, *where)
            for s in WAYS:
                for h in range(1, k[s] + 1):
                    yield s, h, (c, "pass", where, s, h), [(c, where, s, h)], [send(where, s, h + 1)] if h < k[s] else []

        def act(a, needs, sends):
            self.actions[a] = (needs, sends, TURN / 2)

        act((c, "start"), [], own(DIRECT, 0, 0) + own(RING, 0, 0))
        got = [("action", (c, "start"))]
        for s, h, a, needs, sends in passing(DIRECT, 0, 0):
            act(a, needs, sends + own(RING, 0, (-s * h) % n3))
            got.append(("action", a))
        parts = range(self.pieces(c, 1))
        act((c, "line"), got, [x for i in parts for x in own(CROSS, 0, i)])
        for i in parts:
            for s, h, a, needs, sends in passing(CROSS, 0, i):
                after = (-s * h) % n2, i
                if c:
                    act(a, needs, sends + own(RING, *after))
                else:
                    act(a, needs, sends)
                    act((c, "later", *after), [("action", x) for x in (a, (1, "line"), (2, "line"))], own(RING, *after))
        for j in range(n2):
            for i in range(self.pieces(c, j)):
                for _, _, a, needs, sends in passing(RING, j, i):
                    act(a, needs, sends)

    def bind(self, me, G, ssem, rsem):
        self.me, self.G, self.ssem, self.rsem = me, G, ssem, rsem
        return self

    def remote(self, cid, back):
        c, (phase, j, i), s, h = cid
        d1, d2, d3 = self.dims[c]
        n3, up = self.t.n[d3], self.me.up
        off = s * (back - h)
        G = self.G[c]
        if phase == DIRECT:
            ref = G.at[up(d1, 0), up(d2, 0) * n3 + up(d3, off)]
        elif phase == CROSS:
            size = n3 // self.pieces(c, 1)
            ref = G.at[up(d1, 0), pl.ds(up(d2, off) * n3 + i * size, size)]
        elif j == 0:
            ref = G.at[up(d1, off), up(d2, 0) * n3 + up(d3, i)]
        else:
            size = n3 // self.pieces(c, j)
            ref = G.at[up(d1, off), pl.ds(up(d2, j) * n3 + i * size, size)]
        x = self.index[cid]
        return pltpu.make_async_remote_copy(src_ref=ref, dst_ref=ref, send_sem=self.ssem.at[x], recv_sem=self.rsem.at[x], device_id=self.me.peer(self.dims[c][phase], s), device_id_type=MESH)

    def run(self, a):
        needs, sends, _ = self.actions[a]
        for cid in needs:
            if cid in self.index:
                self.remote(cid, 0).wait_recv()
        for cid in sends:
            self.remote(cid, 1).start()

    def wait_sends(self):
        for cid in self.copies:
            self.remote(cid, 1).wait_send()


MIB = 2**20
VMEM_ALL = 67043328
LAYERS, D, FF = 2, 896, 2560
LANES, SUB, ROWS, CHUNK = 128, 8, 144, 48
HIGH = {0: 7, 1: 7, 2: 20}
WIDE = {0: FF, 1: FF, 2: D}
WINDOW = (16, 16, 24)


HALVES, RING_TILES = 2, 8
COLOURS = {0: (1, 2, 0), 1: (1, 2, 0), 2: (0, 1, 2)}
TOKENS, TILE, PART = 2048, 256, 512
LT, STEPS = TILE // LANES, FF // TILE
HALF = STEPS // HALVES


def home(u, ct):
    if u == HALVES:
        return u, ct
    t, k = divmod(ct, 2 * LT)
    m, j = divmod(k, LT)
    return m, (u * HALF + t) * LT + j


def tiles(u):
    high, wide = HIGH[u], WIDE[u] // LANES
    out = []
    for k in range(ROWS // SUB):
        ct, row = divmod(SUB * k, high)
        out.append((ct, row, min(SUB, high - row), ct + 1 < wide))
    return out


def pack(torus, u, X, base, parts, first, count, outs, colours):
    high, ny, nz = HIGH[u], torus.n["y"], torus.n["z"]
    sub = lax.broadcasted_iota(jnp.int32, (SUB, LANES), 0)
    got = tiles(u)

    def body(line, carry):
        x, y = lax.div(first + line, ny), lax.rem(first + line, ny)
        top = pl.multiple_of(line * (high * nz), SUB)

        def piece(z, ct, row, whole, more):
            a = X[pl.ds(top + (base(ct) + high * z + row), SUB), :]
            if whole == SUB:
                return a
            b = X[pl.ds(top + (base(ct + 1) + high * z - whole), SUB), :] if more else jnp.zeros((SUB, LANES), F32)
            return jnp.where(sub < whole, a, b)

        for z in range(nz):
            at = {"x": x, "y": y, "z": z}
            for j in parts:
                both = jnp.concatenate([piece(z, *got[2 * j]), piece(z, *got[2 * j + 1])], axis=0).astype(BF16)
                k, r = divmod(16 * j, CHUNK)
                c = colours[k]
                d1, d2, d3 = ORDERS[c]
                outs[c][at[d1], at[d2] * torus.n[d3] + at[d3], pl.ds(r, 16), :] = both
        return carry

    lax.fori_loop(0, count, body, 0)


def step_and_gather(torus, g, w, m, v, count, collective_id):
    ag = AllGather(torus, LAYERS * 3 * CHUNK * 256)
    plane = [("xy", (i, j)) for i in range(torus.n["x"]) for j in range(torus.n["y"]) if i + j]
    rounds = all_others(torus, "z"), plane

    def window(p, x):
        rows = WINDOW[x]
        first = lax.div(p * HIGH[x], SUB) * SUB
        return pl.multiple_of(jnp.minimum(first, HIGH[x] * torus.size - rows), SUB), rows

    def kernel(g_ref, *refs):
        w_in, m_in, v_in, G, m_out, v_out = (refs[i : i + 3] for i in range(0, 18, 3))
        flat, wflat, part, E, esend, erecv, ssem, rsem, win, wide_win, wsem = refs[18:]
        me = torus.here()
        p = lax.axis_index("dp")
        loads = []
        for x in TRIO:
            first, rows = window(p, x)
            loads.append(pltpu.make_async_copy(w_in[x].at[:, pl.ds(first, rows)], win[x], wsem.at[x]))
            loads[x].start()
        peers = rounds[0] + rounds[1]
        arrive(me, peers)
        acc = jnp.zeros((SUB, LANES), F32)
        for l in range(LAYERS):
            for u in TRIO:
                for k, c in enumerate(COLOURS[u]):
                    value = g_ref[l, u, c]
                    flat[l, u, pl.ds(k * CHUNK, CHUNK), :] = value
                    for r in range(0, CHUNK, SUB):
                        acc = acc + value[r : r + SUB] * value[r : r + SUB]
        part[0] = acc
        meet(peers)
        base = 0
        for i, others in enumerate(rounds):
            copies = []
            for s, (d, rel) in enumerate(others, base):
                copies.append(pltpu.make_async_remote_copy(src_ref=part.at[i], dst_ref=E.at[s], send_sem=esend.at[s], recv_sem=erecv.at[s], device_id=me.peer(d, rel), device_id_type=MESH))
            for copy in copies:
                copy.start()
            if i == 0:
                for x in TRIO:
                    loads[x].wait()
                    for lt in range(WIDE[x] // LANES):
                        wide_win[x][:, lt] = win[x][:, :, pl.ds(lt * LANES, LANES)].astype(F32)
            total = part[i]
            for s, copy in enumerate(copies, base):
                copy.wait_recv()
                total = total + E[s]
            part[i + 1] = total
            for copy in copies:
                copy.wait_send()
            base += len(others)
        mean = jnp.sum(part[2], keepdims=True) / count
        factor = jnp.minimum(1.0, 0.5 * lax.rsqrt(mean + 1e-30))
        for l in range(LAYERS):
            for u in TRIO:
                high = HIGH[u]
                wflat[l, u, pl.ds(ROWS - SUB, SUB), :] = jnp.zeros((SUB, LANES), F32)
                for ct in range(WIDE[u] // LANES):
                    x, lt = home(u, ct)
                    at = (slice(None), l, pl.ds(lt * LANES, LANES))
                    grad = flat[l, u, pl.ds(ct * high, high), :] * factor
                    new_m = 0.9 * m_in[x][at] + 0.1 * grad
                    new_v = 0.95 * v_in[x][at] + 0.05 * grad * grad
                    wide = wide_win[x][l, lt, pl.ds(p * high - window(p, x)[0], high), :]
                    new_w = wide - 0.02 * (new_m * lax.rsqrt(new_v + 1e-8) + 0.1 * wide)
                    m_out[x][at] = new_m
                    v_out[x][at] = new_v
                    wflat[l, u, pl.ds(ct * high, high), :] = new_w
        it = ag.bind(me, G, ssem, rsem)
        for u in TRIO:
            for c in TRIO:
                a, b, d = (me.up(x, 0) for x in ORDERS[c])
                for l in range(LAYERS):
                    G[c][a, b * torus.n[ORDERS[c][DIRECT]] + d, l, u] = wflat[l, u, pl.ds(c * CHUNK, CHUNK), :].astype(BF16)
        for a in ag.order:
            it.run(a)
        it.wait_sends()

    vmem = pl.BlockSpec(memory_space=pltpu.VMEM)
    nsum = len(rounds[0]) + len(rounds[1])
    shapes = [jax.ShapeDtypeStruct((torus.n[a], torus.n[b] * torus.n[d], LAYERS, 3, CHUNK, LANES), BF16) for a, b, d in ORDERS]
    turn = lambda ts: [jnp.transpose(t, (1, 0, 2)) for t in ts]
    m, v = turn(m), turn(v)
    f32 = [jax.ShapeDtypeStruct(t.shape, F32) for t in m]
    k = len(ag.copies)
    got = pl.pallas_call(
        kernel,
        out_shape=[pltpu.MemorySpace.VMEM(s.shape, s.dtype) for s in shapes + f32 * 2],
        in_specs=[vmem] + [pl.BlockSpec(memory_space=pl.ANY)] * 3 + [vmem] * 6,
        out_specs=[vmem] * 9,
        scratch_shapes=[
            pltpu.VMEM((LAYERS, 3, ROWS, LANES), F32),
            pltpu.VMEM((LAYERS, 3, ROWS, LANES), F32),
            pltpu.VMEM((3, SUB, LANES), F32),
            pltpu.VMEM((nsum, SUB, LANES), F32),
            pltpu.SemaphoreType.DMA((nsum,)),
            pltpu.SemaphoreType.DMA((nsum,)),
            pltpu.SemaphoreType.DMA((k,)),
            pltpu.SemaphoreType.DMA((k,)),
            [pltpu.VMEM((LAYERS, WINDOW[x], WIDE[x]), BF16) for x in TRIO],
            [pltpu.VMEM((LAYERS, WIDE[x] // LANES, WINDOW[x], LANES), F32) for x in TRIO],
            pltpu.SemaphoreType.DMA((3,)),
        ],
        compiler_params=pltpu.CompilerParams(collective_id=collective_id, has_side_effects=True, vmem_limit_bytes=26 * MIB),
        name="step_and_gather",
    )(g, *w, *m, *v)
    return got


def unpack(torus, got):
    nx, ny, nz = (torus.n[d] for d in "xyz")
    pair = 2
    group = pair * nz
    groups = torus.size // group
    pairs = ny // pair

    def kernel(g0, g1, g2, *refs):
        moments, outs, kept, (Z, Y, sem) = refs[:6], refs[6:9], refs[9:15], refs[15:]
        l, s = pl.program_id(0), pl.program_id(1)
        copies = [pltpu.make_async_copy(src, dst, sem.at[i]) for i, (src, dst) in enumerate(zip(moments, kept))]

        @pl.when(l + s == 0)
        def _():
            for copy in copies:
                copy.start()

        @pl.when(l + s == LAYERS - 1 + groups - 1)
        def _():
            for copy in copies:
                copy.wait()

        corner = {"x": lax.div(s, pairs), "y": lax.rem(s, pairs) * pair, "z": 0}
        for u in TRIO:
            high, wide = HIGH[u], WIDE[u] // LANES
            for i in range(group):
                y, z = divmod(i, nz)
                at = corner | {"y": corner["y"] + y, "z": z}
                for c, ref in enumerate((g0, g1, g2)):
                    a, b, d = ORDERS[c]
                    chunk = ref[at[a], at[b] * torus.n[d] + at[d], l, u].astype(F32)
                    if high > SUB:
                        for k, (ct, row, whole, more) in enumerate(tiles(u)[c * CHUNK // SUB : (c + 1) * CHUNK // SUB]):
                            Y[ct, pl.ds(high * i + row, whole), :] = chunk[SUB * k : SUB * k + whole]
                            if more and whole < SUB:
                                Y[ct + 1, pl.ds(high * i, SUB - whole), :] = chunk[SUB * k + whole : SUB * k + SUB]
                    else:
                        Z[i, pl.ds(c * CHUNK, CHUNK), :] = chunk
            for i in range(group):
                for ct in range(wide if high <= SUB else 0):
                    Y[ct, pl.ds(high * i, SUB), :] = Z[i, pl.ds(high * ct, SUB), :]
            rows = high * group
            for ct in range(wide):
                x, lt = home(u, ct)
                outs[x][0, :, pl.ds(lt * LANES, LANES)] = Y[ct, pl.ds(0, rows), :].astype(BF16)

    shapes = [(LAYERS, HIGH[u] * torus.size, WIDE[u]) for u in TRIO]
    return pl.pallas_call(
        kernel,
        grid=(LAYERS, groups),
        out_shape=[jax.ShapeDtypeStruct(s, BF16) for s in shapes] + [jax.ShapeDtypeStruct(m.shape, F32) for m in got[3:]],
        in_specs=[pl.BlockSpec(memory_space=pltpu.VMEM)] * 9,
        out_specs=[pl.BlockSpec((1, HIGH[u] * group, WIDE[u]), lambda l, s: (l, s, 0)) for u in TRIO] + [pl.BlockSpec(memory_space=pl.ANY)] * 6,
        scratch_shapes=[
            pltpu.VMEM((group, ROWS + SUB, LANES), F32),
            pltpu.VMEM((FF // LANES, HIGH[2] * group + SUB, LANES), F32),
            pltpu.SemaphoreType.DMA((6,)),
        ],
        compiler_params=pltpu.CompilerParams(vmem_limit_bytes=26 * MIB),
        name="unpack",
    )(*got)


NN, NT = ((1,), (0,)), ((1,), (1,))


def dot(a, b, dims=NN):
    return lax.dot_general(a, b, (dims, ((), ())), preferred_element_type=F32)


def scale_of(wide):
    return lax.rsqrt(jnp.mean(wide * wide, -1, keepdims=True) + 1e-6)


GAP = 24
SIDE_STRIDE, DOWN_STRIDE = D + GAP, FF // HALVES + GAP
DOWN_BASE = RING_TILES * SIDE_STRIDE
X_ROWS = DOWN_BASE + D // LANES * DOWN_STRIDE
COST = {"last": (3.6, 3.5), "first": (2.1, 3.5), "da": (2.5,), "norm": (0.45,)}
PACK_DOWN = 0.4
WHOLE = ((0,), (1, 2), (3, 4), (5, 6), (7, 8))
CHUNKS = {1: 0, 3: 1, 4: 2}
PASSES = ("forward", "last", "da", "norm", "first")
COUNT = {"forward": STEPS, "last": STEPS, "da": STEPS, "norm": TOKENS // TILE, "first": STEPS}
QUARTERS = TOKENS // PART
MAKE = 1


def timeline():
    out, lanes = [], ReduceScatter.LANES[RING]
    for kind in PASSES[1:]:
        layer = {"last": 1, "first": 0}.get(kind)
        for t in range(COUNT[kind]):
            half, tt = divmod(t, HALF)
            for i, cost in enumerate(COST[kind]):
                writes, whole = [], []
                if i == MAKE:
                    unit = (layer, half)
                    if tt == 0:
                        writes += [(unit, c) for c in TRIO]
                    if tt in CHUNKS:
                        whole += [((unit, COLOURS[half][CHUNKS[tt]]), lane) for lane in range(lanes)]
                    if tt == HALF - 1:
                        cost += PACK_DOWN
                        mine = [((layer, HALVES), c) for c in TRIO]
                        writes += [] if half else mine
                        whole += [(key, lane) for key in mine for lane in range(lanes) if half or lane == 0 and ORDERS[key[1]][CROSS] == "x"]
                out.append(((kind, t, i), cost, writes, whole))
    return out


def hidden_back(gate, up, d):
    s = jax.nn.sigmoid(gate)
    act = gate * s
    return (act * up).astype(BF16), (d * up * (s + act * (1.0 - s))).astype(BF16), (d * act).astype(BF16)


def gradients(torus, x, dy, wg, wu, wd, collective_id):
    rs = ReduceScatter(torus, CHUNK, 3)
    actions, copies, balance, flips = {}, {}, Balance(), {}
    for l in range(LAYERS):
        for u in TRIO:
            for c in TRIO:
                flips[l, u, c] = rs.flips(balance, c)
                got, sent = rs.plan((l, u), c, flips[l, u, c])
                copies |= sent
                actions |= got
                if l:
                    key = ((l, u), c)
                    actions[key, "free"] = ([("action", (key, "end", DIRECT))], [], TURN)
    slots = place(actions, copies, timeline())
    lines = torus.n["x"] * torus.n["y"]

    def kernel(x_ref, dy_ref, wg_ref, wu_ref, wd_ref, out, both_ref, gate_ref, up_ref, h1_ref, at0_ref, dyv, av, at, X, Mb, Db, Wb, Vb, Hb, once, pair, hsem, rsem, rsc):
        me = torus.here()
        it = rs.bind(me, rsc)
        copy = pltpu.make_async_copy
        save_at0, load_at0 = copy(at, at0_ref, once.at[1]), copy(at0_ref, at, once.at[1])

        def part(i):
            return pl.ds(i * TILE if isinstance(i, int) else pl.multiple_of(i * TILE, TILE), TILE)

        def sides(layer, t, s):
            return [copy(ref.at[layer, :, part(t)], Wb.at[s, :, part(k)], pair.at[k, s]) for k, ref in enumerate((wg_ref, wu_ref))]

        def fetch(kind, t, s):
            both, rows = pair.at[2, s], pair.at[3, s]
            if kind == "forward":
                return sides(0, t, s) + [copy(wd_ref.at[0, part(t)], Vb.at[s], rows)]
            if kind == "last":
                return sides(1, t, s) + [copy(wd_ref.at[1, part(t)], Vb.at[s], rows)]
            if kind == "da":
                return sides(1, t, s) + [copy(both_ref.at[t], Db.at[s], both)]
            if kind == "norm":
                return [copy(h1_ref.at[part(t)], Vb.at[s], rows)]
            return [copy(wd_ref.at[0, part(t)], Vb.at[s], rows)]

        def save(t, s):
            return copy(Db.at[s], both_ref.at[t], pair.at[4, s])

        def hiddens(t, quarters, out=False):
            got = []
            for q in quarters:
                for k, ref in enumerate((gate_ref, up_ref)):
                    ends = ref.at[pl.ds(t * LT, LT), pl.ds(q * PART, PART)], Hb.at[q, k]
                    got.append(copy(*(ends[::-1] if out else ends), hsem.at[q, k]))
            return got

        def act(a):
            ((l, u), c), what = a[0], a[1:]
            if what[0] == "free":
                it.wait_sends(u, c, flips[l, u, c])
                it.give_credit(u, c)
                return
            if what == ("start", 0) and l == 0:
                it.take_credit(u, c)

            def store(value):
                out[l, u, c] = value

            it.run(u, c, flips[l, u, c], what, store)

        def point(kind, t, i, which):
            for k in range(COUNT[kind]):
                if slots[kind, k, i][which]:

                    @pl.when(t == k)
                    def _(k=k):
                        for a in slots[kind, k, i][which]:
                            act(a)

        def normed_into(r):
            wide = dyv[part(r), :].astype(F32)
            a = (wide * scale_of(wide)).astype(BF16)
            av[part(r), :] = a
            at[:, part(r)] = a.T

        def lanes_of(ct):
            return slice(ct * LANES, (ct + 1) * LANES)

        def forward(t, s):
            for first in range(0, QUARTERS, 2):
                quarters = range(first, first + 2)

                @pl.when(t > 0)
                def _():
                    for f in hiddens(t - 1, quarters, True):
                        f.wait()

                for q in quarters:
                    rows = pl.ds(q * PART, PART)
                    both = dot(av[rows, :], Wb[s])
                    gate, up = both[:, :TILE], both[:, TILE:]
                    for j in range(LT):
                        Hb[q, 0, j], Hb[q, 1, j] = gate[:, lanes_of(j)], up[:, lanes_of(j)]
                    got = dot((jax.nn.silu(gate) * up).astype(BF16), Vb[s])
                    for ct in range(D // LANES):
                        here = pl.ds(ct * TOKENS + q * PART, PART)
                        X[here, :] = jnp.where(t == 0, 0.0, X[here, :]) + got[:, lanes_of(ct)]
                for f in hiddens(t, quarters, True):
                    f.start()

        def turn():
            for f in hiddens(STEPS - 1, range(QUARTERS), True):
                f.wait()
            save_at0.wait()
            count = TOKENS // TILE

            def saves(r):
                return copy(dyv.at[part(r)], h1_ref.at[part(r)], rsem.at[0, r])

            def loads(r):
                return copy(dy_ref.at[part(r)], dyv.at[part(r)], rsem.at[1, r])

            @pl.loop(0, count)
            def _(r):
                total = jnp.concatenate([X[pl.ds(ct * TOKENS + r * TILE, TILE), :] for ct in range(D // LANES)], axis=1)
                dyv[part(r), :] = dyv[part(r), :] + total.astype(BF16)
                normed_into(r)
                saves(r).start()

                @pl.when(r > 0)
                def _():
                    saves(r - 1).wait()
                    loads(r - 1).start()

            saves(count - 1).wait()
            loads(count - 1).start()
            for r in range(count):
                loads(r).wait()

        def hidden(kind, t, s):
            for first in range(0, QUARTERS, 2):
                quarters = range(first, first + 2)
                if kind == "first":
                    for f in hiddens(t, quarters):
                        f.wait()
                for q in quarters:
                    rows = pl.ds(q * PART, PART)
                    if kind == "last":
                        both = dot(av[rows, :], Wb[s])
                        gate, up = both[:, :TILE], both[:, TILE:]
                    else:
                        gate, up = (jnp.concatenate([Hb[q, k, j] for j in range(LT)], axis=1) for k in range(2))
                    d = dot(dyv[rows, :], Vb[s], NT).astype(BF16).astype(F32)
                    mid, Db[s, rows, part(0)], Db[s, rows, part(1)] = hidden_back(gate, up, d)
                    Mb[:, rows] = mid.T
                if kind == "first":

                    @pl.when(t + 1 < STEPS)
                    def _():
                        for f in hiddens(t + 1, quarters):
                            f.start()

        def make(kind, t, s):
            half, tt = lax.div(t, HALF), lax.rem(t, HALF)
            got = dot(at[...], Db[s])
            for k in range(2 * LT):
                X[pl.ds((lax.rem(tt, 2) * 2 * LT + k) * SIDE_STRIDE + 8, D), :] = got[:, lanes_of(k)]
            got = dot(Mb[...], dyv[...])
            for ct in range(D // LANES):
                X[pl.ds(DOWN_BASE + ct * DOWN_STRIDE + 8 + tt * TILE, TILE), :] = got[:, lanes_of(ct)]
            point(kind, t, MAKE, 0)
            for v, parts in enumerate(WHOLE):

                @pl.when(tt == v)
                def _(parts=parts):
                    pack(torus, 0, X, lambda ct: ct % RING_TILES * SIDE_STRIDE + 8, parts, 0, lines, [T.at[half] for T in it.T], COLOURS[0])

            @pl.when(tt == HALF - 1)
            def _():
                some = lines // HALVES
                pack(torus, HALVES, X, lambda ct: DOWN_BASE + ct * DOWN_STRIDE + 8, range(ROWS // 16), half * some, some, [T.at[HALVES] for T in it.T], COLOURS[HALVES])

        def d_a(t, s):
            for r in range(0, TOKENS, PART):
                got = dot(Db[s, pl.ds(r, PART), :], Wb[s], NT)
                for ct in range(D // LANES):
                    rows = pl.ds(ct * TOKENS + r, PART)
                    X[rows, :] = jnp.where(t == 0, 0.0, X[rows, :]) + got[:, lanes_of(ct)]

        def norm(t, s):
            da = jnp.concatenate([X[pl.ds(ct * TOKENS + t * TILE, TILE), :] for ct in range(D // LANES)], axis=1).astype(BF16).astype(F32)
            wide = Vb[s].astype(F32)
            scale = scale_of(wide)
            inner = jnp.mean(da * wide, -1, keepdims=True)
            dyv[part(t), :] = dyv[part(t), :] + (scale * da - wide * (scale * scale * scale * inner)).astype(BF16)

        def load_x(r):
            return copy(x_ref.at[part(r)], dyv.at[part(r)], rsem.at[0, r])

        for f in [load_x(r) for r in range(TOKENS // TILE)] + fetch("forward", 0, 0):
            f.start()
        arrive(me, rs.peers())

        @pl.loop(0, TOKENS // TILE)
        def _(r):
            load_x(r).wait()
            normed_into(r)

        save_at0.start()
        for number, kind in enumerate(PASSES):
            count = COUNT[kind]
            following = PASSES[number + 1] if number + 1 < len(PASSES) else None
            if kind == "last":
                turn()
                meet(rs.peers())
            if kind == "da":
                load_at0.start()
            if kind == "norm":
                for f in hiddens(0, range(QUARTERS)):
                    f.start()
            if kind == "first":
                load_at0.wait()

            def body(t, carry, kind=kind, count=count, following=following):
                s = lax.rem(t, 2)
                for f in fetch(kind, t, s):
                    f.wait()

                @pl.when(t + 1 < count)
                def _():
                    for f in fetch(kind, t + 1, 1 - s):
                        f.start()

                if kind == "last":

                    @pl.when(t > 1)
                    def _():
                        save(t - 2, s).wait()

                if following:

                    @pl.when(t == count - 1)
                    def _():
                        if kind == "last":
                            save(t - 1, 1 - s).wait()
                        for f in fetch(following, 0, 0):
                            f.start()

                if kind in ("last", "first"):
                    hidden(kind, t, s)
                    if kind == "last":
                        save(t, s).start()
                    point(kind, t, 0, 1)
                    make(kind, t, s)
                    point(kind, t, MAKE, 1)
                else:
                    {"forward": forward, "da": d_a, "norm": norm}[kind](t, s)
                    if kind != "forward":
                        point(kind, t, 0, 1)
                return carry

            lax.fori_loop(0, count, body, 0)
            if kind == "last":
                save(count - 1, (count - 1) % 2).wait()
        for u in TRIO:
            for c in TRIO:
                it.wait_sends(u, c, flips[0, u, c])

    any_space = pl.BlockSpec(memory_space=pl.ANY)
    return pl.pallas_call(
        kernel,
        out_shape=[jax.ShapeDtypeStruct((LAYERS, 3, 3, CHUNK, LANES), F32), jax.ShapeDtypeStruct((STEPS, TOKENS, 2 * TILE), BF16)]
        + [jax.ShapeDtypeStruct((FF // LANES, TOKENS, LANES), F32)] * 2
        + [jax.ShapeDtypeStruct((TOKENS, D), BF16), jax.ShapeDtypeStruct((D, TOKENS), BF16)],
        in_specs=[any_space] * 5,
        out_specs=[pl.BlockSpec(memory_space=pltpu.VMEM)] + [any_space] * 5,
        scratch_shapes=[
            pltpu.VMEM((TOKENS, D), BF16),
            pltpu.VMEM((TOKENS, D), BF16),
            pltpu.VMEM((D, TOKENS), BF16),
            pltpu.VMEM((X_ROWS, LANES), F32),
            pltpu.VMEM((TILE, TOKENS), BF16),
            pltpu.VMEM((2, TOKENS, 2 * TILE), BF16),
            pltpu.VMEM((2, D, 2 * TILE), BF16),
            pltpu.VMEM((2, TILE, D), BF16),
            pltpu.VMEM((QUARTERS, 2, LT, PART, LANES), F32),
            pltpu.SemaphoreType.DMA((2,)),
            pltpu.SemaphoreType.DMA((5, 2)),
            pltpu.SemaphoreType.DMA((QUARTERS, 2)),
            pltpu.SemaphoreType.DMA((2, TOKENS // TILE)),
            rs.scratch(),
        ],
        compiler_params=pltpu.CompilerParams(collective_id=collective_id, has_side_effects=True, vmem_limit_bytes=VMEM_ALL),
        cost_estimate=pl.CostEstimate(flops=TOKENS * D * FF * 24, bytes_accessed=TOKENS * FF * 20, transcendentals=0),
        name="gradients",
    )(x, dy, wg, wu, wd)[0]


def solution(mesh):
    torus = Torus(4, 4, 8)
    count = float(LAYERS * 3 * D * FF)

    def step(x, dy, wg, wu, wd, mg, mu, md, vg, vu, vd):
        x, dy = x[0], dy[0]
        g = gradients(torus, x, dy, wg, wu, wd, 1)
        got = step_and_gather(torus, g, (wg, wu, wd), (mg, mu, md), (vg, vu, vd), count, 2)
        new = unpack(torus, got)
        return (*new[:3], *(jnp.transpose(t, (1, 0, 2)) for t in new[3:]))

    P = jax.sharding.PartitionSpec
    return jax.shard_map(
        step,
        mesh=mesh,
        in_specs=(P(("rep", "dp")),) * 2 + (P(),) * 3 + (P(None, "dp"),) * 6,
        out_specs=(P("rep"),) * 3 + (P("rep", "dp"),) * 6,
        check_vma=False,
    )
```
